128 devices in a mesh: dp: 1, tp: 16 (over z, y), sp: 8 (over x, core).
Axes of the slice: x: 4, y: 4, z: 4, core: 2. Of those that a mesh axis runs over, the one named last changes fastest.
Arguments:
- x_in: bfloat16 [32768, 4096], P(('dp', 'sp'))
- w_z: bfloat16 [4096, 8192], P(None, 'tp')
- w_x: bfloat16 [4096, 8192], P(None, 'tp')
- w_bc: bfloat16 [4096, 256], replicated
- w_dt: bfloat16 [4096, 128], P(None, 'tp')
- a_neg: float32 [128], P('tp')
- dt_bias: float32 [128], P('tp')
- d_skip: float32 [128], P('tp')
- w_out: bfloat16 [8192, 4096], P('tp')
Outputs:
- output: bfloat16 [32768, 4096], P(('dp', 'sp', 'tp'))
All inputs are finite; a program needn't handle non-finite values.
Results may differ from the reference program's by a relative error of at most 0.0114328.
Values are sent between devices in bfloat16 or wider.
A program may use at most 1 GiB of HBM per device.

```python
import jax
import jax.numpy as jnp
from jax import lax

D_MODEL = 4096
N_HEADS = 128
HEAD_DIM = 64
D_STATE = 128
TOKENS_DEV = 4096
SEQ_DEVS = 8
PIECE_LEN = 64
D_INNER = N_HEADS * HEAD_DIM
SEQ_LEN = SEQ_DEVS * TOKENS_DEV


def setup_inputs(seed: int = 0, part: int = 0) -> dict:
    keys = jax.random.split(jax.random.key(seed), 9)
    x_key = jax.random.fold_in(keys[0], part)
    x_in = jax.random.normal(x_key, (SEQ_LEN, D_MODEL), jnp.float32)
    w_z = jax.random.normal(keys[1], (D_MODEL, D_INNER), jnp.float32) * D_MODEL ** -0.5
    w_x = jax.random.normal(keys[2], (D_MODEL, D_INNER), jnp.float32) * D_MODEL ** -0.5
    bc_scale = D_MODEL ** -0.5 * (D_STATE * TOKENS_DEV) ** -0.25
    w_bc = jax.random.normal(keys[3], (D_MODEL, 2 * D_STATE), jnp.float32) * bc_scale
    w_dt = jax.random.normal(keys[4], (D_MODEL, N_HEADS), jnp.float32) * (0.5 * D_MODEL ** -0.5)
    a_neg = -jax.random.uniform(keys[5], (N_HEADS,), jnp.float32, minval=0.4, maxval=1.6) / TOKENS_DEV
    dt_bias = jax.random.uniform(keys[6], (N_HEADS,), jnp.float32, minval=-1.0, maxval=1.0)
    d_skip = jax.random.uniform(keys[7], (N_HEADS,), jnp.float32, minval=0.5, maxval=1.5)
    w_out = jax.random.normal(keys[8], (D_INNER, D_MODEL), jnp.float32) * D_INNER ** -0.5
    return dict(x_in=x_in.astype(jnp.bfloat16), w_z=w_z.astype(jnp.bfloat16), w_x=w_x.astype(jnp.bfloat16), w_bc=w_bc.astype(jnp.bfloat16), w_dt=w_dt.astype(jnp.bfloat16), a_neg=a_neg, dt_bias=dt_bias, d_skip=d_skip, w_out=w_out.astype(jnp.bfloat16))


def ssd_scan(x_heads, dt_step, log_a, b_mat, c_mat):
    n_pieces = SEQ_LEN // PIECE_LEN
    pieces = (x_heads.reshape(n_pieces, PIECE_LEN, N_HEADS, HEAD_DIM), dt_step.reshape(n_pieces, PIECE_LEN, N_HEADS), log_a.reshape(n_pieces, PIECE_LEN, N_HEADS), b_mat.reshape(n_pieces, PIECE_LEN, D_STATE), c_mat.reshape(n_pieces, PIECE_LEN, D_STATE))
    positions = jnp.arange(PIECE_LEN)
    causal = (positions[:, None] >= positions[None, :])[:, :, None]

    def piece_step(state, piece):
        x_piece, dt_piece, la_piece, b_piece, c_piece = piece
        cum_log = jnp.cumsum(la_piece, axis=0)
        decay = jnp.where(causal, jnp.exp(jnp.minimum(cum_log[:, None, :] - cum_log[None, :, :], 0.0)), 0.0)
        gram = jnp.einsum('tn,sn->ts', c_piece, b_piece)
        weights = gram[:, :, None] * decay * dt_piece[None, :, :]
        y_piece = jnp.einsum('tsh,shp->thp', weights, x_piece)
        y_piece = y_piece + jnp.exp(cum_log)[:, :, None] * jnp.einsum('hpn,tn->thp', state, c_piece)
        to_end = jnp.exp(cum_log[-1][None, :] - cum_log) * dt_piece
        new_state = jnp.exp(cum_log[-1])[:, None, None] * state + jnp.einsum('sh,shp,sn->hpn', to_end, x_piece, b_piece)
        return new_state, y_piece

    init = jnp.zeros((N_HEADS, HEAD_DIM, D_STATE), jnp.float32)
    _, y_all = lax.scan(piece_step, init, pieces)
    return y_all.reshape(SEQ_LEN, N_HEADS, HEAD_DIM)


def reference(x_in, w_z, w_x, w_bc, w_dt, a_neg, dt_bias, d_skip, w_out):
    z_gate = jnp.dot(x_in, w_z, preferred_element_type=jnp.float32).astype(jnp.bfloat16)
    x_proj = jnp.dot(x_in, w_x, preferred_element_type=jnp.float32).astype(jnp.bfloat16)
    bc_val = jnp.dot(x_in, w_bc, preferred_element_type=jnp.float32).astype(jnp.bfloat16).astype(jnp.float32)
    dt_step = jax.nn.softplus(jnp.dot(x_in, w_dt, preferred_element_type=jnp.float32) + dt_bias)
    log_a = dt_step * a_neg
    x_heads = x_proj.astype(jnp.float32).reshape(SEQ_LEN, N_HEADS, HEAD_DIM)
    b_mat = bc_val[:, :D_STATE]
    c_mat = bc_val[:, D_STATE:]
    y_fwd = ssd_scan(x_heads, dt_step, log_a, b_mat, c_mat)
    y_bwd = ssd_scan(x_heads[::-1], dt_step[::-1], log_a[::-1], b_mat[::-1], c_mat[::-1])[::-1]
    y_sum = y_fwd + y_bwd + 2.0 * d_skip[:, None] * x_heads
    gated = (y_sum.reshape(SEQ_LEN, D_INNER) * jax.nn.silu(z_gate.astype(jnp.float32))).astype(jnp.bfloat16)
    mixed = jnp.dot(gated, w_out, preferred_element_type=jnp.float32)
    return (x_in.astype(jnp.float32) + mixed).astype(jnp.bfloat16)
```

```python
import functools

import jax
import jax.numpy as jnp
from jax import lax
from jax.experimental import pallas as pl
from jax.experimental.pallas import tpu as pltpu
from jax.sharding import PartitionSpec as P

CHUNK = 128
MSG_PAD = 16


def split3(v):
    hi = v.astype(jnp.bfloat16).astype(jnp.float32)
    rest = v - hi
    mid = rest.astype(jnp.bfloat16).astype(jnp.float32)
    return [hi, mid, rest - mid]


def spread_operand(quantities, width):
    rows = [part for q in quantities for part in split3(q)]
    have = sum(r.shape[0] for r in rows)
    rows.append(jnp.zeros((CHUNK - have, width), jnp.float32))
    return jnp.concatenate(rows, axis=0).T.astype(jnp.bfloat16)


def cumsum_lanes(v, lane):
    step = 1
    while step < v.shape[1]:
        v = v + jnp.where(lane >= step, pltpu.roll(v, step, 1), 0.0)
        step *= 2
    return v


def softplus(v):
    return jnp.maximum(v, 0.0) + jnp.log1p(jnp.exp(-jnp.abs(v)))


def scan_kernel(n_blk, n_seq, heads, head_dim, x_ref, wz_ref, wx_ref, wbc_ref, wdt_ref, bias_ref, aneg_ref, skip_ref, g_ref,
                z_s, u_s, bc_s, sf_s, sb_s, f_s, g_s, dt_s, ci_s, ce_s, le_s, lt_s, e_s, msg_s, rcv_s, send_sem, recv_sem):
    i = pl.program_id(0)
    me = lax.axis_index('sp')
    rows = x_ref.shape[0]
    inner = heads * head_dim
    per_blk = rows // CHUNK
    n_state = bc_s.shape[1] // 2
    f32, bf16 = jnp.float32, jnp.bfloat16
    lane = lax.broadcasted_iota(jnp.int32, (heads, CHUNK), 1)

    def peer_copy(s):
        dest = lax.rem(me + s, n_seq)
        side = jnp.where(me + s < n_seq, 0, 1)
        return pltpu.make_async_remote_copy(
            src_ref=msg_s.at[side], dst_ref=rcv_s.at[s - 1], send_sem=send_sem.at[s - 1], recv_sem=recv_sem.at[s - 1],
            device_id={'sp': dest}, device_id_type=pl.DeviceIdType.MESH)

    @pl.when(i == 0)
    def _():
        barrier = pltpu.get_barrier_semaphore()
        for s in range(1, n_seq):
            pl.semaphore_signal(barrier, inc=1, device_id={'sp': lax.rem(me + s, n_seq)}, device_id_type=pl.DeviceIdType.MESH)
        k = lax.broadcasted_iota(jnp.int32, e_s.shape, 0)
        j = lax.broadcasted_iota(jnp.int32, e_s.shape, 1)
        hit = (k // (3 * heads) == j // inner) & (k % heads == (j % inner) // head_dim)
        e_s[...] = jnp.where(hit, 1.0, 0.0).astype(bf16)
        f_s[...] = jnp.zeros_like(f_s)
        g_s[...] = jnp.zeros_like(g_s)
        lt_s[...] = jnp.zeros_like(lt_s)

    @pl.when(i < n_blk)
    def _():
        base = pl.multiple_of(i * rows, rows)
        xb = x_ref[...]
        raw = jnp.dot(xb, wdt_ref[...], preferred_element_type=f32)
        bc_s[pl.ds(base, rows), :] = jnp.dot(xb, wbc_ref[...], preferred_element_type=f32).astype(bf16)
        u_s[pl.ds(base, rows), :] = jnp.dot(xb, wx_ref[...], preferred_element_type=f32).astype(bf16)
        z_s[pl.ds(base, rows), :] = jnp.dot(xb, wz_ref[...], preferred_element_type=f32).astype(bf16)
        for c in range(per_blk):
            cc = i * per_blk + c
            at = pl.multiple_of(base + c * CHUNK, CHUNK)
            dt = softplus(raw[c * CHUNK:(c + 1) * CHUNK, :].T[:heads, :] + bias_ref[...])
            la = dt * aneg_ref[...]
            ci = cumsum_lanes(la, lane)
            ce = ci - la
            end = jnp.broadcast_to(ci[:, CHUNK - 1:], ci.shape)
            dt_s[cc] = dt
            ci_s[cc] = ci
            ce_s[cc] = ce
            q = spread_operand([jnp.exp(end - ci) * dt, jnp.exp(ce) * dt, end], CHUNK)
            w = jnp.dot(q, e_s[:, :2 * inner], preferred_element_type=f32)
            le = jnp.dot(q[:16], e_s[:, 2 * inner:], preferred_element_type=f32)[:8]
            le_s[cc] = le
            u = u_s[pl.ds(at, CHUNK), :].astype(f32)
            b = bc_s[pl.ds(at, CHUNK), :n_state]
            dims = (((0,), (0,)), ((), ()))
            sf = lax.dot_general(b, (u * w[:, :inner]).astype(bf16), dims, preferred_element_type=f32)
            sb = lax.dot_general(b, (u * w[:, inner:]).astype(bf16), dims, preferred_element_type=f32)
            sf_s[cc] = sf
            sb_s[cc] = sb
            lt = lt_s[...]
            f_s[...] = f_s[...] * jnp.exp(le[:1]) + sf
            g_s[...] = g_s[...] + jnp.exp(lt[:1]) * sb
            lt_s[...] = lt + le

    @pl.when(i == n_blk - 1)
    def _():
        lt = lt_s[:1]
        parts = split3(lt)
        row = lax.broadcasted_iota(jnp.int32, (MSG_PAD, inner), 0)
        tail = jnp.where(row == 0, parts[0], jnp.where(row == 1, parts[1], jnp.where(row == 2, parts[2], 0.0))).astype(bf16)
        for side, ref in ((0, f_s), (1, g_s)):
            msg_s[side, :n_state, :] = ref[...].astype(bf16)
            msg_s[side, n_state:, :] = tail
        pl.semaphore_wait(pltpu.get_barrier_semaphore(), n_seq - 1)
        for s in range(1, n_seq):
            peer_copy(s).start()

    @pl.when(i == n_blk)
    def _():
        for s in range(1, n_seq):
            peer_copy(s).wait()

        def log_of(s):
            t = rcv_s[s - 1, n_state:, :].astype(f32)
            return t[0:1] + t[1:2] + t[2:3]

        f_s[...] = jnp.zeros_like(f_s)
        g_s[...] = jnp.zeros_like(g_s)
        acc = jnp.zeros((1, inner), f32)
        for s in range(1, n_seq):
            wgt = jnp.where(s <= me, jnp.exp(acc), 0.0)
            f_s[...] += wgt * rcv_s[s - 1, :n_state, :].astype(f32)
            acc = acc + log_of(s)
        acc = jnp.zeros((1, inner), f32)
        for s in range(n_seq - 1, 0, -1):
            wgt = jnp.where(s > me, jnp.exp(acc), 0.0)
            g_s[...] += wgt * rcv_s[s - 1, :n_state, :].astype(f32)
            acc = acc + log_of(s)

        n_ch = n_blk * per_blk

        def back(t, _):
            c = n_ch - 1 - t
            mine = sb_s[c]
            g = g_s[...]
            sb_s[c] = g
            g_s[...] = g * jnp.exp(le_s[c][:1]) + mine
            return 0

        lax.fori_loop(0, n_ch, back, 0)

    @pl.when(i >= n_blk)
    def _():
        blk = i - n_blk
        base = pl.multiple_of(blk * rows, rows)
        trow = lax.broadcasted_iota(jnp.int32, (CHUNK, CHUNK), 0)
        tcol = lax.broadcasted_iota(jnp.int32, (CHUNK, CHUNK), 1)
        later = trow > tcol
        left = tcol < head_dim
        twice = jnp.where(trow == tcol, 2.0, 1.0)
        for c in range(per_blk):
            cc = blk * per_blk + c
            at = pl.multiple_of(base + c * CHUNK, CHUNK)
            dt, ci, ce = dt_s[cc], ci_s[cc], ce_s[cc]
            end = jnp.broadcast_to(ci[:, CHUNK - 1:], ci.shape)
            q = spread_operand([dt, jnp.exp(ci), jnp.exp(end - ce)], CHUNK)
            w = jnp.dot(q, e_s[...], preferred_element_type=f32)
            col = jnp.concatenate([ci, ce, jnp.zeros((CHUNK - 2 * heads, CHUNK), f32)], axis=0).T
            u = u_s[pl.ds(at, CHUNK), :].astype(f32)
            udt = (u * w[:, :inner]).astype(bf16)
            b = bc_s[pl.ds(at, CHUNK), :n_state]
            cm = bc_s[pl.ds(at, CHUNK), n_state:]
            gram = lax.dot_general(cm, b, (((1,), (1,)), ((), ())), preferred_element_type=f32) * twice
            f_in = f_s[...]
            y = jnp.dot(cm, f_in.astype(bf16), preferred_element_type=f32) * w[:, inner:2 * inner]
            y = y + jnp.dot(cm, sb_s[cc].astype(bf16), preferred_element_type=f32) * w[:, 2 * inner:]
            y = y + skip_ref[...] * u
            f_s[...] = f_in * jnp.exp(le_s[cc][:1]) + sf_s[cc]
            outs = []
            for p in range(heads // 2):
                mats = []
                for h in (2 * p, 2 * p + 1):
                    d = jnp.where(later, col[:, h:h + 1] - ci[h:h + 1, :], ce[h:h + 1, :] - col[:, heads + h:heads + h + 1])
                    mats.append((gram * jnp.exp(jnp.minimum(d, 0.0))).astype(bf16))
                up = udt[:, p * CHUNK:(p + 1) * CHUNK]
                zero = jnp.zeros_like(up)
                rhs = jnp.concatenate([jnp.where(left, up, zero), jnp.where(left, zero, up)], axis=0)
                outs.append(jnp.dot(jnp.concatenate(mats, axis=1), rhs, preferred_element_type=f32))
            y = y + jnp.concatenate(outs, axis=1)
            z = z_s[pl.ds(at, CHUNK), :].astype(f32)
            g_ref[c * CHUNK:(c + 1) * CHUNK, :] = (y * (z / (1.0 + jnp.exp(-z)))).astype(bf16)


def scan_call(x_blk, w_z, w_x, w_bc, w_dt, a_neg, dt_bias, d_skip, n_seq):
    tokens, d_model = x_blk.shape
    heads = a_neg.shape[0]
    inner = w_x.shape[1]
    head_dim = inner // heads
    n_state = w_bc.shape[1] // 2
    rows = min(512, tokens)
    n_blk = tokens // rows
    n_ch = tokens // CHUNK
    w_dt = jnp.pad(w_dt, ((0, 0), (0, CHUNK - heads)))
    bias = jnp.broadcast_to(dt_bias[:, None], (heads, CHUNK))
    aneg = jnp.broadcast_to(a_neg[:, None], (heads, CHUNK))
    skip = jnp.repeat(2.0 * d_skip, head_dim)[None, :]
    f32, bf16 = jnp.float32, jnp.bfloat16

    def whole(a):
        return pl.BlockSpec(a.shape, lambda i: (0, 0), pipeline_mode=pl.Buffered(1))

    return pl.pallas_call(
        functools.partial(scan_kernel, n_blk, n_seq, heads, head_dim),
        grid=(2 * n_blk,),
        out_shape=jax.ShapeDtypeStruct((tokens, inner), bf16),
        in_specs=[pl.BlockSpec((rows, d_model), lambda i: (jnp.minimum(i, n_blk - 1), 0))]
        + [whole(a) for a in (w_z, w_x, w_bc, w_dt, bias, aneg, skip)],
        out_specs=pl.BlockSpec((rows, inner), lambda i: (jnp.maximum(i - n_blk, 0), 0)),
        scratch_shapes=[
            pltpu.VMEM((tokens, inner), bf16),
            pltpu.VMEM((tokens, inner), bf16),
            pltpu.VMEM((tokens, 2 * n_state), bf16),
            pltpu.VMEM((n_ch, n_state, inner), f32),
            pltpu.VMEM((n_ch, n_state, inner), f32),
            pltpu.VMEM((n_state, inner), f32),
            pltpu.VMEM((n_state, inner), f32),
            pltpu.VMEM((n_ch, heads, CHUNK), f32),
            pltpu.VMEM((n_ch, heads, CHUNK), f32),
            pltpu.VMEM((n_ch, heads, CHUNK), f32),
            pltpu.VMEM((n_ch, 8, inner), f32),
            pltpu.VMEM((8, inner), f32),
            pltpu.VMEM((CHUNK, 3 * inner), bf16),
            pltpu.VMEM((2, n_state + MSG_PAD, inner), bf16),
            pltpu.VMEM((n_seq - 1, n_state + MSG_PAD, inner), bf16),
            pltpu.SemaphoreType.DMA((n_seq - 1,)),
            pltpu.SemaphoreType.DMA((n_seq - 1,)),
        ],
        compiler_params=pltpu.CompilerParams(collective_id=0, has_side_effects=True, vmem_limit_bytes=60 * 1024 * 1024,
                                             dimension_semantics=('arbitrary',)),
        cost_estimate=pl.CostEstimate(flops=2 * tokens * d_model * (2 * inner + 3 * n_state) * 3, bytes_accessed=60 << 20, transcendentals=0),
    )(x_blk, w_z, w_x, w_bc, w_dt, bias, aneg, skip)


def solution(mesh):
    n_model = mesh.shape['tp']
    n_seq = mesh.shape['sp']

    def device_fn(x_blk, w_z, w_x, w_bc, w_dt, a_neg, dt_bias, d_skip, w_out):
        tokens = x_blk.shape[0]
        inner, d_model = w_out.shape
        rows = tokens // n_model
        half = d_model // 2
        core = lax.axis_index('sp') % 2
        pair = [(i, i ^ 1) for i in range(n_seq)]
        w_half = lax.dynamic_slice_in_dim(w_out, core * half, half, axis=1)
        w_all = lax.all_gather(w_half, 'tp', axis=0, tiled=True)
        g = scan_call(x_blk, w_z, w_x, w_bc, w_dt, a_neg, dt_bias, d_skip, n_seq)
        g_mine = lax.all_to_all(g.reshape(n_model, rows, inner), 'tp', 0, 0, tiled=True)
        g_mine = g_mine.transpose(1, 0, 2).reshape(rows, n_model * inner)
        g_other = lax.ppermute(g_mine, 'sp', pair)
        out_other = jnp.dot(g_other, w_all, preferred_element_type=jnp.float32)
        back = lax.ppermute(out_other, 'sp', pair)
        out_mine = jnp.dot(g_mine, w_all, preferred_element_type=jnp.float32)
        first = core == 0
        mixed = jnp.concatenate([jnp.where(first, out_mine, back), jnp.where(first, back, out_mine)], axis=1)
        resid = lax.dynamic_slice_in_dim(x_blk, lax.axis_index('tp') * rows, rows, axis=0)
        return (resid.astype(jnp.float32) + mixed).astype(jnp.bfloat16)

    in_specs = (P(('dp', 'sp'), None), P(None, 'tp'), P(None, 'tp'), P(None, None), P(None, 'tp'), P('tp'), P('tp'), P('tp'), P('tp', None))
    out_specs = P(('dp', 'sp', 'tp'), None)
    return jax.shard_map(device_fn, mesh=mesh, in_specs=in_specs, out_specs=out_specs, check_vma=False)
```

```python
import functools

import jax
import jax.numpy as jnp
from jax import lax
from jax.experimental import pallas as pl
from jax.experimental.pallas import tpu as pltpu
from jax.sharding import PartitionSpec as P

CHUNK = 128
MSG_PAD = 16
RING = 4


def split3(v):
    hi = v.astype(jnp.bfloat16).astype(jnp.float32)
    rest = v - hi
    mid = rest.astype(jnp.bfloat16).astype(jnp.float32)
    return [hi, mid, rest - mid]


def spread_operand(quantities, width):
    rows = [part for q in quantities for part in split3(q)]
    have = sum(r.shape[0] for r in rows)
    rows.append(jnp.zeros((CHUNK - have, width), jnp.float32))
    return jnp.concatenate(rows, axis=0).T.astype(jnp.bfloat16)


def cumsum_lanes(v, lane):
    step = 1
    while step < v.shape[1]:
        v = v + jnp.where(lane >= step, pltpu.roll(v, step, 1), 0.0)
        step *= 2
    return v


def softplus(v):
    return jnp.maximum(v, 0.0) + jnp.log1p(jnp.exp(-jnp.abs(v)))


def tp_coords():
    index = lax.axis_index('tp')
    return index // RING, lax.rem(index, RING)


def ring_peer(zy, axis, dist):
    z, y = zy
    if axis == 0:
        return z * RING + lax.rem(y + dist, RING)
    return lax.rem(z + dist, RING) * RING + y


def scan_kernel(n_blk, n_seq, heads, head_dim, x_ref, wz_ref, wx_ref, wbc_ref, wdt_ref, bias_ref, aneg_ref, skip_ref, wo_ref, ga_ref, wg_ref,
                z_s, u_s, bc_s, sf_s, sb_s, f_s, g_s, dt_s, ci_s, ce_s, le_s, lt_s, e_s, msg_s, rcv_s, send_sem, recv_sem, ws_sem, wr_sem, gs_sem, gr_sem, own_sem):
    i = pl.program_id(0)
    me = lax.axis_index('sp')
    rows = x_ref.shape[0]
    inner = heads * head_dim
    per_blk = rows // CHUNK
    n_state = bc_s.shape[1] // 2
    f32, bf16 = jnp.float32, jnp.bfloat16
    lane = lax.broadcasted_iota(jnp.int32, (heads, CHUNK), 1)

    def peer_copy(s):
        dest = lax.rem(me + s, n_seq)
        side = jnp.where(me + s < n_seq, 0, 1)
        return pltpu.make_async_remote_copy(
            src_ref=msg_s.at[side], dst_ref=rcv_s.at[s - 1], send_sem=send_sem.at[s - 1], recv_sem=recv_sem.at[s - 1],
            device_id={'sp': dest}, device_id_type=pl.DeviceIdType.MESH)

    zy = tp_coords()

    def weight_copy(k):
        part = wo_ref.shape[0] // 2
        mine = pl.multiple_of(lax.rem(me, 2) * part, part)
        if k < 8:
            axis, back = k // 2 % 2, k % 2
            dist = RING - 1 if back else 1
            if k < 4:
                rows_at, src, slot = pl.ds(mine, part), wo_ref, dist
            else:
                rows_at = pl.ds(pl.multiple_of(mine + back * (part // 2), part // 2), part // 2)
                src, slot = wg_ref.at[axis * 3 + dist - 1], 2
            dest = {'tp': ring_peer(zy, axis, dist)}
        else:
            axis, slot = ((k - 8) // 2, (1, 3)[k % 2]) if k < 12 else (k - 12, 2)
            rows_at, src = pl.ds(mine, part), wg_ref.at[axis * 3 + slot - 1]
            dest = {'sp': me + 1 - 2 * lax.rem(me, 2)}
        return pltpu.make_async_remote_copy(
            src_ref=src.at[rows_at, :], dst_ref=wg_ref.at[axis * 3 + slot - 1, rows_at, :], send_sem=ws_sem.at[k], recv_sem=wr_sem.at[k],
            device_id=dest, device_id_type=pl.DeviceIdType.MESH)

    def gate_copy(side, dist, group, at):
        return pltpu.make_async_remote_copy(
            src_ref=z_s.at[pl.ds(at, CHUNK), :], dst_ref=ga_ref.at[side, dist, pl.ds(pl.multiple_of(group * CHUNK, CHUNK), CHUNK), :],
            send_sem=gs_sem.at[side, dist, group], recv_sem=gr_sem.at[side, dist, group],
            device_id={'tp': ring_peer(zy, side, dist)}, device_id_type=pl.DeviceIdType.MESH)

    def own_copy(side, group, at):
        return pltpu.make_async_copy(z_s.at[pl.ds(at, CHUNK), :], ga_ref.at[side, 0, pl.ds(pl.multiple_of(group * CHUNK, CHUNK), CHUNK), :],
                                     own_sem.at[side, group])

    @pl.when(i == 0)
    def _():
        barrier = pltpu.get_barrier_semaphore()
        for s in range(1, n_seq):
            pl.semaphore_signal(barrier, inc=1, device_id={'sp': lax.rem(me + s, n_seq)}, device_id_type=pl.DeviceIdType.MESH)
        for axis in range(2):
            for dist in range(1, RING):
                pl.semaphore_signal(barrier, inc=1, device_id={'tp': ring_peer(zy, axis, dist)}, device_id_type=pl.DeviceIdType.MESH)
        pl.semaphore_wait(barrier, n_seq - 1 + 2 * (RING - 1))
        for k in range(4):
            weight_copy(k).start()
        k = lax.broadcasted_iota(jnp.int32, e_s.shape, 0)
        j = lax.broadcasted_iota(jnp.int32, e_s.shape, 1)
        hit = (k // (3 * heads) == j // inner) & (k % heads == (j % inner) // head_dim)
        e_s[...] = jnp.where(hit, 1.0, 0.0).astype(bf16)
        f_s[...] = jnp.zeros_like(f_s)
        g_s[...] = jnp.zeros_like(g_s)
        lt_s[...] = jnp.zeros_like(lt_s)

    @pl.when(i < n_blk)
    def _():
        base = pl.multiple_of(i * rows, rows)
        xb = x_ref[...]
        raw = jnp.dot(xb, wdt_ref[...], preferred_element_type=f32)
        bc_s[pl.ds(base, rows), :] = jnp.dot(xb, wbc_ref[...], preferred_element_type=f32).astype(bf16)
        u_s[pl.ds(base, rows), :] = jnp.dot(xb, wx_ref[...], preferred_element_type=f32).astype(bf16)
        z_s[pl.ds(base, rows), :] = jnp.dot(xb, wz_ref[...], preferred_element_type=f32).astype(bf16)
        for c in range(per_blk):
            cc = i * per_blk + c
            at = pl.multiple_of(base + c * CHUNK, CHUNK)
            dt = softplus(raw[c * CHUNK:(c + 1) * CHUNK, :].T[:heads, :] + bias_ref[...])
            la = dt * aneg_ref[...]
            ci = cumsum_lanes(la, lane)
            ce = ci - la
            end = jnp.broadcast_to(ci[:, CHUNK - 1:], ci.shape)
            dt_s[cc] = dt
            ci_s[cc] = ci
            ce_s[cc] = ce
            q = spread_operand([jnp.exp(end - ci) * dt, jnp.exp(ce) * dt, end], CHUNK)
            w = jnp.dot(q, e_s[:, :2 * inner], preferred_element_type=f32)
            le = jnp.dot(q[:16], e_s[:, 2 * inner:], preferred_element_type=f32)[:8]
            le_s[cc] = le
            u = u_s[pl.ds(at, CHUNK), :].astype(f32)
            b = bc_s[pl.ds(at, CHUNK), :n_state]
            dims = (((0,), (0,)), ((), ()))
            sf = lax.dot_general(b, (u * w[:, :inner]).astype(bf16), dims, preferred_element_type=f32)
            sb = lax.dot_general(b, (u * w[:, inner:]).astype(bf16), dims, preferred_element_type=f32)
            sf_s[cc] = sf
            sb_s[cc] = sb
            lt = lt_s[...]
            f_s[...] = f_s[...] * jnp.exp(le[:1]) + sf
            g_s[...] = g_s[...] + jnp.exp(lt[:1]) * sb
            lt_s[...] = lt + le

    @pl.when(i == n_blk - 1)
    def _():
        lt = lt_s[:1]
        parts = split3(lt)
        row = lax.broadcasted_iota(jnp.int32, (MSG_PAD, inner), 0)
        tail = jnp.where(row == 0, parts[0], jnp.where(row == 1, parts[1], jnp.where(row == 2, parts[2], 0.0))).astype(bf16)
        for side, ref in ((0, f_s), (1, g_s)):
            msg_s[side, :n_state, :] = ref[...].astype(bf16)
            msg_s[side, n_state:, :] = tail
        for s in range(1, n_seq):
            peer_copy(s).start()

    @pl.when(i == n_blk)
    def _():
        for k in range(4):
            weight_copy(k).wait()
        for k in range(4, 12):
            weight_copy(k).start()
        for s in range(1, n_seq):
            peer_copy(s).wait()

        def log_of(s):
            t = rcv_s[s - 1, n_state:, :].astype(f32)
            return t[0:1] + t[1:2] + t[2:3]

        f_s[...] = jnp.zeros_like(f_s)
        g_s[...] = jnp.zeros_like(g_s)
        acc = jnp.zeros((1, inner), f32)
        for s in range(1, n_seq):
            wgt = jnp.where(s <= me, jnp.exp(acc), 0.0)
            f_s[...] += wgt * rcv_s[s - 1, :n_state, :].astype(f32)
            acc = acc + log_of(s)
        acc = jnp.zeros((1, inner), f32)
        for s in range(n_seq - 1, 0, -1):
            wgt = jnp.where(s > me, jnp.exp(acc), 0.0)
            g_s[...] += wgt * rcv_s[s - 1, :n_state, :].astype(f32)
            acc = acc + log_of(s)

        n_ch = n_blk * per_blk

        def back(t, _):
            c = n_ch - 1 - t
            mine = sb_s[c]
            g = g_s[...]
            sb_s[c] = g
            g_s[...] = g * jnp.exp(le_s[c][:1]) + mine
            return 0

        lax.fori_loop(0, n_ch, back, 0)

    @pl.when(i >= n_blk)
    def _():
        blk = i - n_blk
        base = pl.multiple_of(blk * rows, rows)
        trow = lax.broadcasted_iota(jnp.int32, (CHUNK, CHUNK), 0)
        tcol = lax.broadcasted_iota(jnp.int32, (CHUNK, CHUNK), 1)
        later = trow > tcol
        left = tcol < head_dim
        twice = jnp.where(trow == tcol, 2.0, 1.0)
        for c in range(per_blk):
            cc = blk * per_blk + c
            at = pl.multiple_of(base + c * CHUNK, CHUNK)
            dt, ci, ce = dt_s[cc], ci_s[cc], ce_s[cc]
            end = jnp.broadcast_to(ci[:, CHUNK - 1:], ci.shape)
            q = spread_operand([dt, jnp.exp(ci), jnp.exp(end - ce)], CHUNK)
            w = jnp.dot(q, e_s[...], preferred_element_type=f32)
            col = jnp.concatenate([ci, ce, jnp.zeros((CHUNK - 2 * heads, CHUNK), f32)], axis=0).T
            u = u_s[pl.ds(at, CHUNK), :].astype(f32)
            udt = (u * w[:, :inner]).astype(bf16)
            b = bc_s[pl.ds(at, CHUNK), :n_state]
            cm = bc_s[pl.ds(at, CHUNK), n_state:]
            gram = lax.dot_general(cm, b, (((1,), (1,)), ((), ())), preferred_element_type=f32) * twice
            f_in = f_s[...]
            y = jnp.dot(cm, f_in.astype(bf16), preferred_element_type=f32) * w[:, inner:2 * inner]
            y = y + jnp.dot(cm, sb_s[cc].astype(bf16), preferred_element_type=f32) * w[:, 2 * inner:]
            y = y + skip_ref[...] * u
            f_s[...] = f_in * jnp.exp(le_s[cc][:1]) + sf_s[cc]
            outs = []
            for p in range(heads // 2):
                mats = []
                for h in (2 * p, 2 * p + 1):
                    d = jnp.where(later, col[:, h:h + 1] - ci[h:h + 1, :], ce[h:h + 1, :] - col[:, heads + h:heads + h + 1])
                    mats.append((gram * jnp.exp(jnp.minimum(d, 0.0))).astype(bf16))
                up = udt[:, p * CHUNK:(p + 1) * CHUNK]
                zero = jnp.zeros_like(up)
                rhs = jnp.concatenate([jnp.where(left, up, zero), jnp.where(left, zero, up)], axis=0)
                outs.append(jnp.dot(jnp.concatenate(mats, axis=1), rhs, preferred_element_type=f32))
            y = y + jnp.concatenate(outs, axis=1)
            z = z_s[pl.ds(at, CHUNK), :].astype(f32)
            z_s[pl.ds(at, CHUNK), :] = (y * (z / (1.0 + jnp.exp(-z)))).astype(bf16)
        for c in range(per_blk):
            at = pl.multiple_of(base + c * CHUNK, CHUNK)
            side = c % 2
            owner = blk * (per_blk // 2) + c // 2
            far = (lax.rem(owner // RING - zy[0] + RING, RING), lax.rem(lax.rem(owner, RING) - zy[1] + RING, RING))
            dist, group = (far[1], far[0]) if side == 0 else (far[0], far[1])

            @pl.when(dist == 0)
            def _():
                own_copy(side, group, at).start()

            @pl.when(dist > 0)
            def _():
                gate_copy(side, dist, group, at).start()

    @pl.when(i == n_blk + n_blk // 2)
    def _():
        for k in range(4, 8):
            weight_copy(k).wait()
        for k in range(12, 14):
            weight_copy(k).start()

    @pl.when(i == 2 * n_blk - 1)
    def _():
        for side in range(2):
            for group in range(RING):
                own_copy(side, group, 0).wait()
                for dist in range(1, RING):
                    gate_copy(side, dist, group, 0).wait()
        for k in range(8, 14):
            weight_copy(k).wait()


def scan_call(x_blk, w_z, w_x, w_bc, w_dt, a_neg, dt_bias, d_skip, w_out, n_seq):
    tokens, d_model = x_blk.shape
    heads = a_neg.shape[0]
    inner = w_x.shape[1]
    head_dim = inner // heads
    n_state = w_bc.shape[1] // 2
    rows = min(512, tokens)
    n_blk = tokens // rows
    n_ch = tokens // CHUNK
    w_dt = jnp.pad(w_dt, ((0, 0), (0, CHUNK - heads)))
    bias = jnp.broadcast_to(dt_bias[:, None], (heads, CHUNK))
    aneg = jnp.broadcast_to(a_neg[:, None], (heads, CHUNK))
    skip = jnp.repeat(2.0 * d_skip, head_dim)[None, :]
    f32, bf16 = jnp.float32, jnp.bfloat16

    def whole(a):
        return pl.BlockSpec(a.shape, lambda i: (0, 0), pipeline_mode=pl.Buffered(1))

    return pl.pallas_call(
        functools.partial(scan_kernel, n_blk, n_seq, heads, head_dim),
        grid=(2 * n_blk,),
        out_shape=(jax.ShapeDtypeStruct((2, RING, tokens // (2 * RING), inner), bf16),
                   jax.ShapeDtypeStruct((2 * (RING - 1),) + w_out.shape, bf16)),
        in_specs=[pl.BlockSpec((rows, d_model), lambda i: (jnp.minimum(i, n_blk - 1), 0))]
        + [whole(a) for a in (w_z, w_x, w_bc, w_dt, bias, aneg, skip)] + [pl.BlockSpec(memory_space=pl.ANY)],
        out_specs=(pl.BlockSpec(memory_space=pl.ANY), pl.BlockSpec(memory_space=pl.ANY)),
        scratch_shapes=[
            pltpu.VMEM((tokens, inner), bf16),
            pltpu.VMEM((tokens, inner), bf16),
            pltpu.VMEM((tokens, 2 * n_state), bf16),
            pltpu.VMEM((n_ch, n_state, inner), f32),
            pltpu.VMEM((n_ch, n_state, inner), f32),
            pltpu.VMEM((n_state, inner), f32),
            pltpu.VMEM((n_state, inner), f32),
            pltpu.VMEM((n_ch, heads, CHUNK), f32),
            pltpu.VMEM((n_ch, heads, CHUNK), f32),
            pltpu.VMEM((n_ch, heads, CHUNK), f32),
            pltpu.VMEM((n_ch, 8, inner), f32),
            pltpu.VMEM((8, inner), f32),
            pltpu.VMEM((CHUNK, 3 * inner), bf16),
            pltpu.VMEM((2, n_state + MSG_PAD, inner), bf16),
            pltpu.VMEM((n_seq - 1, n_state + MSG_PAD, inner), bf16),
            pltpu.SemaphoreType.DMA((n_seq - 1,)),
            pltpu.SemaphoreType.DMA((n_seq - 1,)),
            pltpu.SemaphoreType.DMA((14,)),
            pltpu.SemaphoreType.DMA((14,)),
            pltpu.SemaphoreType.DMA((2, RING, RING)),
            pltpu.SemaphoreType.DMA((2, RING, RING)),
            pltpu.SemaphoreType.DMA((2, RING)),
        ],
        compiler_params=pltpu.CompilerParams(collective_id=0, has_side_effects=True, vmem_limit_bytes=60 * 1024 * 1024,
                                             dimension_semantics=('arbitrary',)),
        cost_estimate=pl.CostEstimate(flops=2 * tokens * d_model * (2 * inner + 3 * n_state) * 3, bytes_accessed=60 << 20, transcendentals=0),
    )(x_blk, w_z, w_x, w_bc, w_dt, bias, aneg, skip, w_out)


def out_kernel(n_col, ga_ref, wo_ref, wg_ref, x_ref, out_ref, send_s, recv_s, own_s, x_s, x_sem, send_sem, recv_sem):
    i = pl.program_id(0)
    zy = tp_coords()
    width = wo_ref.shape[1]
    f32, bf16 = jnp.float32, jnp.bfloat16

    def part_copy(side, dist, b):
        return pltpu.make_async_remote_copy(
            src_ref=send_s.at[side, dist - 1, b], dst_ref=recv_s.at[side, dist - 1, b],
            send_sem=send_sem.at[side, dist - 1, b], recv_sem=recv_sem.at[side, dist - 1, b],
            device_id={'tp': ring_peer(zy, 1 - side, dist)}, device_id_type=pl.DeviceIdType.MESH)

    def x_copy():
        rows = x_s.shape[0]
        at = pl.multiple_of(lax.axis_index('tp') * rows, rows)
        return pltpu.make_async_copy(x_ref.at[pl.ds(at, rows), :], x_s, x_sem)

    @pl.when(i == 0)
    def _():
        x_copy().start()
        barrier = pltpu.get_barrier_semaphore()
        for axis in range(2):
            for dist in range(1, RING):
                pl.semaphore_signal(barrier, inc=1, device_id={'tp': ring_peer(zy, axis, dist)}, device_id_type=pl.DeviceIdType.MESH)

    @pl.when(i < n_col)
    def _():
        for side in range(2):
            acc = jnp.dot(ga_ref[side, 0], wo_ref[...], preferred_element_type=f32)
            for dist in range(1, RING):
                acc = acc + jnp.dot(ga_ref[side, dist], wg_ref[side * 3 + dist - 1], preferred_element_type=f32)
            own_s[side, i] = acc[:CHUNK]
            for dist in range(1, RING):
                send_s[side, dist - 1, i] = acc[dist * CHUNK:(dist + 1) * CHUNK].astype(bf16)

    @pl.when(i == 0)
    def _():
        pl.semaphore_wait(pltpu.get_barrier_semaphore(), 2 * (RING - 1))

    @pl.when(i < n_col)
    def _():
        for side in range(2):
            for dist in range(1, RING):
                part_copy(side, dist, i).start()

    @pl.when(i == n_col)
    def _():
        x_copy().wait()

    @pl.when(i >= n_col)
    def _():
        b = i - n_col
        cols = pl.ds(pl.multiple_of(b * width, width), width)
        for side in range(2):
            acc = own_s[side, b]
            for dist in range(1, RING):
                part_copy(side, dist, b).wait()
                acc = acc + recv_s[side, dist - 1, b].astype(f32)
            at = side * CHUNK
            out_ref[at:at + CHUNK, :] = (x_s[at:at + CHUNK, cols].astype(f32) + acc).astype(bf16)


def out_call(g_all, w_out, w_got, x_blk):
    inner, d_model = w_out.shape
    rows = 2 * CHUNK
    width = min(512, d_model)
    n_col = d_model // width
    f32, bf16 = jnp.float32, jnp.bfloat16

    def column(i):
        return jnp.minimum(i, n_col - 1)

    return pl.pallas_call(
        functools.partial(out_kernel, n_col),
        grid=(2 * n_col,),
        out_shape=jax.ShapeDtypeStruct((rows, d_model), bf16),
        in_specs=[pl.BlockSpec(g_all.shape, lambda i: (0, 0, 0, 0), pipeline_mode=pl.Buffered(1)),
                  pl.BlockSpec((inner, width), lambda i: (0, column(i))),
                  pl.BlockSpec((2 * (RING - 1), inner, width), lambda i: (0, 0, column(i))),
                  pl.BlockSpec(memory_space=pl.ANY)],
        out_specs=pl.BlockSpec((rows, width), lambda i: (0, jnp.maximum(i - n_col, 0))),
        scratch_shapes=[
            pltpu.VMEM((2, RING - 1, n_col, CHUNK, width), bf16),
            pltpu.VMEM((2, RING - 1, n_col, CHUNK, width), bf16),
            pltpu.VMEM((2, n_col, CHUNK, width), f32),
            pltpu.VMEM((rows, d_model), bf16),
            pltpu.SemaphoreType.DMA,
            pltpu.SemaphoreType.DMA((2, RING - 1, n_col)),
            pltpu.SemaphoreType.DMA((2, RING - 1, n_col)),
        ],
        compiler_params=pltpu.CompilerParams(collective_id=1, has_side_effects=True, vmem_limit_bytes=60 * 1024 * 1024,
                                             dimension_semantics=('arbitrary',)),
        cost_estimate=pl.CostEstimate(flops=2 * 2 * 4 * CHUNK * 4 * inner * d_model, bytes_accessed=40 << 20, transcendentals=0),
    )(g_all, w_out, w_got, x_blk)


def solution(mesh):
    n_seq = mesh.shape['sp']

    def device_fn(x_blk, w_z, w_x, w_bc, w_dt, a_neg, dt_bias, d_skip, w_out):
        g_all, w_got = scan_call(x_blk, w_z, w_x, w_bc, w_dt, a_neg, dt_bias, d_skip, w_out, n_seq)
        return out_call(g_all, w_out, w_got, x_blk)

    in_specs = (P(('dp', 'sp'), None), P(None, 'tp'), P(None, 'tp'), P(None, None), P(None, 'tp'), P('tp'), P('tp'), P('tp'), P('tp', None))
    out_specs = P(('dp', 'sp', 'tp'), None)
    return jax.shard_map(device_fn, mesh=mesh, in_specs=in_specs, out_specs=out_specs, check_vma=False)
```

```python
import functools

import jax
import jax.numpy as jnp
from jax import lax
from jax.experimental import pallas as pl
from jax.experimental.pallas import tpu as pltpu
from jax.sharding import PartitionSpec as P

CHUNK = 128
MSG_PAD = 16
RING = 4


def split3(v):
    hi = v.astype(jnp.bfloat16).astype(jnp.float32)
    rest = v - hi
    mid = rest.astype(jnp.bfloat16).astype(jnp.float32)
    return [hi, mid, rest - mid]


def spread_operand(quantities, width):
    rows = [part for q in quantities for part in split3(q)]
    have = sum(r.shape[0] for r in rows)
    rows.append(jnp.zeros((CHUNK - have, width), jnp.float32))
    return jnp.concatenate(rows, axis=0).T.astype(jnp.bfloat16)


def cumsum_lanes(v, lane):
    step = 1
    while step < v.shape[1]:
        v = v + jnp.where(lane >= step, pltpu.roll(v, step, 1), 0.0)
        step *= 2
    return v


def softplus(v):
    return jnp.maximum(v, 0.0) + jnp.log1p(jnp.exp(-jnp.abs(v)))


def tp_coords():
    index = lax.axis_index('tp')
    return index // RING, lax.rem(index, RING)


def ring_peer(zy, axis, dist):
    z, y = zy
    if axis == 0:
        return z * RING + lax.rem(y + dist, RING)
    return lax.rem(z + dist, RING) * RING + y


def scan_kernel(n_blk, n_seq, heads, head_dim, x_ref, wz_ref, wx_ref, wbc_ref, wdt_ref, bias_sm, aneg_sm, skip_sm, wo_ref, ga_ref, wg_ref,
                z_s, u_s, bc_s, sf_s, sb_s, f_s, g_s, dt_s, ci_s, ce_s, le_s, lt_s, e_s, msg_s, rcv_s, bias_ref, aneg_ref, skip_ref, wz_s, wz_sem, send_sem, recv_sem, ws_sem, wr_sem, gs_sem, gr_sem, own_sem):
    i = pl.program_id(0)
    me = lax.axis_index('sp')
    rows = x_ref.shape[0]
    inner = heads * head_dim
    per_blk = rows // CHUNK
    n_state = bc_s.shape[1] // 2
    f32, bf16 = jnp.float32, jnp.bfloat16
    lane = lax.broadcasted_iota(jnp.int32, (heads, CHUNK), 1)

    def peer_copy(s):
        dest = lax.rem(me + s, n_seq)
        side = jnp.where(me + s < n_seq, 0, 1)
        return pltpu.make_async_remote_copy(
            src_ref=msg_s.at[side], dst_ref=rcv_s.at[s - 1], send_sem=send_sem.at[s - 1], recv_sem=recv_sem.at[s - 1],
            device_id={'sp': dest}, device_id_type=pl.DeviceIdType.MESH)

    zy = tp_coords()
    z_first, y_first = n_blk, 2 * n_blk

    def wz_copy():
        return pltpu.make_async_copy(wz_ref, wz_s, wz_sem)

    def weight_copy(k):
        part = wo_ref.shape[0] // 2
        mine = pl.multiple_of(lax.rem(me, 2) * part, part)
        if k < 8:
            axis, back = k // 2 % 2, k % 2
            dist = RING - 1 if back else 1
            if k < 4:
                rows_at, src, slot = pl.ds(mine, part), wo_ref, dist
            else:
                rows_at = pl.ds(pl.multiple_of(mine + back * (part // 2), part // 2), part // 2)
                src, slot = wg_ref.at[axis * 3 + dist - 1], 2
            dest = {'tp': ring_peer(zy, axis, dist)}
        else:
            axis, slot = ((k - 8) // 2, (1, 3)[k % 2]) if k < 12 else (k - 12, 2)
            rows_at, src = pl.ds(mine, part), wg_ref.at[axis * 3 + slot - 1]
            dest = {'sp': me + 1 - 2 * lax.rem(me, 2)}
        return pltpu.make_async_remote_copy(
            src_ref=src.at[rows_at, :], dst_ref=wg_ref.at[axis * 3 + slot - 1, rows_at, :], send_sem=ws_sem.at[k], recv_sem=wr_sem.at[k],
            device_id=dest, device_id_type=pl.DeviceIdType.MESH)

    def gate_copy(side, dist, group, at):
        return pltpu.make_async_remote_copy(
            src_ref=z_s.at[pl.ds(at, CHUNK), :], dst_ref=ga_ref.at[side, dist, pl.ds(pl.multiple_of(group * CHUNK, CHUNK), CHUNK), :],
            send_sem=gs_sem.at[side, dist, group], recv_sem=gr_sem.at[side, dist, group],
            device_id={'tp': ring_peer(zy, side, dist)}, device_id_type=pl.DeviceIdType.MESH)

    def own_copy(side, group, at):
        return pltpu.make_async_copy(z_s.at[pl.ds(at, CHUNK), :], ga_ref.at[side, 0, pl.ds(pl.multiple_of(group * CHUNK, CHUNK), CHUNK), :],
                                     own_sem.at[side, group])

    @pl.when(i == 0)
    def _():
        barrier = pltpu.get_barrier_semaphore()
        for s in range(1, n_seq):
            pl.semaphore_signal(barrier, inc=1, device_id={'sp': lax.rem(me + s, n_seq)}, device_id_type=pl.DeviceIdType.MESH)
        for axis in range(2):
            for dist in range(1, RING):
                pl.semaphore_signal(barrier, inc=1, device_id={'tp': ring_peer(zy, axis, dist)}, device_id_type=pl.DeviceIdType.MESH)
        pl.semaphore_wait(barrier, n_seq - 1 + 2 * (RING - 1))
        for k in range(4):
            weight_copy(k).start()
        wz_copy().start()
        head = lax.broadcasted_iota(jnp.int32, bias_ref.shape, 0)
        owner = lax.broadcasted_iota(jnp.int32, skip_ref.shape, 1) // head_dim
        bias, aneg, skip = jnp.zeros_like(bias_ref), jnp.zeros_like(aneg_ref), jnp.zeros_like(skip_ref)
        for h in range(heads):
            bias = jnp.where(head == h, bias_sm[h], bias)
            aneg = jnp.where(head == h, aneg_sm[h], aneg)
            skip = jnp.where(owner == h, 2.0 * skip_sm[h], skip)
        bias_ref[...] = bias
        aneg_ref[...] = aneg
        skip_ref[...] = skip
        k = lax.broadcasted_iota(jnp.int32, e_s.shape, 0)
        j = lax.broadcasted_iota(jnp.int32, e_s.shape, 1)
        hit = (k // (3 * heads) == j // inner) & (k % heads == (j % inner) // head_dim)
        e_s[...] = jnp.where(hit, 1.0, 0.0).astype(bf16)
        f_s[...] = jnp.zeros_like(f_s)
        g_s[...] = jnp.zeros_like(g_s)
        lt_s[...] = jnp.zeros_like(lt_s)

    @pl.when(i < n_blk)
    def _():
        base = pl.multiple_of(i * rows, rows)
        xb = x_ref[...]
        raw = lax.dot_general(xb, wdt_ref[...], (((1,), (1,)), ((), ())), preferred_element_type=f32)
        bc_s[pl.ds(base, rows), :] = jnp.dot(xb, wbc_ref[...], preferred_element_type=f32).astype(bf16)
        u_s[pl.ds(base, rows), :] = jnp.dot(xb, wx_ref[...], preferred_element_type=f32).astype(bf16)
        for c in range(per_blk):
            cc = i * per_blk + c
            at = pl.multiple_of(base + c * CHUNK, CHUNK)
            dt = softplus(raw[c * CHUNK:(c + 1) * CHUNK, :].T + bias_ref[...])
            la = dt * aneg_ref[...]
            ci = cumsum_lanes(la, lane)
            ce = ci - la
            end = jnp.broadcast_to(ci[:, CHUNK - 1:], ci.shape)
            dt_s[cc] = dt
            ci_s[cc] = ci
            ce_s[cc] = ce
            q = spread_operand([jnp.exp(end - ci) * dt, jnp.exp(ce) * dt, end], CHUNK)
            w = jnp.dot(q, e_s[:, :2 * inner], preferred_element_type=f32)
            le = jnp.dot(q[:16], e_s[:, 2 * inner:], preferred_element_type=f32)[:8]
            le_s[cc] = le
            u = u_s[pl.ds(at, CHUNK), :].astype(f32)
            b = bc_s[pl.ds(at, CHUNK), :n_state]
            dims = (((0,), (0,)), ((), ()))
            sf = lax.dot_general(b, (u * w[:, :inner]).astype(bf16), dims, preferred_element_type=f32)
            sb = lax.dot_general(b, (u * w[:, inner:]).astype(bf16), dims, preferred_element_type=f32)
            sf_s[cc] = sf
            sb_s[cc] = sb
            lt = lt_s[...]
            f_s[...] = f_s[...] * jnp.exp(le[:1]) + sf
            g_s[...] = g_s[...] + jnp.exp(lt[:1]) * sb
            lt_s[...] = lt + le

    @pl.when(i == n_blk - 1)
    def _():
        lt = lt_s[:1]
        parts = split3(lt)
        row = lax.broadcasted_iota(jnp.int32, (MSG_PAD, inner), 0)
        tail = jnp.where(row == 0, parts[0], jnp.where(row == 1, parts[1], jnp.where(row == 2, parts[2], 0.0))).astype(bf16)
        for side, ref in ((0, f_s), (1, g_s)):
            msg_s[side, :n_state, :] = ref[...].astype(bf16)
            msg_s[side, n_state:, :] = tail
        for s in range(1, n_seq):
            peer_copy(s).start()

    @pl.when(i == z_first)
    def _():
        wz_copy().wait()

    @pl.when((i >= z_first) & (i < y_first))
    def _():
        base = pl.multiple_of((i - z_first) * rows, rows)
        z_s[pl.ds(base, rows), :] = jnp.dot(x_ref[...], wz_s[...], preferred_element_type=f32).astype(bf16)

    @pl.when(i == z_first + n_blk // 2)
    def _():
        for k in range(4):
            weight_copy(k).wait()
        for k in range(4, 12):
            weight_copy(k).start()

    @pl.when(i == y_first)
    def _():
        for s in range(1, n_seq):
            peer_copy(s).wait()

        def log_of(s):
            t = rcv_s[s - 1, n_state:, :].astype(f32)
            return t[0:1] + t[1:2] + t[2:3]

        f_s[...] = jnp.zeros_like(f_s)
        g_s[...] = jnp.zeros_like(g_s)
        acc = jnp.zeros((1, inner), f32)
        for s in range(1, n_seq):
            wgt = jnp.where(s <= me, jnp.exp(acc), 0.0)
            f_s[...] += wgt * rcv_s[s - 1, :n_state, :].astype(f32)
            acc = acc + log_of(s)
        acc = jnp.zeros((1, inner), f32)
        for s in range(n_seq - 1, 0, -1):
            wgt = jnp.where(s > me, jnp.exp(acc), 0.0)
            g_s[...] += wgt * rcv_s[s - 1, :n_state, :].astype(f32)
            acc = acc + log_of(s)

        n_ch = n_blk * per_blk

        def back(t, _):
            c = n_ch - 1 - t
            mine = sb_s[c]
            g = g_s[...]
            sb_s[c] = g
            g_s[...] = g * jnp.exp(le_s[c][:1]) + mine
            return 0

        lax.fori_loop(0, n_ch, back, 0)

    @pl.when(i >= y_first)
    def _():
        blk = i - y_first
        base = pl.multiple_of(blk * rows, rows)
        trow = lax.broadcasted_iota(jnp.int32, (CHUNK, CHUNK), 0)
        tcol = lax.broadcasted_iota(jnp.int32, (CHUNK, CHUNK), 1)
        later = trow > tcol
        left = tcol < head_dim
        twice = jnp.where(trow == tcol, 2.0, 1.0)
        for c in range(per_blk):
            cc = blk * per_blk + c
            at = pl.multiple_of(base + c * CHUNK, CHUNK)
            dt, ci, ce = dt_s[cc], ci_s[cc], ce_s[cc]
            end = jnp.broadcast_to(ci[:, CHUNK - 1:], ci.shape)
            q = spread_operand([dt, jnp.exp(ci), jnp.exp(end - ce)], CHUNK)
            w = jnp.dot(q, e_s[...], preferred_element_type=f32)
            col = jnp.concatenate([ci, ce, jnp.zeros((CHUNK - 2 * heads, CHUNK), f32)], axis=0).T
            u = u_s[pl.ds(at, CHUNK), :].astype(f32)
            udt = (u * w[:, :inner]).astype(bf16)
            b = bc_s[pl.ds(at, CHUNK), :n_state]
            cm = bc_s[pl.ds(at, CHUNK), n_state:]
            gram = lax.dot_general(cm, b, (((1,), (1,)), ((), ())), preferred_element_type=f32) * twice
            f_in = f_s[...]
            y = jnp.dot(cm, f_in.astype(bf16), preferred_element_type=f32) * w[:, inner:2 * inner]
            y = y + jnp.dot(cm, sb_s[cc].astype(bf16), preferred_element_type=f32) * w[:, 2 * inner:]
            y = y + skip_ref[...] * u
            f_s[...] = f_in * jnp.exp(le_s[cc][:1]) + sf_s[cc]
            outs = []
            for p in range(heads // 2):
                mats = []
                for h in (2 * p, 2 * p + 1):
                    d = jnp.where(later, col[:, h:h + 1] - ci[h:h + 1, :], ce[h:h + 1, :] - col[:, heads + h:heads + h + 1])
                    mats.append((gram * jnp.exp(jnp.minimum(d, 0.0))).astype(bf16))
                up = udt[:, p * CHUNK:(p + 1) * CHUNK]
                zero = jnp.zeros_like(up)
                rhs = jnp.concatenate([jnp.where(left, up, zero), jnp.where(left, zero, up)], axis=0)
                outs.append(jnp.dot(jnp.concatenate(mats, axis=1), rhs, preferred_element_type=f32))
            y = y + jnp.concatenate(outs, axis=1)
            z = z_s[pl.ds(at, CHUNK), :].astype(f32)
            z_s[pl.ds(at, CHUNK), :] = (y * (z / (1.0 + jnp.exp(-z)))).astype(bf16)
        for c in range(per_blk):
            at = pl.multiple_of(base + c * CHUNK, CHUNK)
            side = c % 2
            owner = blk * (per_blk // 2) + c // 2
            far = (lax.rem(owner // RING - zy[0] + RING, RING), lax.rem(lax.rem(owner, RING) - zy[1] + RING, RING))
            dist, group = (far[1], far[0]) if side == 0 else (far[0], far[1])

            @pl.when(dist == 0)
            def _():
                own_copy(side, group, at).start()

            @pl.when(dist > 0)
            def _():
                gate_copy(side, dist, group, at).start()

    @pl.when(i == y_first + n_blk // 2)
    def _():
        for k in range(4, 8):
            weight_copy(k).wait()
        for k in range(12, 14):
            weight_copy(k).start()

    @pl.when(i == 3 * n_blk - 1)
    def _():
        for side in range(2):
            for group in range(RING):
                own_copy(side, group, 0).wait()
                for dist in range(1, RING):
                    gate_copy(side, dist, group, 0).wait()
        for k in range(8, 14):
            weight_copy(k).wait()


def scan_call(x_blk, w_z, w_x, w_bc, w_dt, a_neg, dt_bias, d_skip, w_out, n_seq):
    tokens, d_model = x_blk.shape
    heads = a_neg.shape[0]
    inner = w_x.shape[1]
    head_dim = inner // heads
    n_state = w_bc.shape[1] // 2
    rows = min(512, tokens)
    n_blk = tokens // rows
    n_ch = tokens // CHUNK
    w_dt = w_dt.T
    f32, bf16 = jnp.float32, jnp.bfloat16

    def whole(a):
        return pl.BlockSpec(a.shape, lambda i: (0, 0), pipeline_mode=pl.Buffered(1))

    return pl.pallas_call(
        functools.partial(scan_kernel, n_blk, n_seq, heads, head_dim),
        grid=(3 * n_blk,),
        out_shape=(jax.ShapeDtypeStruct((2, RING, tokens // (2 * RING), inner), bf16),
                   jax.ShapeDtypeStruct((2 * (RING - 1),) + w_out.shape, bf16)),
        in_specs=[pl.BlockSpec((rows, d_model), lambda i: (jnp.where(i < n_blk, i, jnp.minimum(i - n_blk, n_blk - 1)), 0)),
                  pl.BlockSpec(memory_space=pl.ANY)]
        + [whole(a) for a in (w_x, w_bc, w_dt)] + [pl.BlockSpec(memory_space=pltpu.SMEM)] * 3 + [pl.BlockSpec(memory_space=pl.ANY)],
        out_specs=(pl.BlockSpec(memory_space=pl.ANY), pl.BlockSpec(memory_space=pl.ANY)),
        scratch_shapes=[
            pltpu.VMEM((tokens, inner), bf16),
            pltpu.VMEM((tokens, inner), bf16),
            pltpu.VMEM((tokens, 2 * n_state), bf16),
            pltpu.VMEM((n_ch, n_state, inner), f32),
            pltpu.VMEM((n_ch, n_state, inner), f32),
            pltpu.VMEM((n_state, inner), f32),
            pltpu.VMEM((n_state, inner), f32),
            pltpu.VMEM((n_ch, heads, CHUNK), f32),
            pltpu.VMEM((n_ch, heads, CHUNK), f32),
            pltpu.VMEM((n_ch, heads, CHUNK), f32),
            pltpu.VMEM((n_ch, 8, inner), f32),
            pltpu.VMEM((8, inner), f32),
            pltpu.VMEM((CHUNK, 3 * inner), bf16),
            pltpu.VMEM((2, n_state + MSG_PAD, inner), bf16),
            pltpu.VMEM((n_seq - 1, n_state + MSG_PAD, inner), bf16),
            pltpu.VMEM((heads, CHUNK), f32),
            pltpu.VMEM((heads, CHUNK), f32),
            pltpu.VMEM((1, inner), f32),
            pltpu.VMEM(w_z.shape, bf16),
            pltpu.SemaphoreType.DMA,
            pltpu.SemaphoreType.DMA((n_seq - 1,)),
            pltpu.SemaphoreType.DMA((n_seq - 1,)),
            pltpu.SemaphoreType.DMA((14,)),
            pltpu.SemaphoreType.DMA((14,)),
            pltpu.SemaphoreType.DMA((2, RING, RING)),
            pltpu.SemaphoreType.DMA((2, RING, RING)),
            pltpu.SemaphoreType.DMA((2, RING)),
        ],
        compiler_params=pltpu.CompilerParams(collective_id=0, has_side_effects=True, vmem_limit_bytes=60 * 1024 * 1024,
                                             dimension_semantics=('arbitrary',)),
        cost_estimate=pl.CostEstimate(flops=2 * tokens * d_model * (2 * inner + 3 * n_state) * 3, bytes_accessed=60 << 20, transcendentals=0),
    )(x_blk, w_z, w_x, w_bc, w_dt, dt_bias, a_neg, d_skip, w_out)


def out_kernel(n_col, ga_ref, wo_ref, wg_ref, x_ref, out_ref, send_s, recv_s, own_s, x_s, x_sem, send_sem, recv_sem):
    i = pl.program_id(0)
    zy = tp_coords()
    width = wo_ref.shape[1]
    f32, bf16 = jnp.float32, jnp.bfloat16

    def part_copy(side, dist, b):
        return pltpu.make_async_remote_copy(
            src_ref=send_s.at[side, dist - 1, b], dst_ref=recv_s.at[side, dist - 1, b],
            send_sem=send_sem.at[side, dist - 1, b], recv_sem=recv_sem.at[side, dist - 1, b],
            device_id={'tp': ring_peer(zy, 1 - side, dist)}, device_id_type=pl.DeviceIdType.MESH)

    def x_copy():
        rows = x_s.shape[0]
        at = pl.multiple_of(lax.axis_index('tp') * rows, rows)
        return pltpu.make_async_copy(x_ref.at[pl.ds(at, rows), :], x_s, x_sem)

    @pl.when(i == 0)
    def _():
        x_copy().start()
        barrier = pltpu.get_barrier_semaphore()
        for axis in range(2):
            for dist in range(1, RING):
                pl.semaphore_signal(barrier, inc=1, device_id={'tp': ring_peer(zy, axis, dist)}, device_id_type=pl.DeviceIdType.MESH)

    @pl.when(i < n_col)
    def _():
        for side in range(2):
            acc = jnp.dot(ga_ref[side, 0], wo_ref[...], preferred_element_type=f32)
            for dist in range(1, RING):
                acc = acc + jnp.dot(ga_ref[side, dist], wg_ref[side * 3 + dist - 1], preferred_element_type=f32)
            own_s[side, i] = acc[:CHUNK]
            for dist in range(1, RING):
                send_s[side, dist - 1, i] = acc[dist * CHUNK:(dist + 1) * CHUNK].astype(bf16)

    @pl.when(i == 0)
    def _():
        pl.semaphore_wait(pltpu.get_barrier_semaphore(), 2 * (RING - 1))

    @pl.when(i < n_col)
    def _():
        for side in range(2):
            for dist in range(1, RING):
                part_copy(side, dist, i).start()

    @pl.when(i == n_col)
    def _():
        x_copy().wait()

    @pl.when(i >= n_col)
    def _():
        b = i - n_col
        cols = pl.ds(pl.multiple_of(b * width, width), width)
        for side in range(2):
            acc = own_s[side, b]
            for dist in range(1, RING):
                part_copy(side, dist, b).wait()
                acc = acc + recv_s[side, dist - 1, b].astype(f32)
            at = side * CHUNK
            out_ref[at:at + CHUNK, :] = (x_s[at:at + CHUNK, cols].astype(f32) + acc).astype(bf16)


def out_call(g_all, w_out, w_got, x_blk):
    inner, d_model = w_out.shape
    rows = 2 * CHUNK
    width = min(512, d_model)
    n_col = d_model // width
    f32, bf16 = jnp.float32, jnp.bfloat16

    def column(i):
        return jnp.minimum(i, n_col - 1)

    return pl.pallas_call(
        functools.partial(out_kernel, n_col),
        grid=(2 * n_col,),
        out_shape=jax.ShapeDtypeStruct((rows, d_model), bf16),
        in_specs=[pl.BlockSpec(g_all.shape, lambda i: (0, 0, 0, 0), pipeline_mode=pl.Buffered(1)),
                  pl.BlockSpec((inner, width), lambda i: (0, column(i))),
                  pl.BlockSpec((2 * (RING - 1), inner, width), lambda i: (0, 0, column(i))),
                  pl.BlockSpec(memory_space=pl.ANY)],
        out_specs=pl.BlockSpec((rows, width), lambda i: (0, jnp.maximum(i - n_col, 0))),
        scratch_shapes=[
            pltpu.VMEM((2, RING - 1, n_col, CHUNK, width), bf16),
            pltpu.VMEM((2, RING - 1, n_col, CHUNK, width), bf16),
            pltpu.VMEM((2, n_col, CHUNK, width), f32),
            pltpu.VMEM((rows, d_model), bf16),
            pltpu.SemaphoreType.DMA,
            pltpu.SemaphoreType.DMA((2, RING - 1, n_col)),
            pltpu.SemaphoreType.DMA((2, RING - 1, n_col)),
        ],
        compiler_params=pltpu.CompilerParams(collective_id=1, has_side_effects=True, vmem_limit_bytes=60 * 1024 * 1024,
                                             dimension_semantics=('arbitrary',)),
        cost_estimate=pl.CostEstimate(flops=2 * 2 * 4 * CHUNK * 4 * inner * d_model, bytes_accessed=40 << 20, transcendentals=0),
    )(g_all, w_out, w_got, x_blk)


def solution(mesh):
    n_seq = mesh.shape['sp']

    def device_fn(x_blk, w_z, w_x, w_bc, w_dt, a_neg, dt_bias, d_skip, w_out):
        g_all, w_got = scan_call(x_blk, w_z, w_x, w_bc, w_dt, a_neg, dt_bias, d_skip, w_out, n_seq)
        return out_call(g_all, w_out, w_got, x_blk)

    in_specs = (P(('dp', 'sp'), None), P(None, 'tp'), P(None, 'tp'), P(None, None), P(None, 'tp'), P('tp'), P('tp'), P('tp'), P('tp', None))
    out_specs = P(('dp', 'sp', 'tp'), None)
    return jax.shard_map(device_fn, mesh=mesh, in_specs=in_specs, out_specs=out_specs, check_vma=False)
```

```python
import functools

import jax
import jax.numpy as jnp
from jax import lax
from jax.experimental import pallas as pl
from jax.experimental.pallas import tpu as pltpu
from jax.sharding import PartitionSpec as P

CHUNK = 128
MSG_PAD = 16
RING = 4
SHARE = 16


def split3(v):
    hi = v.astype(jnp.bfloat16).astype(jnp.float32)
    rest = v - hi
    mid = rest.astype(jnp.bfloat16).astype(jnp.float32)
    return [hi, mid, rest - mid]


def spread_operand(quantities, width):
    rows = [part for q in quantities for part in split3(q)]
    have = sum(r.shape[0] for r in rows)
    rows.append(jnp.zeros((CHUNK - have, width), jnp.float32))
    return jnp.concatenate(rows, axis=0).T.astype(jnp.bfloat16)


def cumsum_lanes(v, lane):
    step = 1
    while step < v.shape[1]:
        v = v + jnp.where(lane >= step, pltpu.roll(v, step, 1), 0.0)
        step *= 2
    return v


def softplus(v):
    return jnp.maximum(v, 0.0) + jnp.log1p(jnp.exp(-jnp.abs(v)))


def tp_coords():
    index = lax.axis_index('tp')
    return index // RING, lax.rem(index, RING)


def ring_peer(zy, axis, dist):
    z, y = zy
    if axis == 0:
        return z * RING + lax.rem(y + dist, RING)
    return lax.rem(z + dist, RING) * RING + y


def scan_kernel(n_blk, n_seq, heads, head_dim, x_ref, wz_ref, wx_ref, wbc_ref, wdt_ref, bias_sm, aneg_sm, skip_sm, wo_ref, ga_ref, wg_ref,
                z_s, u_s, bc_s, sf_s, sb_s, f_s, g_s, dt_s, ci_s, ce_s, le_s, lt_s, e_s, msg_s, rcv_s, bias_ref, aneg_ref, skip_ref, wx_s, wbc_s, wz_s, load_sem, send_sem, recv_sem, ws_sem, wr_sem, gs_sem, gr_sem, own_sem):
    i = pl.program_id(0)
    me = lax.axis_index('sp')
    rows = x_ref.shape[0]
    inner = heads * head_dim
    per_blk = rows // CHUNK
    n_state = bc_s.shape[1] // 2
    f32, bf16 = jnp.float32, jnp.bfloat16
    lane = lax.broadcasted_iota(jnp.int32, (heads, CHUNK), 1)

    def peer_copy(s):
        dest = lax.rem(me + s, n_seq)
        side = jnp.where(me + s < n_seq, 0, 1)
        return pltpu.make_async_remote_copy(
            src_ref=msg_s.at[side], dst_ref=rcv_s.at[s - 1], send_sem=send_sem.at[s - 1], recv_sem=recv_sem.at[s - 1],
            device_id={'sp': dest}, device_id_type=pl.DeviceIdType.MESH)

    zy = tp_coords()
    z_first, y_first = n_blk, 2 * n_blk

    def load(k):
        src, dst = ((wx_ref, wx_s), (wbc_ref, wbc_s), (wz_ref, wz_s))[k]
        return pltpu.make_async_copy(src, dst, load_sem.at[k])

    n_chip = n_seq // 2
    chip, core = me // 2, lax.rem(me, 2)
    half = wo_ref.shape[0] // 2
    whole_rows = half - n_chip * SHARE

    def span(shared, everyone=False):
        at = core * half
        if not shared:
            return at, whole_rows
        if everyone:
            return at + whole_rows, n_chip * SHARE
        return at + whole_rows + chip * SHARE, SHARE

    def weight_copy(k, src, slot, at, size, dest):
        rows_at = pl.ds(pl.multiple_of(at, 8), size)
        return pltpu.make_async_remote_copy(
            src_ref=src.at[rows_at, :], dst_ref=wg_ref.at[slot, rows_at, :], send_sem=ws_sem.at[k], recv_sem=wr_sem.at[k],
            device_id=dest, device_id_type=pl.DeviceIdType.MESH)

    def ring_copies(hop):
        out = []
        for axis in range(2):
            for back in range(2):
                dist = RING - 1 if back else 1
                for shared in range(2):
                    at, size = span(shared)
                    k = ((hop * 2 + axis) * 2 + back) * 2 + shared
                    dest = {'tp': ring_peer(zy, axis, dist)}
                    if hop == 0:
                        out.append(weight_copy(k, wo_ref, axis * 3 + dist - 1, at, size, dest))
                    else:
                        out.append(weight_copy(k, wg_ref.at[axis * 3 + dist - 1], axis * 3 + 1, at + back * (size // 2), size // 2, dest))
        return out

    near, opposite = (0, 2, 3, 5), (1, 4)

    def along_x(slots):
        at, size = span(1)
        return [weight_copy(16 + slot * (n_chip - 1) + d - 1, wg_ref.at[slot], slot, at, size, {'sp': lax.rem(chip + d, n_chip) * 2 + core})
                for slot in slots for d in range(1, n_chip)]

    def to_partner(slots, shared):
        at, size = span(shared, everyone=True)
        first = 16 + 6 * (n_chip - 1)
        return [weight_copy(first + slot * 2 + shared, wg_ref.at[slot], slot, at, size, {'sp': chip * 2 + 1 - core}) for slot in slots]

    def start(copies):
        for c in copies:
            c.start()

    def wait(copies):
        for c in copies:
            c.wait()

    def gate_copy(side, dist, group, at):
        return pltpu.make_async_remote_copy(
            src_ref=z_s.at[pl.ds(at, CHUNK), :], dst_ref=ga_ref.at[side, dist, pl.ds(pl.multiple_of(group * CHUNK, CHUNK), CHUNK), :],
            send_sem=gs_sem.at[side, dist, group], recv_sem=gr_sem.at[side, dist, group],
            device_id={'tp': ring_peer(zy, side, dist)}, device_id_type=pl.DeviceIdType.MESH)

    def own_copy(side, group, at):
        return pltpu.make_async_copy(z_s.at[pl.ds(at, CHUNK), :], ga_ref.at[side, 0, pl.ds(pl.multiple_of(group * CHUNK, CHUNK), CHUNK), :],
                                     own_sem.at[side, group])

    @pl.when(i == 0)
    def _():
        barrier = pltpu.get_barrier_semaphore()
        for k in range(3):
            load(k).start()
        for s in range(1, n_seq):
            pl.semaphore_signal(barrier, inc=1, device_id={'sp': lax.rem(me + s, n_seq)}, device_id_type=pl.DeviceIdType.MESH)
        for axis in range(2):
            for dist in range(1, RING):
                pl.semaphore_signal(barrier, inc=1, device_id={'tp': ring_peer(zy, axis, dist)}, device_id_type=pl.DeviceIdType.MESH)
        pl.semaphore_wait(barrier, n_seq - 1 + 2 * (RING - 1))
        start(ring_copies(0))
        head = lax.broadcasted_iota(jnp.int32, bias_ref.shape, 0)
        owner = lax.broadcasted_iota(jnp.int32, skip_ref.shape, 1) // head_dim
        bias, aneg, skip = jnp.zeros_like(bias_ref), jnp.zeros_like(aneg_ref), jnp.zeros_like(skip_ref)
        for h in range(heads):
            bias = jnp.where(head == h, bias_sm[h], bias)
            aneg = jnp.where(head == h, aneg_sm[h], aneg)
            skip = jnp.where(owner == h, 2.0 * skip_sm[h], skip)
        bias_ref[...] = bias
        aneg_ref[...] = aneg
        skip_ref[...] = skip
        k = lax.broadcasted_iota(jnp.int32, e_s.shape, 0)
        j = lax.broadcasted_iota(jnp.int32, e_s.shape, 1)
        hit = (k // (3 * heads) == j // inner) & (k % heads == (j % inner) // head_dim)
        e_s[...] = jnp.where(hit, 1.0, 0.0).astype(bf16)
        f_s[...] = jnp.zeros_like(f_s)
        g_s[...] = jnp.zeros_like(g_s)
        lt_s[...] = jnp.zeros_like(lt_s)
        load(0).wait()
        load(1).wait()

    @pl.when(i < n_blk)
    def _():
        base = pl.multiple_of(i * rows, rows)
        xb = x_ref[...]
        raw = lax.dot_general(xb, wdt_ref[...], (((1,), (1,)), ((), ())), preferred_element_type=f32)
        bc_s[pl.ds(base, rows), :] = jnp.dot(xb, wbc_s[...], preferred_element_type=f32).astype(bf16)
        u_s[pl.ds(base, rows), :] = jnp.dot(xb, wx_s[...], preferred_element_type=f32).astype(bf16)
        for c in range(per_blk):
            cc = i * per_blk + c
            at = pl.multiple_of(base + c * CHUNK, CHUNK)
            dt = softplus(raw[c * CHUNK:(c + 1) * CHUNK, :].T + bias_ref[...])
            la = dt * aneg_ref[...]
            ci = cumsum_lanes(la, lane)
            ce = ci - la
            end = jnp.broadcast_to(ci[:, CHUNK - 1:], ci.shape)
            dt_s[cc] = dt
            ci_s[cc] = ci
            ce_s[cc] = ce
            q = spread_operand([jnp.exp(end - ci) * dt, jnp.exp(ce) * dt, end], CHUNK)
            w = jnp.dot(q, e_s[:, :2 * inner], preferred_element_type=f32)
            le = jnp.dot(q[:16], e_s[:, 2 * inner:], preferred_element_type=f32)[:8]
            le_s[cc] = le
            u = u_s[pl.ds(at, CHUNK), :].astype(f32)
            b = bc_s[pl.ds(at, CHUNK), :n_state]
            dims = (((0,), (0,)), ((), ()))
            sf = lax.dot_general(b, (u * w[:, :inner]).astype(bf16), dims, preferred_element_type=f32)
            sb = lax.dot_general(b, (u * w[:, inner:]).astype(bf16), dims, preferred_element_type=f32)
            sf_s[cc] = sf
            sb_s[cc] = sb
            lt = lt_s[...]
            f_s[...] = f_s[...] * jnp.exp(le[:1]) + sf
            g_s[...] = g_s[...] + jnp.exp(lt[:1]) * sb
            lt_s[...] = lt + le

    @pl.when(i == n_blk - 1)
    def _():
        lt = lt_s[:1]
        parts = split3(lt)
        row = lax.broadcasted_iota(jnp.int32, (MSG_PAD, inner), 0)
        tail = jnp.where(row == 0, parts[0], jnp.where(row == 1, parts[1], jnp.where(row == 2, parts[2], 0.0))).astype(bf16)
        for side, ref in ((0, f_s), (1, g_s)):
            msg_s[side, :n_state, :] = ref[...].astype(bf16)
            msg_s[side, n_state:, :] = tail
        for s in range(1, n_seq):
            peer_copy(s).start()

    @pl.when(i == z_first)
    def _():
        load(2).wait()

    @pl.when((i >= z_first) & (i < y_first))
    def _():
        base = pl.multiple_of((i - z_first) * rows, rows)
        z_s[pl.ds(base, rows), :] = jnp.dot(x_ref[...], wz_s[...], preferred_element_type=f32).astype(bf16)

    @pl.when(i == z_first + n_blk // 4)
    def _():
        wait(ring_copies(0))
        start(ring_copies(1) + along_x(near) + to_partner(near, 0))

    @pl.when(i == y_first)
    def _():
        for s in range(1, n_seq):
            peer_copy(s).wait()

        def log_of(s):
            t = rcv_s[s - 1, n_state:, :].astype(f32)
            return t[0:1] + t[1:2] + t[2:3]

        f_s[...] = jnp.zeros_like(f_s)
        g_s[...] = jnp.zeros_like(g_s)
        acc = jnp.zeros((1, inner), f32)
        for s in range(1, n_seq):
            wgt = jnp.where(s <= me, jnp.exp(acc), 0.0)
            f_s[...] += wgt * rcv_s[s - 1, :n_state, :].astype(f32)
            acc = acc + log_of(s)
        acc = jnp.zeros((1, inner), f32)
        for s in range(n_seq - 1, 0, -1):
            wgt = jnp.where(s > me, jnp.exp(acc), 0.0)
            g_s[...] += wgt * rcv_s[s - 1, :n_state, :].astype(f32)
            acc = acc + log_of(s)

        n_ch = n_blk * per_blk

        def back(t, _):
            c = n_ch - 1 - t
            mine = sb_s[c]
            g = g_s[...]
            sb_s[c] = g
            g_s[...] = g * jnp.exp(le_s[c][:1]) + mine
            return 0

        lax.fori_loop(0, n_ch, back, 0)

    @pl.when(i >= y_first)
    def _():
        blk = i - y_first
        base = pl.multiple_of(blk * rows, rows)
        trow = lax.broadcasted_iota(jnp.int32, (CHUNK, CHUNK), 0)
        tcol = lax.broadcasted_iota(jnp.int32, (CHUNK, CHUNK), 1)
        later = trow > tcol
        left = tcol < head_dim
        twice = jnp.where(trow == tcol, 2.0, 1.0)
        for c in range(per_blk):
            cc = blk * per_blk + c
            at = pl.multiple_of(base + c * CHUNK, CHUNK)
            dt, ci, ce = dt_s[cc], ci_s[cc], ce_s[cc]
            end = jnp.broadcast_to(ci[:, CHUNK - 1:], ci.shape)
            q = spread_operand([dt, jnp.exp(ci), jnp.exp(end - ce)], CHUNK)
            w = jnp.dot(q, e_s[...], preferred_element_type=f32)
            col = jnp.concatenate([ci, ce, jnp.zeros((CHUNK - 2 * heads, CHUNK), f32)], axis=0).T
            u = u_s[pl.ds(at, CHUNK), :].astype(f32)
            udt = (u * w[:, :inner]).astype(bf16)
            b = bc_s[pl.ds(at, CHUNK), :n_state]
            cm = bc_s[pl.ds(at, CHUNK), n_state:]
            gram = lax.dot_general(cm, b, (((1,), (1,)), ((), ())), preferred_element_type=f32) * twice
            f_in = f_s[...]
            y = jnp.dot(cm, f_in.astype(bf16), preferred_element_type=f32) * w[:, inner:2 * inner]
            y = y + jnp.dot(cm, sb_s[cc].astype(bf16), preferred_element_type=f32) * w[:, 2 * inner:]
            y = y + skip_ref[...] * u
            f_s[...] = f_in * jnp.exp(le_s[cc][:1]) + sf_s[cc]
            outs = []
            for p in range(heads // 2):
                mats = []
                for h in (2 * p, 2 * p + 1):
                    d = jnp.where(later, col[:, h:h + 1] - ci[h:h + 1, :], ce[h:h + 1, :] - col[:, heads + h:heads + h + 1])
                    mats.append((gram * jnp.exp(jnp.minimum(d, 0.0))).astype(bf16))
                up = udt[:, p * CHUNK:(p + 1) * CHUNK]
                zero = jnp.zeros_like(up)
                rhs = jnp.concatenate([jnp.where(left, up, zero), jnp.where(left, zero, up)], axis=0)
                outs.append(jnp.dot(jnp.concatenate(mats, axis=1), rhs, preferred_element_type=f32))
            y = y + jnp.concatenate(outs, axis=1)
            z = z_s[pl.ds(at, CHUNK), :].astype(f32)
            z_s[pl.ds(at, CHUNK), :] = (y * (z / (1.0 + jnp.exp(-z)))).astype(bf16)
        for c in range(per_blk):
            at = pl.multiple_of(base + c * CHUNK, CHUNK)
            side = c % 2
            owner = blk * (per_blk // 2) + c // 2
            far = (lax.rem(owner // RING - zy[0] + RING, RING), lax.rem(lax.rem(owner, RING) - zy[1] + RING, RING))
            dist, group = (far[1], far[0]) if side == 0 else (far[0], far[1])

            @pl.when(dist == 0)
            def _():
                own_copy(side, group, at).start()

            @pl.when(dist > 0)
            def _():
                gate_copy(side, dist, group, at).start()

    @pl.when(i == y_first + n_blk // 4)
    def _():
        wait(ring_copies(1))
        start(along_x(opposite) + to_partner(opposite, 0))

    @pl.when(i == y_first + 3 * n_blk // 4)
    def _():
        wait(along_x(near))
        start(to_partner(near, 1))

    @pl.when(i == 3 * n_blk - 1)
    def _():
        wait(along_x(opposite))
        start(to_partner(opposite, 1))
        for side in range(2):
            for group in range(RING):
                own_copy(side, group, 0).wait()
                for dist in range(1, RING):
                    gate_copy(side, dist, group, 0).wait()
        wait(to_partner(near + opposite, 0) + to_partner(near + opposite, 1))


def scan_call(x_blk, w_z, w_x, w_bc, w_dt, a_neg, dt_bias, d_skip, w_out, n_seq):
    tokens, d_model = x_blk.shape
    heads = a_neg.shape[0]
    inner = w_x.shape[1]
    head_dim = inner // heads
    n_state = w_bc.shape[1] // 2
    rows = min(512, tokens)
    n_blk = tokens // rows
    n_ch = tokens // CHUNK
    n_copies = 16 + 6 * (n_seq // 2 - 1) + 12
    w_dt = w_dt.T
    f32, bf16 = jnp.float32, jnp.bfloat16

    def whole(a):
        return pl.BlockSpec(a.shape, lambda i: (0, 0), pipeline_mode=pl.Buffered(1))

    return pl.pallas_call(
        functools.partial(scan_kernel, n_blk, n_seq, heads, head_dim),
        grid=(3 * n_blk,),
        out_shape=(jax.ShapeDtypeStruct((2, RING, tokens // (2 * RING), inner), bf16),
                   jax.ShapeDtypeStruct((2 * (RING - 1),) + w_out.shape, bf16)),
        in_specs=[pl.BlockSpec((rows, d_model), lambda i: (jnp.where(i < n_blk, i, jnp.minimum(i - n_blk, n_blk - 1)), 0)),
                  pl.BlockSpec(memory_space=pl.ANY), pl.BlockSpec(memory_space=pl.ANY), pl.BlockSpec(memory_space=pl.ANY), whole(w_dt)]
        + [pl.BlockSpec(memory_space=pltpu.SMEM)] * 3 + [pl.BlockSpec(memory_space=pl.ANY)],
        out_specs=(pl.BlockSpec(memory_space=pl.ANY), pl.BlockSpec(memory_space=pl.ANY)),
        scratch_shapes=[
            pltpu.VMEM((tokens, inner), bf16),
            pltpu.VMEM((tokens, inner), bf16),
            pltpu.VMEM((tokens, 2 * n_state), bf16),
            pltpu.VMEM((n_ch, n_state, inner), f32),
            pltpu.VMEM((n_ch, n_state, inner), f32),
            pltpu.VMEM((n_state, inner), f32),
            pltpu.VMEM((n_state, inner), f32),
            pltpu.VMEM((n_ch, heads, CHUNK), f32),
            pltpu.VMEM((n_ch, heads, CHUNK), f32),
            pltpu.VMEM((n_ch, heads, CHUNK), f32),
            pltpu.VMEM((n_ch, 8, inner), f32),
            pltpu.VMEM((8, inner), f32),
            pltpu.VMEM((CHUNK, 3 * inner), bf16),
            pltpu.VMEM((2, n_state + MSG_PAD, inner), bf16),
            pltpu.VMEM((n_seq - 1, n_state + MSG_PAD, inner), bf16),
            pltpu.VMEM((heads, CHUNK), f32),
            pltpu.VMEM((heads, CHUNK), f32),
            pltpu.VMEM((1, inner), f32),
            pltpu.VMEM(w_x.shape, bf16),
            pltpu.VMEM(w_bc.shape, bf16),
            pltpu.VMEM(w_z.shape, bf16),
            pltpu.SemaphoreType.DMA((3,)),
            pltpu.SemaphoreType.DMA((n_seq - 1,)),
            pltpu.SemaphoreType.DMA((n_seq - 1,)),
            pltpu.SemaphoreType.DMA((n_copies,)),
            pltpu.SemaphoreType.DMA((n_copies,)),
            pltpu.SemaphoreType.DMA((2, RING, RING)),
            pltpu.SemaphoreType.DMA((2, RING, RING)),
            pltpu.SemaphoreType.DMA((2, RING)),
        ],
        compiler_params=pltpu.CompilerParams(collective_id=0, has_side_effects=True, vmem_limit_bytes=60 * 1024 * 1024,
                                             dimension_semantics=('arbitrary',)),
        cost_estimate=pl.CostEstimate(flops=2 * tokens * d_model * (2 * inner + 3 * n_state) * 3, bytes_accessed=60 << 20, transcendentals=0),
    )(x_blk, w_z, w_x, w_bc, w_dt, dt_bias, a_neg, d_skip, w_out)


def out_kernel(n_col, ga_ref, wo_ref, wg_ref, x_ref, out_ref, send_s, recv_s, own_s, x_s, x_sem, send_sem, recv_sem):
    i = pl.program_id(0)
    zy = tp_coords()
    width = wo_ref.shape[1]
    f32, bf16 = jnp.float32, jnp.bfloat16

    def part_copy(side, dist, b):
        return pltpu.make_async_remote_copy(
            src_ref=send_s.at[side, dist - 1, b], dst_ref=recv_s.at[side, dist - 1, b],
            send_sem=send_sem.at[side, dist - 1, b], recv_sem=recv_sem.at[side, dist - 1, b],
            device_id={'tp': ring_peer(zy, 1 - side, dist)}, device_id_type=pl.DeviceIdType.MESH)

    def x_copy():
        rows = x_s.shape[0]
        at = pl.multiple_of(lax.axis_index('tp') * rows, rows)
        return pltpu.make_async_copy(x_ref.at[pl.ds(at, rows), :], x_s, x_sem)

    @pl.when(i == 0)
    def _():
        x_copy().start()
        barrier = pltpu.get_barrier_semaphore()
        for axis in range(2):
            for dist in range(1, RING):
                pl.semaphore_signal(barrier, inc=1, device_id={'tp': ring_peer(zy, axis, dist)}, device_id_type=pl.DeviceIdType.MESH)

    @pl.when(i < n_col)
    def _():
        for side in range(2):
            acc = jnp.dot(ga_ref[side, 0], wo_ref[...], preferred_element_type=f32)
            for dist in range(1, RING):
                acc = acc + jnp.dot(ga_ref[side, dist], wg_ref[side * 3 + dist - 1], preferred_element_type=f32)
            own_s[side, i] = acc[:CHUNK]
            for dist in range(1, RING):
                send_s[side, dist - 1, i] = acc[dist * CHUNK:(dist + 1) * CHUNK].astype(bf16)

    @pl.when(i == 0)
    def _():
        pl.semaphore_wait(pltpu.get_barrier_semaphore(), 2 * (RING - 1))

    @pl.when(i < n_col)
    def _():
        for side in range(2):
            for dist in range(1, RING):
                part_copy(side, dist, i).start()

    @pl.when(i == n_col)
    def _():
        x_copy().wait()

    @pl.when(i >= n_col)
    def _():
        b = i - n_col
        cols = pl.ds(pl.multiple_of(b * width, width), width)
        for side in range(2):
            acc = own_s[side, b]
            for dist in range(1, RING):
                part_copy(side, dist, b).wait()
                acc = acc + recv_s[side, dist - 1, b].astype(f32)
            at = side * CHUNK
            out_ref[at:at + CHUNK, :] = (x_s[at:at + CHUNK, cols].astype(f32) + acc).astype(bf16)


def out_call(g_all, w_out, w_got, x_blk):
    inner, d_model = w_out.shape
    rows = 2 * CHUNK
    width = min(512, d_model)
    n_col = d_model // width
    f32, bf16 = jnp.float32, jnp.bfloat16

    def column(i):
        return jnp.minimum(i, n_col - 1)

    return pl.pallas_call(
        functools.partial(out_kernel, n_col),
        grid=(2 * n_col,),
        out_shape=jax.ShapeDtypeStruct((rows, d_model), bf16),
        in_specs=[pl.BlockSpec(g_all.shape, lambda i: (0, 0, 0, 0), pipeline_mode=pl.Buffered(1)),
                  pl.BlockSpec((inner, width), lambda i: (0, column(i))),
                  pl.BlockSpec((2 * (RING - 1), inner, width), lambda i: (0, 0, column(i))),
                  pl.BlockSpec(memory_space=pl.ANY)],
        out_specs=pl.BlockSpec((rows, width), lambda i: (0, jnp.maximum(i - n_col, 0))),
        scratch_shapes=[
            pltpu.VMEM((2, RING - 1, n_col, CHUNK, width), bf16),
            pltpu.VMEM((2, RING - 1, n_col, CHUNK, width), bf16),
            pltpu.VMEM((2, n_col, CHUNK, width), f32),
            pltpu.VMEM((rows, d_model), bf16),
            pltpu.SemaphoreType.DMA,
            pltpu.SemaphoreType.DMA((2, RING - 1, n_col)),
            pltpu.SemaphoreType.DMA((2, RING - 1, n_col)),
        ],
        compiler_params=pltpu.CompilerParams(collective_id=1, has_side_effects=True, vmem_limit_bytes=60 * 1024 * 1024,
                                             dimension_semantics=('arbitrary',)),
        cost_estimate=pl.CostEstimate(flops=2 * 2 * 4 * CHUNK * 4 * inner * d_model, bytes_accessed=40 << 20, transcendentals=0),
    )(g_all, w_out, w_got, x_blk)


def solution(mesh):
    n_seq = mesh.shape['sp']

    def device_fn(x_blk, w_z, w_x, w_bc, w_dt, a_neg, dt_bias, d_skip, w_out):
        g_all, w_got = scan_call(x_blk, w_z, w_x, w_bc, w_dt, a_neg, dt_bias, d_skip, w_out, n_seq)
        return out_call(g_all, w_out, w_got, x_blk)

    in_specs = (P(('dp', 'sp'), None), P(None, 'tp'), P(None, 'tp'), P(None, None), P(None, 'tp'), P('tp'), P('tp'), P('tp'), P('tp', None))
    out_specs = P(('dp', 'sp', 'tp'), None)
    return jax.shard_map(device_fn, mesh=mesh, in_specs=in_specs, out_specs=out_specs, check_vma=False)
```

```python
import functools

import jax
import jax.numpy as jnp
from jax import lax
from jax.experimental import pallas as pl
from jax.experimental.pallas import tpu as pltpu
from jax.sharding import PartitionSpec as P

CHUNK = 128
MSG_PAD = 16
RING = 4
SHARE = 16


def split3(v):
    hi = v.astype(jnp.bfloat16).astype(jnp.float32)
    rest = v - hi
    mid = rest.astype(jnp.bfloat16).astype(jnp.float32)
    return [hi, mid, rest - mid]


def spread_operand(quantities, width):
    rows = [part for q in quantities for part in split3(q)]
    have = sum(r.shape[0] for r in rows)
    rows.append(jnp.zeros((CHUNK - have, width), jnp.float32))
    return jnp.concatenate(rows, axis=0).T.astype(jnp.bfloat16)


def cumsum_lanes(v, lane):
    step = 1
    while step < v.shape[1]:
        v = v + jnp.where(lane >= step, pltpu.roll(v, step, 1), 0.0)
        step *= 2
    return v


def softplus(v):
    return jnp.maximum(v, 0.0) + jnp.log1p(jnp.exp(-jnp.abs(v)))


def tp_coords():
    index = lax.axis_index('tp')
    return index // RING, lax.rem(index, RING)


def ring_peer(zy, axis, dist):
    z, y = zy
    if axis == 0:
        return z * RING + lax.rem(y + dist, RING)
    return lax.rem(z + dist, RING) * RING + y


def scan_kernel(n_blk, n_seq, heads, head_dim, x_ref, wz_ref, wx_ref, wbc_ref, wdt_ref, bias_sm, aneg_sm, skip_sm, wo_ref, ga_ref, wg_ref,
                z_s, u_s, bc_s, sf_s, sb_s, f_s, g_s, dt_s, ci_s, ce_s, le_s, lt_s, e_s, msg_s, rcv_s, bias_ref, aneg_ref, skip_ref, wx_s, wbc_s, wz_s, load_sem, send_sem, recv_sem, ws_sem, wr_sem, gs_sem, gr_sem, own_sem):
    i = pl.program_id(0)
    me = lax.axis_index('sp')
    rows = x_ref.shape[0]
    inner = heads * head_dim
    per_blk = rows // CHUNK
    n_state = bc_s.shape[1] // 2
    f32, bf16 = jnp.float32, jnp.bfloat16
    lane = lax.broadcasted_iota(jnp.int32, (heads, CHUNK), 1)

    def peer_copy(s):
        dest = lax.rem(me + s, n_seq)
        side = jnp.where(me + s < n_seq, 0, 1)
        return pltpu.make_async_remote_copy(
            src_ref=msg_s.at[side], dst_ref=rcv_s.at[s - 1], send_sem=send_sem.at[s - 1], recv_sem=recv_sem.at[s - 1],
            device_id={'sp': dest}, device_id_type=pl.DeviceIdType.MESH)

    zy = tp_coords()
    z_first, y_first = n_blk, 2 * n_blk

    def load(k):
        src, dst = ((wx_ref, wx_s), (wbc_ref, wbc_s), (wz_ref, wz_s))[k]
        return pltpu.make_async_copy(src, dst, load_sem.at[k])

    n_chip = n_seq // 2
    chip, core = me // 2, lax.rem(me, 2)
    half = wo_ref.shape[0] // 2
    whole_rows = half - n_chip * SHARE

    def span(shared, everyone=False):
        at = core * half
        if not shared:
            return at, whole_rows
        if everyone:
            return at + whole_rows, n_chip * SHARE
        return at + whole_rows + chip * SHARE, SHARE

    def weight_copy(k, src, slot, at, size, dest):
        rows_at = pl.ds(pl.multiple_of(at, 8), size)
        return pltpu.make_async_remote_copy(
            src_ref=src.at[rows_at, :], dst_ref=wg_ref.at[slot, rows_at, :], send_sem=ws_sem.at[k], recv_sem=wr_sem.at[k],
            device_id=dest, device_id_type=pl.DeviceIdType.MESH)

    def ring_copies(hop):
        out = []
        for axis in range(2):
            for back in range(2):
                dist = RING - 1 if back else 1
                for shared in range(2):
                    at, size = span(shared)
                    k = ((hop * 2 + axis) * 2 + back) * 2 + shared
                    dest = {'tp': ring_peer(zy, axis, dist)}
                    if hop == 0:
                        out.append(weight_copy(k, wo_ref, axis * 3 + dist - 1, at, size, dest))
                    else:
                        out.append(weight_copy(k, wg_ref.at[axis * 3 + dist - 1], axis * 3 + 1, at + back * (size // 2), size // 2, dest))
        return out

    near, opposite = (0, 2, 3, 5), (1, 4)

    def along_x(slots):
        at, size = span(1)
        return [weight_copy(16 + slot * (n_chip - 1) + d - 1, wg_ref.at[slot], slot, at, size, {'sp': lax.rem(chip + d, n_chip) * 2 + core})
                for slot in slots for d in range(1, n_chip)]

    def to_partner(slots, shared):
        at, size = span(shared, everyone=True)
        first = 16 + 6 * (n_chip - 1)
        return [weight_copy(first + slot * 2 + shared, wg_ref.at[slot], slot, at, size, {'sp': chip * 2 + 1 - core}) for slot in slots]

    def start(copies):
        for c in copies:
            c.start()

    def wait(copies):
        for c in copies:
            c.wait()

    def gate_copy(side, dist, group, at):
        return pltpu.make_async_remote_copy(
            src_ref=z_s.at[pl.ds(at, CHUNK), :], dst_ref=ga_ref.at[side, dist, pl.ds(pl.multiple_of(group * CHUNK, CHUNK), CHUNK), :],
            send_sem=gs_sem.at[side, dist, group], recv_sem=gr_sem.at[side, dist, group],
            device_id={'tp': ring_peer(zy, side, dist)}, device_id_type=pl.DeviceIdType.MESH)

    def own_copy(side, group, at):
        return pltpu.make_async_copy(z_s.at[pl.ds(at, CHUNK), :], ga_ref.at[side, 0, pl.ds(pl.multiple_of(group * CHUNK, CHUNK), CHUNK), :],
                                     own_sem.at[side, group])

    @pl.when(i == 0)
    def _():
        barrier = pltpu.get_barrier_semaphore()
        for k in range(3):
            load(k).start()
        for s in range(1, n_seq):
            pl.semaphore_signal(barrier, inc=1, device_id={'sp': lax.rem(me + s, n_seq)}, device_id_type=pl.DeviceIdType.MESH)
        for axis in range(2):
            for dist in range(1, RING):
                pl.semaphore_signal(barrier, inc=1, device_id={'tp': ring_peer(zy, axis, dist)}, device_id_type=pl.DeviceIdType.MESH)
        pl.semaphore_wait(barrier, n_seq - 1 + 2 * (RING - 1))
        start(ring_copies(0))
        head = lax.broadcasted_iota(jnp.int32, bias_ref.shape, 0)
        owner = lax.broadcasted_iota(jnp.int32, skip_ref.shape, 1) // head_dim
        bias, aneg, skip = jnp.zeros_like(bias_ref), jnp.zeros_like(aneg_ref), jnp.zeros_like(skip_ref)
        for h in range(heads):
            bias = jnp.where(head == h, bias_sm[h], bias)
            aneg = jnp.where(head == h, aneg_sm[h], aneg)
            skip = jnp.where(owner == h, 2.0 * skip_sm[h], skip)
        bias_ref[...] = bias
        aneg_ref[...] = aneg
        skip_ref[...] = skip
        k = lax.broadcasted_iota(jnp.int32, e_s.shape, 0)
        j = lax.broadcasted_iota(jnp.int32, e_s.shape, 1)
        hit = (k // (3 * heads) == j // inner) & (k % heads == (j % inner) // head_dim)
        e_s[...] = jnp.where(hit, 1.0, 0.0).astype(bf16)
        f_s[...] = jnp.zeros_like(f_s)
        g_s[...] = jnp.zeros_like(g_s)
        lt_s[...] = jnp.zeros_like(lt_s)
        load(0).wait()
        load(1).wait()

    @pl.when(i < n_blk)
    def _():
        base = pl.multiple_of(i * rows, rows)
        xb = x_ref[...]
        raw = lax.dot_general(xb, wdt_ref[...], (((1,), (1,)), ((), ())), preferred_element_type=f32)
        bc_s[pl.ds(base, rows), :] = jnp.dot(xb, wbc_s[...], preferred_element_type=f32).astype(bf16)
        u_s[pl.ds(base, rows), :] = jnp.dot(xb, wx_s[...], preferred_element_type=f32).astype(bf16)
        for c in range(per_blk):
            cc = i * per_blk + c
            at = pl.multiple_of(base + c * CHUNK, CHUNK)
            dt = softplus(raw[c * CHUNK:(c + 1) * CHUNK, :].T + bias_ref[...])
            la = dt * aneg_ref[...]
            ci = cumsum_lanes(la, lane)
            ce = ci - la
            end = jnp.broadcast_to(ci[:, CHUNK - 1:], ci.shape)
            dt_s[cc] = dt
            ci_s[cc] = ci
            ce_s[cc] = ce
            q = spread_operand([jnp.exp(end - ci) * dt, jnp.exp(ce) * dt, end], CHUNK)
            w = jnp.dot(q, e_s[:, :2 * inner], preferred_element_type=f32)
            le = jnp.dot(q[:16], e_s[:, 2 * inner:], preferred_element_type=f32)[:8]
            le_s[cc] = le
            u = u_s[pl.ds(at, CHUNK), :].astype(f32)
            b = bc_s[pl.ds(at, CHUNK), :n_state]
            dims = (((0,), (0,)), ((), ()))
            sf = lax.dot_general(b, (u * w[:, :inner]).astype(bf16), dims, preferred_element_type=f32)
            sb = lax.dot_general(b, (u * w[:, inner:]).astype(bf16), dims, preferred_element_type=f32)
            sf_s[cc] = sf
            sb_s[cc] = sb
            lt = lt_s[...]
            f_s[...] = f_s[...] * jnp.exp(le[:1]) + sf
            g_s[...] = g_s[...] + jnp.exp(lt[:1]) * sb
            lt_s[...] = lt + le

    @pl.when(i == n_blk - 1)
    def _():
        lt = lt_s[:1]
        parts = split3(lt)
        row = lax.broadcasted_iota(jnp.int32, (MSG_PAD, inner), 0)
        tail = jnp.where(row == 0, parts[0], jnp.where(row == 1, parts[1], jnp.where(row == 2, parts[2], 0.0))).astype(bf16)
        for side, ref in ((0, f_s), (1, g_s)):
            msg_s[side, :n_state, :] = ref[...].astype(bf16)
            msg_s[side, n_state:, :] = tail
        for s in range(1, n_seq):
            peer_copy(s).start()

    @pl.when(i == z_first)
    def _():
        load(2).wait()

    @pl.when((i >= z_first) & (i < y_first))
    def _():
        base = pl.multiple_of((i - z_first) * rows, rows)
        z_s[pl.ds(base, rows), :] = jnp.dot(x_ref[...], wz_s[...], preferred_element_type=f32).astype(bf16)

    @pl.when(i == z_first + n_blk // 4)
    def _():
        wait(ring_copies(0))
        start(ring_copies(1) + along_x(near) + to_partner(near, 0))

    @pl.when(i == y_first)
    def _():
        for s in range(1, n_seq):
            peer_copy(s).wait()

        def log_of(s):
            t = rcv_s[s - 1, n_state:, :].astype(f32)
            return t[0:1] + t[1:2] + t[2:3]

        f_s[...] = jnp.zeros_like(f_s)
        g_s[...] = jnp.zeros_like(g_s)
        acc = jnp.zeros((1, inner), f32)
        for s in range(1, n_seq):
            wgt = jnp.where(s <= me, jnp.exp(acc), 0.0)
            f_s[...] += wgt * rcv_s[s - 1, :n_state, :].astype(f32)
            acc = acc + log_of(s)
        acc = jnp.zeros((1, inner), f32)
        for s in range(n_seq - 1, 0, -1):
            wgt = jnp.where(s > me, jnp.exp(acc), 0.0)
            g_s[...] += wgt * rcv_s[s - 1, :n_state, :].astype(f32)
            acc = acc + log_of(s)

        n_ch = n_blk * per_blk

        def sweep(t, _):
            for ref, state, c in ((sf_s, f_s, t), (sb_s, g_s, n_ch - 1 - t)):
                mine = ref[c]
                before = state[...]
                ref[c] = before
                state[...] = before * jnp.exp(le_s[c][:1]) + mine
            return 0

        lax.fori_loop(0, n_ch, sweep, 0)

    @pl.when(i >= y_first)
    def _():
        step = i - y_first
        blk = 2 * lax.rem(zy[0] + 1 + step // 2, RING) + lax.rem(step + 1 - zy[1] // 2, 2)
        base = pl.multiple_of(blk * rows, rows)
        trow = lax.broadcasted_iota(jnp.int32, (CHUNK, CHUNK), 0)
        tcol = lax.broadcasted_iota(jnp.int32, (CHUNK, CHUNK), 1)
        later = trow > tcol
        left = tcol < head_dim
        twice = jnp.where(trow == tcol, 2.0, 1.0)
        for c in range(per_blk):
            cc = blk * per_blk + c
            at = pl.multiple_of(base + c * CHUNK, CHUNK)
            dt, ci, ce = dt_s[cc], ci_s[cc], ce_s[cc]
            end = jnp.broadcast_to(ci[:, CHUNK - 1:], ci.shape)
            q = spread_operand([dt, jnp.exp(ci), jnp.exp(end - ce)], CHUNK)
            w = jnp.dot(q, e_s[...], preferred_element_type=f32)
            col = jnp.concatenate([ci, ce, jnp.zeros((CHUNK - 2 * heads, CHUNK), f32)], axis=0).T
            u = u_s[pl.ds(at, CHUNK), :].astype(f32)
            udt = (u * w[:, :inner]).astype(bf16)
            b = bc_s[pl.ds(at, CHUNK), :n_state]
            cm = bc_s[pl.ds(at, CHUNK), n_state:]
            gram = lax.dot_general(cm, b, (((1,), (1,)), ((), ())), preferred_element_type=f32) * twice
            y = jnp.dot(cm, sf_s[cc].astype(bf16), preferred_element_type=f32) * w[:, inner:2 * inner]
            y = y + jnp.dot(cm, sb_s[cc].astype(bf16), preferred_element_type=f32) * w[:, 2 * inner:]
            y = y + skip_ref[...] * u
            outs = []
            for p in range(heads // 2):
                mats = []
                for h in (2 * p, 2 * p + 1):
                    d = jnp.where(later, col[:, h:h + 1] - ci[h:h + 1, :], ce[h:h + 1, :] - col[:, heads + h:heads + h + 1])
                    mats.append((gram * jnp.exp(jnp.minimum(d, 0.0))).astype(bf16))
                up = udt[:, p * CHUNK:(p + 1) * CHUNK]
                zero = jnp.zeros_like(up)
                rhs = jnp.concatenate([jnp.where(left, up, zero), jnp.where(left, zero, up)], axis=0)
                outs.append(jnp.dot(jnp.concatenate(mats, axis=1), rhs, preferred_element_type=f32))
            y = y + jnp.concatenate(outs, axis=1)
            z = z_s[pl.ds(at, CHUNK), :].astype(f32)
            z_s[pl.ds(at, CHUNK), :] = (y * (z / (1.0 + jnp.exp(-z)))).astype(bf16)
        for c in range(per_blk):
            at = pl.multiple_of(base + c * CHUNK, CHUNK)
            side = c % 2
            owner = blk * (per_blk // 2) + c // 2
            far = (lax.rem(owner // RING - zy[0] + RING, RING), lax.rem(lax.rem(owner, RING) - zy[1] + RING, RING))
            dist, group = (far[1], far[0]) if side == 0 else (far[0], far[1])

            @pl.when(dist == 0)
            def _():
                own_copy(side, group, at).start()

            @pl.when(dist > 0)
            def _():
                gate_copy(side, dist, group, at).start()

    @pl.when(i == y_first + n_blk // 4)
    def _():
        wait(ring_copies(1))
        start(along_x(opposite) + to_partner(opposite, 0))

    @pl.when(i == y_first + 3 * n_blk // 4)
    def _():
        wait(along_x(near + opposite))
        start(to_partner(near + opposite, 1))

    @pl.when(i == 3 * n_blk - 1)
    def _():
        for side in range(2):
            for group in range(RING):
                own_copy(side, group, 0).wait()
                for dist in range(1, RING):
                    gate_copy(side, dist, group, 0).wait()
        wait(to_partner(near + opposite, 0) + to_partner(near + opposite, 1))


def scan_call(x_blk, w_z, w_x, w_bc, w_dt, a_neg, dt_bias, d_skip, w_out, n_seq):
    tokens, d_model = x_blk.shape
    heads = a_neg.shape[0]
    inner = w_x.shape[1]
    head_dim = inner // heads
    n_state = w_bc.shape[1] // 2
    rows = min(512, tokens)
    n_blk = tokens // rows
    n_ch = tokens // CHUNK
    n_copies = 16 + 6 * (n_seq // 2 - 1) + 12
    w_dt = w_dt.T
    f32, bf16 = jnp.float32, jnp.bfloat16

    def whole(a):
        return pl.BlockSpec(a.shape, lambda i: (0, 0), pipeline_mode=pl.Buffered(1))

    return pl.pallas_call(
        functools.partial(scan_kernel, n_blk, n_seq, heads, head_dim),
        grid=(3 * n_blk,),
        out_shape=(jax.ShapeDtypeStruct((2, RING, tokens // (2 * RING), inner), bf16),
                   jax.ShapeDtypeStruct((2 * (RING - 1),) + w_out.shape, bf16)),
        in_specs=[pl.BlockSpec((rows, d_model), lambda i: (jnp.where(i < n_blk, i, jnp.minimum(i - n_blk, n_blk - 1)), 0)),
                  pl.BlockSpec(memory_space=pl.ANY), pl.BlockSpec(memory_space=pl.ANY), pl.BlockSpec(memory_space=pl.ANY), whole(w_dt)]
        + [pl.BlockSpec(memory_space=pltpu.SMEM)] * 3 + [pl.BlockSpec(memory_space=pl.ANY)],
        out_specs=(pl.BlockSpec(memory_space=pl.ANY), pl.BlockSpec(memory_space=pl.ANY)),
        scratch_shapes=[
            pltpu.VMEM((tokens, inner), bf16),
            pltpu.VMEM((tokens, inner), bf16),
            pltpu.VMEM((tokens, 2 * n_state), bf16),
            pltpu.VMEM((n_ch, n_state, inner), f32),
            pltpu.VMEM((n_ch, n_state, inner), f32),
            pltpu.VMEM((n_state, inner), f32),
            pltpu.VMEM((n_state, inner), f32),
            pltpu.VMEM((n_ch, heads, CHUNK), f32),
            pltpu.VMEM((n_ch, heads, CHUNK), f32),
            pltpu.VMEM((n_ch, heads, CHUNK), f32),
            pltpu.VMEM((n_ch, 8, inner), f32),
            pltpu.VMEM((8, inner), f32),
            pltpu.VMEM((CHUNK, 3 * inner), bf16),
            pltpu.VMEM((2, n_state + MSG_PAD, inner), bf16),
            pltpu.VMEM((n_seq - 1, n_state + MSG_PAD, inner), bf16),
            pltpu.VMEM((heads, CHUNK), f32),
            pltpu.VMEM((heads, CHUNK), f32),
            pltpu.VMEM((1, inner), f32),
            pltpu.VMEM(w_x.shape, bf16),
            pltpu.VMEM(w_bc.shape, bf16),
            pltpu.VMEM(w_z.shape, bf16),
            pltpu.SemaphoreType.DMA((3,)),
            pltpu.SemaphoreType.DMA((n_seq - 1,)),
            pltpu.SemaphoreType.DMA((n_seq - 1,)),
            pltpu.SemaphoreType.DMA((n_copies,)),
            pltpu.SemaphoreType.DMA((n_copies,)),
            pltpu.SemaphoreType.DMA((2, RING, RING)),
            pltpu.SemaphoreType.DMA((2, RING, RING)),
            pltpu.SemaphoreType.DMA((2, RING)),
        ],
        compiler_params=pltpu.CompilerParams(collective_id=0, has_side_effects=True, vmem_limit_bytes=60 * 1024 * 1024,
                                             dimension_semantics=('arbitrary',)),
        cost_estimate=pl.CostEstimate(flops=2 * tokens * d_model * (2 * inner + 3 * n_state) * 3, bytes_accessed=60 << 20, transcendentals=0),
    )(x_blk, w_z, w_x, w_bc, w_dt, dt_bias, a_neg, d_skip, w_out)


def out_kernel(n_col, ga_ref, wo_ref, wg_ref, x_ref, out_ref, send_s, recv_s, own_s, x_s, x_sem, send_sem, recv_sem):
    i = pl.program_id(0)
    zy = tp_coords()
    width = wo_ref.shape[1]
    f32, bf16 = jnp.float32, jnp.bfloat16

    def part_copy(side, dist, b):
        return pltpu.make_async_remote_copy(
            src_ref=send_s.at[side, dist - 1, b], dst_ref=recv_s.at[side, dist - 1, b],
            send_sem=send_sem.at[side, dist - 1, b], recv_sem=recv_sem.at[side, dist - 1, b],
            device_id={'tp': ring_peer(zy, 1 - side, dist)}, device_id_type=pl.DeviceIdType.MESH)

    def x_copy():
        rows = x_s.shape[0]
        at = pl.multiple_of(lax.axis_index('tp') * rows, rows)
        return pltpu.make_async_copy(x_ref.at[pl.ds(at, rows), :], x_s, x_sem)

    @pl.when(i == 0)
    def _():
        x_copy().start()
        barrier = pltpu.get_barrier_semaphore()
        for axis in range(2):
            for dist in range(1, RING):
                pl.semaphore_signal(barrier, inc=1, device_id={'tp': ring_peer(zy, axis, dist)}, device_id_type=pl.DeviceIdType.MESH)

    @pl.when(i < n_col)
    def _():
        for side in range(2):
            acc = jnp.dot(ga_ref[side, 0], wo_ref[...], preferred_element_type=f32)
            for dist in range(1, RING):
                acc = acc + jnp.dot(ga_ref[side, dist], wg_ref[side * 3 + dist - 1], preferred_element_type=f32)
            own_s[side, i] = acc[:CHUNK]
            for dist in range(1, RING):
                send_s[side, dist - 1, i] = acc[dist * CHUNK:(dist + 1) * CHUNK].astype(bf16)

    @pl.when(i == 0)
    def _():
        pl.semaphore_wait(pltpu.get_barrier_semaphore(), 2 * (RING - 1))

    @pl.when(i < n_col)
    def _():
        for side in range(2):
            for dist in range(1, RING):
                part_copy(side, dist, i).start()

    @pl.when(i == n_col)
    def _():
        x_copy().wait()

    @pl.when(i >= n_col)
    def _():
        b = i - n_col
        cols = pl.ds(pl.multiple_of(b * width, width), width)
        for side in range(2):
            acc = own_s[side, b]
            for dist in range(1, RING):
                part_copy(side, dist, b).wait()
                acc = acc + recv_s[side, dist - 1, b].astype(f32)
            at = side * CHUNK
            out_ref[at:at + CHUNK, :] = (x_s[at:at + CHUNK, cols].astype(f32) + acc).astype(bf16)


def out_call(g_all, w_out, w_got, x_blk):
    inner, d_model = w_out.shape
    rows = 2 * CHUNK
    width = min(512, d_model)
    n_col = d_model // width
    f32, bf16 = jnp.float32, jnp.bfloat16

    def column(i):
        return jnp.minimum(i, n_col - 1)

    return pl.pallas_call(
        functools.partial(out_kernel, n_col),
        grid=(2 * n_col,),
        out_shape=jax.ShapeDtypeStruct((rows, d_model), bf16),
        in_specs=[pl.BlockSpec(g_all.shape, lambda i: (0, 0, 0, 0), pipeline_mode=pl.Buffered(1)),
                  pl.BlockSpec((inner, width), lambda i: (0, column(i))),
                  pl.BlockSpec((2 * (RING - 1), inner, width), lambda i: (0, 0, column(i))),
                  pl.BlockSpec(memory_space=pl.ANY)],
        out_specs=pl.BlockSpec((rows, width), lambda i: (0, jnp.maximum(i - n_col, 0))),
        scratch_shapes=[
            pltpu.VMEM((2, RING - 1, n_col, CHUNK, width), bf16),
            pltpu.VMEM((2, RING - 1, n_col, CHUNK, width), bf16),
            pltpu.VMEM((2, n_col, CHUNK, width), f32),
            pltpu.VMEM((rows, d_model), bf16),
            pltpu.SemaphoreType.DMA,
            pltpu.SemaphoreType.DMA((2, RING - 1, n_col)),
            pltpu.SemaphoreType.DMA((2, RING - 1, n_col)),
        ],
        compiler_params=pltpu.CompilerParams(collective_id=1, has_side_effects=True, vmem_limit_bytes=60 * 1024 * 1024,
                                             dimension_semantics=('arbitrary',)),
        cost_estimate=pl.CostEstimate(flops=2 * 2 * 4 * CHUNK * 4 * inner * d_model, bytes_accessed=40 << 20, transcendentals=0),
    )(g_all, w_out, w_got, x_blk)


def solution(mesh):
    n_seq = mesh.shape['sp']

    def device_fn(x_blk, w_z, w_x, w_bc, w_dt, a_neg, dt_bias, d_skip, w_out):
        g_all, w_got = scan_call(x_blk, w_z, w_x, w_bc, w_dt, a_neg, dt_bias, d_skip, w_out, n_seq)
        return out_call(g_all, w_out, w_got, x_blk)

    in_specs = (P(('dp', 'sp'), None), P(None, 'tp'), P(None, 'tp'), P(None, None), P(None, 'tp'), P('tp'), P('tp'), P('tp'), P('tp', None))
    out_specs = P(('dp', 'sp', 'tp'), None)
    return jax.shard_map(device_fn, mesh=mesh, in_specs=in_specs, out_specs=out_specs, check_vma=False)
```

```python
import functools

import jax
import jax.numpy as jnp
from jax import lax
from jax.experimental import pallas as pl
from jax.experimental.pallas import tpu as pltpu
from jax.sharding import PartitionSpec as P

CHUNK = 128
MSG_PAD = 16
RING = 4
SHARE = 16
LAG = 3


def split3(v):
    hi = v.astype(jnp.bfloat16).astype(jnp.float32)
    rest = v - hi
    mid = rest.astype(jnp.bfloat16).astype(jnp.float32)
    return [hi, mid, rest - mid]


def spread_operand(quantities, width):
    rows = [part for q in quantities for part in split3(q)]
    have = sum(r.shape[0] for r in rows)
    rows.append(jnp.zeros((CHUNK - have, width), jnp.float32))
    return jnp.concatenate(rows, axis=0).T.astype(jnp.bfloat16)


def cumsum_lanes(v, lane):
    step = 1
    while step < v.shape[1]:
        v = v + jnp.where(lane >= step, pltpu.roll(v, step, 1), 0.0)
        step *= 2
    return v


def softplus(v):
    return jnp.maximum(v, 0.0) + jnp.log1p(jnp.exp(-jnp.abs(v)))


def tp_coords():
    index = lax.axis_index('tp')
    return index // RING, lax.rem(index, RING)


def ring_peer(zy, axis, dist):
    z, y = zy
    if axis == 0:
        return z * RING + lax.rem(y + dist, RING)
    return lax.rem(z + dist, RING) * RING + y


def scan_kernel(n_blk, n_seq, heads, head_dim, x_ref, wz_ref, wx_ref, wbc_ref, wdt_ref, bias_sm, aneg_sm, skip_sm, wo_ref, ga_ref, wg_ref,
                z_s, u_s, bc_s, sf_s, sb_s, f_s, g_s, dt_s, ci_s, ce_s, le_s, lt_s, e_s, msg_s, rcv_s, bias_ref, aneg_ref, skip_ref, wx_s, wbc_s, wz_s, load_sem, send_sem, recv_sem, ws_sem, wr_sem, gs_sem, gr_sem, own_sem):
    i = pl.program_id(0)
    me = lax.axis_index('sp')
    rows = x_ref.shape[0]
    inner = heads * head_dim
    per_blk = rows // CHUNK
    n_state = bc_s.shape[1] // 2
    f32, bf16 = jnp.float32, jnp.bfloat16
    lane = lax.broadcasted_iota(jnp.int32, (heads, CHUNK), 1)

    def peer_copy(s):
        dest = lax.rem(me + s, n_seq)
        side = jnp.where(me + s < n_seq, 0, 1)
        return pltpu.make_async_remote_copy(
            src_ref=msg_s.at[side], dst_ref=rcv_s.at[s - 1], send_sem=send_sem.at[s - 1], recv_sem=recv_sem.at[s - 1],
            device_id={'sp': dest}, device_id_type=pl.DeviceIdType.MESH)

    zy = tp_coords()
    z_first, y_first = n_blk, 2 * n_blk

    def load(k):
        src, dst = ((wx_ref, wx_s), (wbc_ref, wbc_s), (wz_ref, wz_s))[k]
        return pltpu.make_async_copy(src, dst, load_sem.at[k])

    n_chip = n_seq // 2
    chip, core = me // 2, lax.rem(me, 2)
    half = wo_ref.shape[0] // 2
    whole_rows = half - n_chip * SHARE

    def span(shared, everyone=False):
        at = core * half
        if not shared:
            return at, whole_rows
        if everyone:
            return at + whole_rows, n_chip * SHARE
        return at + whole_rows + chip * SHARE, SHARE

    def weight_copy(k, src, slot, at, size, dest):
        rows_at = pl.ds(pl.multiple_of(at, 8), size)
        return pltpu.make_async_remote_copy(
            src_ref=src.at[rows_at, :], dst_ref=wg_ref.at[slot, rows_at, :], send_sem=ws_sem.at[k], recv_sem=wr_sem.at[k],
            device_id=dest, device_id_type=pl.DeviceIdType.MESH)

    def ring_copies(hop):
        out = []
        for axis in range(2):
            for back in range(2):
                dist = RING - 1 if back else 1
                for shared in range(2):
                    at, size = span(shared)
                    k = ((hop * 2 + axis) * 2 + back) * 2 + shared
                    dest = {'tp': ring_peer(zy, axis, dist)}
                    if hop == 0:
                        out.append(weight_copy(k, wo_ref, axis * 3 + dist - 1, at, size, dest))
                    else:
                        out.append(weight_copy(k, wg_ref.at[axis * 3 + dist - 1], axis * 3 + 1, at + back * (size // 2), size // 2, dest))
        return out

    near, opposite = (0, 2, 3, 5), (1, 4)

    def along_x(slots):
        at, size = span(1)
        return [weight_copy(16 + slot * (n_chip - 1) + d - 1, wg_ref.at[slot], slot, at, size, {'sp': lax.rem(chip + d, n_chip) * 2 + core})
                for slot in slots for d in range(1, n_chip)]

    def to_partner(slots, shared):
        at, size = span(shared, everyone=True)
        first = 16 + 6 * (n_chip - 1)
        return [weight_copy(first + slot * 2 + shared, wg_ref.at[slot], slot, at, size, {'sp': chip * 2 + 1 - core}) for slot in slots]

    def start(copies):
        for c in copies:
            c.start()

    def wait(copies):
        for c in copies:
            c.wait()

    def gate_copy(side, dist, group, at):
        return pltpu.make_async_remote_copy(
            src_ref=z_s.at[pl.ds(at, CHUNK), :], dst_ref=ga_ref.at[side, dist, pl.ds(pl.multiple_of(group * CHUNK, CHUNK), CHUNK), :],
            send_sem=gs_sem.at[side, dist, group], recv_sem=gr_sem.at[side, dist, group],
            device_id={'tp': ring_peer(zy, side, dist)}, device_id_type=pl.DeviceIdType.MESH)

    def own_copy(side, group, at):
        return pltpu.make_async_copy(z_s.at[pl.ds(at, CHUNK), :], ga_ref.at[side, 0, pl.ds(pl.multiple_of(group * CHUNK, CHUNK), CHUNK), :],
                                     own_sem.at[side, group])

    @pl.when(i == 0)
    def _():
        barrier = pltpu.get_barrier_semaphore()
        for k in range(3):
            load(k).start()
        for s in range(1, n_seq):
            pl.semaphore_signal(barrier, inc=1, device_id={'sp': lax.rem(me + s, n_seq)}, device_id_type=pl.DeviceIdType.MESH)
        for axis in range(2):
            for dist in range(1, RING):
                pl.semaphore_signal(barrier, inc=1, device_id={'tp': ring_peer(zy, axis, dist)}, device_id_type=pl.DeviceIdType.MESH)
        pl.semaphore_wait(barrier, n_seq - 1 + 2 * (RING - 1))
        start(ring_copies(0))
        head = lax.broadcasted_iota(jnp.int32, bias_ref.shape, 0)
        owner = lax.broadcasted_iota(jnp.int32, skip_ref.shape, 1) // head_dim
        bias, aneg, skip = jnp.zeros_like(bias_ref), jnp.zeros_like(aneg_ref), jnp.zeros_like(skip_ref)
        for h in range(heads):
            bias = jnp.where(head == h, bias_sm[h], bias)
            aneg = jnp.where(head == h, aneg_sm[h], aneg)
            skip = jnp.where(owner == h, 2.0 * skip_sm[h], skip)
        bias_ref[...] = bias
        aneg_ref[...] = aneg
        skip_ref[...] = skip
        k = lax.broadcasted_iota(jnp.int32, e_s.shape, 0)
        j = lax.broadcasted_iota(jnp.int32, e_s.shape, 1)
        hit = (k // (3 * heads) == j // inner) & (k % heads == (j % inner) // head_dim)
        e_s[...] = jnp.where(hit, 1.0, 0.0).astype(bf16)
        f_s[...] = jnp.zeros_like(f_s)
        g_s[...] = jnp.zeros_like(g_s)
        lt_s[...] = jnp.zeros_like(lt_s)
        load(0).wait()
        load(1).wait()

    @pl.when(i < n_blk)
    def _():
        base = pl.multiple_of(i * rows, rows)
        xb = x_ref[...]
        raw = lax.dot_general(xb, wdt_ref[...], (((1,), (1,)), ((), ())), preferred_element_type=f32)
        bc_s[pl.ds(base, rows), :] = jnp.dot(xb, wbc_s[...], preferred_element_type=f32).astype(bf16)
        u_s[pl.ds(base, rows), :] = jnp.dot(xb, wx_s[...], preferred_element_type=f32).astype(bf16)
        for c in range(per_blk):
            cc = i * per_blk + c
            at = pl.multiple_of(base + c * CHUNK, CHUNK)
            dt = softplus(raw[c * CHUNK:(c + 1) * CHUNK, :].T + bias_ref[...])
            la = dt * aneg_ref[...]
            ci = cumsum_lanes(la, lane)
            ce = ci - la
            end = jnp.broadcast_to(ci[:, CHUNK - 1:], ci.shape)
            dt_s[cc] = dt
            ci_s[cc] = ci
            ce_s[cc] = ce
            q = spread_operand([jnp.exp(end - ci) * dt, jnp.exp(ce) * dt, end], CHUNK)
            w = jnp.dot(q, e_s[:, :2 * inner], preferred_element_type=f32)
            le = jnp.dot(q[:16], e_s[:, 2 * inner:], preferred_element_type=f32)[:8]
            le_s[cc] = le
            u = u_s[pl.ds(at, CHUNK), :].astype(f32)
            b = bc_s[pl.ds(at, CHUNK), :n_state]
            dims = (((0,), (0,)), ((), ()))
            sf = lax.dot_general(b, (u * w[:, :inner]).astype(bf16), dims, preferred_element_type=f32)
            sb = lax.dot_general(b, (u * w[:, inner:]).astype(bf16), dims, preferred_element_type=f32)
            sf_s[cc] = sf
            sb_s[cc] = sb
            lt = lt_s[...]
            f_s[...] = f_s[...] * jnp.exp(le[:1]) + sf
            g_s[...] = g_s[...] + jnp.exp(lt[:1]) * sb
            lt_s[...] = lt + le

    @pl.when(i == n_blk - 1)
    def _():
        lt = lt_s[:1]
        parts = split3(lt)
        row = lax.broadcasted_iota(jnp.int32, (MSG_PAD, inner), 0)
        tail = jnp.where(row == 0, parts[0], jnp.where(row == 1, parts[1], jnp.where(row == 2, parts[2], 0.0))).astype(bf16)
        for side, ref in ((0, f_s), (1, g_s)):
            msg_s[side, :n_state, :] = ref[...].astype(bf16)
            msg_s[side, n_state:, :] = tail
        for s in range(1, n_seq):
            peer_copy(s).start()

    @pl.when(i == z_first)
    def _():
        load(2).wait()

    @pl.when((i >= z_first) & (i < y_first))
    def _():
        base = pl.multiple_of((i - z_first) * rows, rows)
        z_s[pl.ds(base, rows), :] = jnp.dot(x_ref[...], wz_s[...], preferred_element_type=f32).astype(bf16)

    @pl.when(i == z_first + n_blk // 4)
    def _():
        wait(ring_copies(0))
        start(ring_copies(1) + along_x(near) + to_partner(near, 0))

    @pl.when(i == y_first)
    def _():
        for s in range(1, n_seq):
            peer_copy(s).wait()

        def log_of(s):
            t = rcv_s[s - 1, n_state:, :].astype(f32)
            return t[0:1] + t[1:2] + t[2:3]

        f_s[...] = jnp.zeros_like(f_s)
        g_s[...] = jnp.zeros_like(g_s)
        acc = jnp.zeros((1, inner), f32)
        for s in range(1, n_seq):
            wgt = jnp.where(s <= me, jnp.exp(acc), 0.0)
            f_s[...] += wgt * rcv_s[s - 1, :n_state, :].astype(f32)
            acc = acc + log_of(s)
        acc = jnp.zeros((1, inner), f32)
        for s in range(n_seq - 1, 0, -1):
            wgt = jnp.where(s > me, jnp.exp(acc), 0.0)
            g_s[...] += wgt * rcv_s[s - 1, :n_state, :].astype(f32)
            acc = acc + log_of(s)

        n_ch = n_blk * per_blk

        def sweep(t, _):
            for ref, state, c in ((sf_s, f_s, t), (sb_s, g_s, n_ch - 1 - t)):
                mine = ref[c]
                before = state[...]
                ref[c] = before
                state[...] = before * jnp.exp(le_s[c][:1]) + mine
            return 0

        lax.fori_loop(0, n_ch, sweep, 0)

    @pl.when(i >= y_first)
    def _():
        step = i - y_first
        blk = 2 * lax.rem(zy[0] + 1 + step // 2, RING) + lax.rem(step + 1 - zy[1] // 2, 2)
        base = pl.multiple_of(blk * rows, rows)
        trow = lax.broadcasted_iota(jnp.int32, (CHUNK, CHUNK), 0)
        tcol = lax.broadcasted_iota(jnp.int32, (CHUNK, CHUNK), 1)
        later = trow > tcol
        left = tcol < head_dim
        twice = jnp.where(trow == tcol, 2.0, 1.0)
        for c in range(per_blk):
            cc = blk * per_blk + c
            at = pl.multiple_of(base + c * CHUNK, CHUNK)
            dt, ci, ce = dt_s[cc], ci_s[cc], ce_s[cc]
            end = jnp.broadcast_to(ci[:, CHUNK - 1:], ci.shape)
            q = spread_operand([dt, jnp.exp(ci), jnp.exp(end - ce)], CHUNK)
            w = jnp.dot(q, e_s[...], preferred_element_type=f32)
            col = jnp.concatenate([ci, ce, jnp.zeros((CHUNK - 2 * heads, CHUNK), f32)], axis=0).T
            u = u_s[pl.ds(at, CHUNK), :].astype(f32)
            udt = (u * w[:, :inner]).astype(bf16)
            b = bc_s[pl.ds(at, CHUNK), :n_state]
            cm = bc_s[pl.ds(at, CHUNK), n_state:]
            gram = lax.dot_general(cm, b, (((1,), (1,)), ((), ())), preferred_element_type=f32) * twice
            y = jnp.dot(cm, sf_s[cc].astype(bf16), preferred_element_type=f32) * w[:, inner:2 * inner]
            y = y + jnp.dot(cm, sb_s[cc].astype(bf16), preferred_element_type=f32) * w[:, 2 * inner:]
            y = y + skip_ref[...] * u
            outs = []
            for p in range(heads // 2):
                mats = []
                for h in (2 * p, 2 * p + 1):
                    d = jnp.where(later, col[:, h:h + 1] - ci[h:h + 1, :], ce[h:h + 1, :] - col[:, heads + h:heads + h + 1])
                    mats.append((gram * jnp.exp(jnp.minimum(d, 0.0))).astype(bf16))
                up = udt[:, p * CHUNK:(p + 1) * CHUNK]
                zero = jnp.zeros_like(up)
                rhs = jnp.concatenate([jnp.where(left, up, zero), jnp.where(left, zero, up)], axis=0)
                outs.append(jnp.dot(jnp.concatenate(mats, axis=1), rhs, preferred_element_type=f32))
            y = y + jnp.concatenate(outs, axis=1)
            z = z_s[pl.ds(at, CHUNK), :].astype(f32)
            z_s[pl.ds(at, CHUNK), :] = (y * (z / (1.0 + jnp.exp(-z)))).astype(bf16)
        for c in range(per_blk):
            at = pl.multiple_of(base + c * CHUNK, CHUNK)
            side = c % 2
            owner = blk * (per_blk // 2) + c // 2
            far = (lax.rem(owner // RING - zy[0] + RING, RING), lax.rem(lax.rem(owner, RING) - zy[1] + RING, RING))
            dist, group = (far[1], far[0]) if side == 0 else (far[0], far[1])

            @pl.when(dist == 0)
            def _():
                own_copy(side, group, at).start()

            @pl.when(dist > 0)
            def _():
                gate_copy(side, dist, group, at).start()

    @pl.when(i == y_first + n_blk // 4)
    def _():
        wait(ring_copies(1))
        start(along_x(opposite) + to_partner(opposite, 0))

    @pl.when(i == y_first + 3 * n_blk // 4)
    def _():
        wait(along_x(near + opposite))
        start(to_partner(near + opposite, 1))

    @pl.when(i == 3 * n_blk - 1)
    def _():
        for side in range(2):
            for group in range(RING):
                own_copy(side, group, 0).wait()
                for dist in range(1, RING):
                    gate_copy(side, dist, group, 0).wait()
        wait(to_partner(near + opposite, 0) + to_partner(near + opposite, 1))


def scan_call(x_blk, w_z, w_x, w_bc, w_dt, a_neg, dt_bias, d_skip, w_out, n_seq):
    tokens, d_model = x_blk.shape
    heads = a_neg.shape[0]
    inner = w_x.shape[1]
    head_dim = inner // heads
    n_state = w_bc.shape[1] // 2
    rows = min(512, tokens)
    n_blk = tokens // rows
    n_ch = tokens // CHUNK
    n_copies = 16 + 6 * (n_seq // 2 - 1) + 12
    w_dt = w_dt.T
    f32, bf16 = jnp.float32, jnp.bfloat16

    def whole(a):
        return pl.BlockSpec(a.shape, lambda i: (0, 0), pipeline_mode=pl.Buffered(1))

    return pl.pallas_call(
        functools.partial(scan_kernel, n_blk, n_seq, heads, head_dim),
        grid=(3 * n_blk,),
        out_shape=(jax.ShapeDtypeStruct((2, RING, tokens // (2 * RING), inner), bf16),
                   jax.ShapeDtypeStruct((2 * (RING - 1),) + w_out.shape, bf16)),
        in_specs=[pl.BlockSpec((rows, d_model), lambda i: (jnp.where(i < n_blk, i, jnp.minimum(i - n_blk, n_blk - 1)), 0)),
                  pl.BlockSpec(memory_space=pl.ANY), pl.BlockSpec(memory_space=pl.ANY), pl.BlockSpec(memory_space=pl.ANY), whole(w_dt)]
        + [pl.BlockSpec(memory_space=pltpu.SMEM)] * 3 + [pl.BlockSpec(memory_space=pl.ANY)],
        out_specs=(pl.BlockSpec(memory_space=pl.ANY), pl.BlockSpec(memory_space=pl.ANY)),
        scratch_shapes=[
            pltpu.VMEM((tokens, inner), bf16),
            pltpu.VMEM((tokens, inner), bf16),
            pltpu.VMEM((tokens, 2 * n_state), bf16),
            pltpu.VMEM((n_ch, n_state, inner), f32),
            pltpu.VMEM((n_ch, n_state, inner), f32),
            pltpu.VMEM((n_state, inner), f32),
            pltpu.VMEM((n_state, inner), f32),
            pltpu.VMEM((n_ch, heads, CHUNK), f32),
            pltpu.VMEM((n_ch, heads, CHUNK), f32),
            pltpu.VMEM((n_ch, heads, CHUNK), f32),
            pltpu.VMEM((n_ch, 8, inner), f32),
            pltpu.VMEM((8, inner), f32),
            pltpu.VMEM((CHUNK, 3 * inner), bf16),
            pltpu.VMEM((2, n_state + MSG_PAD, inner), bf16),
            pltpu.VMEM((n_seq - 1, n_state + MSG_PAD, inner), bf16),
            pltpu.VMEM((heads, CHUNK), f32),
            pltpu.VMEM((heads, CHUNK), f32),
            pltpu.VMEM((1, inner), f32),
            pltpu.VMEM(w_x.shape, bf16),
            pltpu.VMEM(w_bc.shape, bf16),
            pltpu.VMEM(w_z.shape, bf16),
            pltpu.SemaphoreType.DMA((3,)),
            pltpu.SemaphoreType.DMA((n_seq - 1,)),
            pltpu.SemaphoreType.DMA((n_seq - 1,)),
            pltpu.SemaphoreType.DMA((n_copies,)),
            pltpu.SemaphoreType.DMA((n_copies,)),
            pltpu.SemaphoreType.DMA((2, RING, RING)),
            pltpu.SemaphoreType.DMA((2, RING, RING)),
            pltpu.SemaphoreType.DMA((2, RING)),
        ],
        compiler_params=pltpu.CompilerParams(collective_id=0, has_side_effects=True, vmem_limit_bytes=60 * 1024 * 1024,
                                             dimension_semantics=('arbitrary',)),
        cost_estimate=pl.CostEstimate(flops=2 * tokens * d_model * (2 * inner + 3 * n_state) * 3, bytes_accessed=60 << 20, transcendentals=0),
    )(x_blk, w_z, w_x, w_bc, w_dt, dt_bias, a_neg, d_skip, w_out)


def out_kernel(n_col, ga_ref, wo_ref, wg_ref, x_ref, out_ref, send_s, recv_s, own_s, near_s, x_s, x_sem, send_sem, recv_sem):
    i = pl.program_id(0)
    zy = tp_coords()
    width = wo_ref.shape[1]
    f32, bf16 = jnp.float32, jnp.bfloat16
    relay, direct, joined = range(3)

    def part_copy(kind, side, b):
        dist = 1 + 2 * lax.rem(b, 2)
        if kind == direct:
            dist = RING - dist
        return pltpu.make_async_remote_copy(
            src_ref=send_s.at[kind, side, b], dst_ref=recv_s.at[kind, side, b],
            send_sem=send_sem.at[kind, side, b], recv_sem=recv_sem.at[kind, side, b],
            device_id={'tp': ring_peer(zy, 1 - side, dist)}, device_id_type=pl.DeviceIdType.MESH)

    def x_copy():
        rows = x_s.shape[0]
        at = pl.multiple_of(lax.axis_index('tp') * rows, rows)
        return pltpu.make_async_copy(x_ref.at[pl.ds(at, rows), :], x_s, x_sem)

    @pl.when(i == 0)
    def _():
        x_copy().start()
        barrier = pltpu.get_barrier_semaphore()
        for axis in range(2):
            for dist in (1, RING - 1):
                pl.semaphore_signal(barrier, inc=1, device_id={'tp': ring_peer(zy, axis, dist)}, device_id_type=pl.DeviceIdType.MESH)

    @pl.when(i < n_col)
    def _():
        right = lax.rem(i, 2) == 0
        for side in range(2):
            acc = jnp.dot(ga_ref[side, 0], wo_ref[...], preferred_element_type=f32)
            for dist in range(1, RING):
                acc = acc + jnp.dot(ga_ref[side, dist], wg_ref[side * 3 + dist - 1], preferred_element_type=f32)
            one, two, three = (acc[dist * CHUNK:(dist + 1) * CHUNK] for dist in range(1, RING))
            own_s[side, i] = acc[:CHUNK]
            send_s[relay, side, i] = two.astype(bf16)
            send_s[direct, side, i] = jnp.where(right, three, one).astype(bf16)
            near_s[side, i] = jnp.where(right, one, three)

    @pl.when(i == 0)
    def _():
        pl.semaphore_wait(pltpu.get_barrier_semaphore(), 4)

    @pl.when(i < n_col)
    def _():
        for kind in (relay, direct):
            for side in range(2):
                part_copy(kind, side, i).start()

    @pl.when((i >= LAG) & (i < n_col + LAG))
    def _():
        b = i - LAG
        for side in range(2):
            part_copy(relay, side, b).wait_recv()
            send_s[joined, side, b] = (near_s[side, b] + recv_s[relay, side, b].astype(f32)).astype(bf16)
        for side in range(2):
            part_copy(joined, side, b).start()

    @pl.when(i == n_col + LAG)
    def _():
        x_copy().wait()

    @pl.when(i >= n_col + LAG)
    def _():
        b = i - n_col - LAG
        cols = pl.ds(pl.multiple_of(b * width, width), width)
        for side in range(2):
            part_copy(relay, side, b).wait_send()
            part_copy(direct, side, b).wait()
            part_copy(joined, side, b).wait()
            acc = own_s[side, b] + recv_s[direct, side, b].astype(f32) + recv_s[joined, side, b].astype(f32)
            at = side * CHUNK
            out_ref[at:at + CHUNK, :] = (x_s[at:at + CHUNK, cols].astype(f32) + acc).astype(bf16)


def out_call(g_all, w_out, w_got, x_blk):
    inner, d_model = w_out.shape
    rows = 2 * CHUNK
    width = min(512, d_model)
    n_col = d_model // width
    f32, bf16 = jnp.float32, jnp.bfloat16

    def column(i):
        return jnp.minimum(i, n_col - 1)

    return pl.pallas_call(
        functools.partial(out_kernel, n_col),
        grid=(2 * n_col + LAG,),
        out_shape=jax.ShapeDtypeStruct((rows, d_model), bf16),
        in_specs=[pl.BlockSpec(g_all.shape, lambda i: (0, 0, 0, 0), pipeline_mode=pl.Buffered(1)),
                  pl.BlockSpec((inner, width), lambda i: (0, column(i))),
                  pl.BlockSpec((2 * (RING - 1), inner, width), lambda i: (0, 0, column(i))),
                  pl.BlockSpec(memory_space=pl.ANY)],
        out_specs=pl.BlockSpec((rows, width), lambda i: (0, jnp.maximum(i - n_col - LAG, 0))),
        scratch_shapes=[
            pltpu.VMEM((3, 2, n_col, CHUNK, width), bf16),
            pltpu.VMEM((3, 2, n_col, CHUNK, width), bf16),
            pltpu.VMEM((2, n_col, CHUNK, width), f32),
            pltpu.VMEM((2, n_col, CHUNK, width), f32),
            pltpu.VMEM((rows, d_model), bf16),
            pltpu.SemaphoreType.DMA,
            pltpu.SemaphoreType.DMA((3, 2, n_col)),
            pltpu.SemaphoreType.DMA((3, 2, n_col)),
        ],
        compiler_params=pltpu.CompilerParams(collective_id=1, has_side_effects=True, vmem_limit_bytes=60 * 1024 * 1024,
                                             dimension_semantics=('arbitrary',)),
        cost_estimate=pl.CostEstimate(flops=2 * 2 * 4 * CHUNK * 4 * inner * d_model, bytes_accessed=40 << 20, transcendentals=0),
    )(g_all, w_out, w_got, x_blk)


def solution(mesh):
    n_seq = mesh.shape['sp']

    def device_fn(x_blk, w_z, w_x, w_bc, w_dt, a_neg, dt_bias, d_skip, w_out):
        g_all, w_got = scan_call(x_blk, w_z, w_x, w_bc, w_dt, a_neg, dt_bias, d_skip, w_out, n_seq)
        return out_call(g_all, w_out, w_got, x_blk)

    in_specs = (P(('dp', 'sp'), None), P(None, 'tp'), P(None, 'tp'), P(None, None), P(None, 'tp'), P('tp'), P('tp'), P('tp'), P('tp', None))
    out_specs = P(('dp', 'sp', 'tp'), None)
    return jax.shard_map(device_fn, mesh=mesh, in_specs=in_specs, out_specs=out_specs, check_vma=False)
```

```python
import functools

import jax
import jax.numpy as jnp
from jax import lax
from jax.experimental import pallas as pl
from jax.experimental.pallas import tpu as pltpu
from jax.sharding import PartitionSpec as P

CHUNK = 128
MSG_PAD = 16
RING = 4
SHARE = 16
LAG = 3
SPAN = 256


def split3(v):
    hi = v.astype(jnp.bfloat16).astype(jnp.float32)
    rest = v - hi
    mid = rest.astype(jnp.bfloat16).astype(jnp.float32)
    return [hi, mid, rest - mid]


def spread_operand(quantities, width):
    rows = [part for q in quantities for part in split3(q)]
    have = sum(r.shape[0] for r in rows)
    rows.append(jnp.zeros((CHUNK - have, width), jnp.float32))
    return jnp.concatenate(rows, axis=0).T.astype(jnp.bfloat16)


def cumsum_lanes(v, lane):
    step = 1
    while step < v.shape[1]:
        v = v + jnp.where(lane >= step, pltpu.roll(v, step, 1), 0.0)
        step *= 2
    return v


def softplus(v):
    return jnp.maximum(v, 0.0) + jnp.log1p(jnp.exp(-jnp.abs(v)))


def tp_coords():
    index = lax.axis_index('tp')
    return index // RING, lax.rem(index, RING)


def ring_peer(zy, axis, dist):
    z, y = zy
    if axis == 0:
        return z * RING + lax.rem(y + dist, RING)
    return lax.rem(z + dist, RING) * RING + y


def scan_kernel(n_blk, n_seq, heads, head_dim, x_ref, wz_ref, wx_ref, wbc_ref, wdt_ref, bias_sm, aneg_sm, skip_sm, wo_ref, ga_ref, wg_ref,
                z_s, u_s, bc_s, sf_s, sb_s, f_s, g_s, dt_s, ci_s, ce_s, le_s, lt_s, e_s, msg_s, rcv_s, bias_ref, aneg_ref, skip_ref, wx_s, wbc_s, wz_s, load_sem, send_sem, recv_sem, ws_sem, wr_sem, gs_sem, gr_sem, own_sem):
    i = pl.program_id(0)
    me = lax.axis_index('sp')
    rows = x_ref.shape[0]
    inner = heads * head_dim
    per_blk = rows // CHUNK
    n_state = bc_s.shape[1] // 2
    f32, bf16 = jnp.float32, jnp.bfloat16
    lane = lax.broadcasted_iota(jnp.int32, (heads, CHUNK), 1)

    zy = tp_coords()
    z_first, y_first = n_blk, 2 * n_blk

    def load(k):
        src, dst = ((wx_ref, wx_s), (wbc_ref, wbc_s), (wz_ref, wz_s))[k]
        return pltpu.make_async_copy(src, dst, load_sem.at[k])

    n_chip = n_seq // 2
    chip, core = me // 2, lax.rem(me, 2)
    half = wo_ref.shape[0] // 2
    whole_rows = half - n_chip * SHARE

    def state_copy(k):
        far = n_chip - 1
        if k < far:
            d = k + 1
            src, slot = msg_s.at[jnp.where(chip + d < n_chip, 0, 1)], 2 * d
            dest = lax.rem(chip + d, n_chip) * 2 + core
        elif k < 2 * far:
            d = k - far + 1
            src, slot, dest = rcv_s.at[2 * d - 1], 2 * d + 1 - 2 * core, chip * 2 + 1 - core
        else:
            src, slot, dest = msg_s.at[core], jnp.where(core == 0, 1, n_seq - 1), chip * 2 + 1 - core
        return pltpu.make_async_remote_copy(
            src_ref=src, dst_ref=rcv_s.at[slot - 1], send_sem=send_sem.at[k], recv_sem=recv_sem.at[k],
            device_id={'sp': dest}, device_id_type=pl.DeviceIdType.MESH)

    def span(shared, everyone=False):
        at = core * half
        if not shared:
            return at, whole_rows
        if everyone:
            return at + whole_rows, n_chip * SHARE
        return at + whole_rows + chip * SHARE, SHARE

    def weight_copy(k, src, slot, at, size, dest):
        rows_at = pl.ds(pl.multiple_of(at, 8), size)
        return pltpu.make_async_remote_copy(
            src_ref=src.at[rows_at, :], dst_ref=wg_ref.at[slot, rows_at, :], send_sem=ws_sem.at[k], recv_sem=wr_sem.at[k],
            device_id=dest, device_id_type=pl.DeviceIdType.MESH)

    def ring_copies(hop):
        out = []
        for axis in range(2):
            for back in range(2):
                dist = RING - 1 if back else 1
                for shared in range(2):
                    at, size = span(shared)
                    k = ((hop * 2 + axis) * 2 + back) * 2 + shared
                    dest = {'tp': ring_peer(zy, axis, dist)}
                    if hop == 0:
                        out.append(weight_copy(k, wo_ref, axis * 3 + dist - 1, at, size, dest))
                    else:
                        out.append(weight_copy(k, wg_ref.at[axis * 3 + dist - 1], axis * 3 + 1, at + back * (size // 2), size // 2, dest))
        return out

    near, opposite = (0, 2, 3, 5), (1, 4)

    def along_x(slots):
        at, size = span(1)
        return [weight_copy(16 + slot * (n_chip - 1) + d - 1, wg_ref.at[slot], slot, at, size, {'sp': lax.rem(chip + d, n_chip) * 2 + core})
                for slot in slots for d in range(1, n_chip)]

    def to_partner(slots, shared):
        at, size = span(shared, everyone=True)
        first = 16 + 6 * (n_chip - 1)
        return [weight_copy(first + slot * 2 + shared, wg_ref.at[slot], slot, at, size, {'sp': chip * 2 + 1 - core}) for slot in slots]

    def start(copies):
        for c in copies:
            c.start()

    def wait(copies):
        for c in copies:
            c.wait()

    def gate_copy(side, dist, group, at):
        return pltpu.make_async_remote_copy(
            src_ref=z_s.at[pl.ds(at, CHUNK), :], dst_ref=ga_ref.at[side, dist, pl.ds(pl.multiple_of(group * CHUNK, CHUNK), CHUNK), :],
            send_sem=gs_sem.at[side, dist, group], recv_sem=gr_sem.at[side, dist, group],
            device_id={'tp': ring_peer(zy, side, dist)}, device_id_type=pl.DeviceIdType.MESH)

    def own_copy(side, group, at):
        return pltpu.make_async_copy(z_s.at[pl.ds(at, CHUNK), :], ga_ref.at[side, 0, pl.ds(pl.multiple_of(group * CHUNK, CHUNK), CHUNK), :],
                                     own_sem.at[side, group])

    @pl.when(i == 0)
    def _():
        barrier = pltpu.get_barrier_semaphore()
        for k in range(3):
            load(k).start()
        for s in range(1, n_seq):
            pl.semaphore_signal(barrier, inc=1, device_id={'sp': lax.rem(me + s, n_seq)}, device_id_type=pl.DeviceIdType.MESH)
        for axis in range(2):
            for dist in range(1, RING):
                pl.semaphore_signal(barrier, inc=1, device_id={'tp': ring_peer(zy, axis, dist)}, device_id_type=pl.DeviceIdType.MESH)
        pl.semaphore_wait(barrier, n_seq - 1 + 2 * (RING - 1))
        start(ring_copies(0))
        head = lax.broadcasted_iota(jnp.int32, bias_ref.shape, 0)
        owner = lax.broadcasted_iota(jnp.int32, skip_ref.shape, 1) // head_dim
        bias, aneg, skip = jnp.zeros_like(bias_ref), jnp.zeros_like(aneg_ref), jnp.zeros_like(skip_ref)
        for h in range(heads):
            bias = jnp.where(head == h, bias_sm[h], bias)
            aneg = jnp.where(head == h, aneg_sm[h], aneg)
            skip = jnp.where(owner == h, 2.0 * skip_sm[h], skip)
        bias_ref[...] = bias
        aneg_ref[...] = aneg
        skip_ref[...] = skip
        k = lax.broadcasted_iota(jnp.int32, e_s.shape, 0)
        j = lax.broadcasted_iota(jnp.int32, e_s.shape, 1)
        hit = (k // (3 * heads) == j // inner) & (k % heads == (j % inner) // head_dim)
        e_s[...] = jnp.where(hit, 1.0, 0.0).astype(bf16)
        f_s[...] = jnp.zeros_like(f_s)
        g_s[...] = jnp.zeros_like(g_s)
        lt_s[...] = jnp.zeros_like(lt_s)
        load(0).wait()
        load(1).wait()

    @pl.when(i < n_blk)
    def _():
        base = pl.multiple_of(i * rows, rows)
        xb = x_ref[...]
        raw = lax.dot_general(xb, wdt_ref[...], (((1,), (1,)), ((), ())), preferred_element_type=f32)
        bc_s[pl.ds(base, rows), :] = jnp.dot(xb, wbc_s[...], preferred_element_type=f32).astype(bf16)
        u_s[pl.ds(base, rows), :] = jnp.dot(xb, wx_s[...], preferred_element_type=f32).astype(bf16)
        for c in range(per_blk):
            cc = i * per_blk + c
            at = pl.multiple_of(base + c * CHUNK, CHUNK)
            dt = softplus(raw[c * CHUNK:(c + 1) * CHUNK, :].T + bias_ref[...])
            la = dt * aneg_ref[...]
            ci = cumsum_lanes(la, lane)
            ce = ci - la
            end = jnp.broadcast_to(ci[:, CHUNK - 1:], ci.shape)
            dt_s[cc] = dt
            ci_s[cc] = ci
            ce_s[cc] = ce
            q = spread_operand([jnp.exp(end - ci) * dt, jnp.exp(ce) * dt, end], CHUNK)
            w = jnp.dot(q, e_s[:, :2 * inner], preferred_element_type=f32)
            le = jnp.dot(q[:16], e_s[:, 2 * inner:], preferred_element_type=f32)[:8]
            le_s[cc] = le
            u = u_s[pl.ds(at, CHUNK), :].astype(f32)
            b = bc_s[pl.ds(at, CHUNK), :n_state]
            dims = (((0,), (0,)), ((), ()))
            sf = lax.dot_general(b, (u * w[:, :inner]).astype(bf16), dims, preferred_element_type=f32)
            sb = lax.dot_general(b, (u * w[:, inner:]).astype(bf16), dims, preferred_element_type=f32)
            sf_s[cc] = sf
            sb_s[cc] = sb
            lt = lt_s[...]
            f_s[...] = f_s[...] * jnp.exp(le[:1]) + sf
            g_s[...] = g_s[...] + jnp.exp(lt[:1]) * sb
            lt_s[...] = lt + le

    @pl.when(i == n_blk - 1)
    def _():
        lt = lt_s[:1]
        parts = split3(lt)
        row = lax.broadcasted_iota(jnp.int32, (MSG_PAD, inner), 0)
        tail = jnp.where(row == 0, parts[0], jnp.where(row == 1, parts[1], jnp.where(row == 2, parts[2], 0.0))).astype(bf16)
        for side, ref in ((0, f_s), (1, g_s)):
            msg_s[side, :n_state, :] = ref[...].astype(bf16)
            msg_s[side, n_state:, :] = tail
        start([state_copy(k) for k in (*range(n_chip - 1), 2 * n_chip - 2)])

    @pl.when(i == z_first)
    def _():
        load(2).wait()

    @pl.when((i >= z_first) & (i < y_first))
    def _():
        base = pl.multiple_of((i - z_first) * rows, rows)
        z_s[pl.ds(base, rows), :] = jnp.dot(x_ref[...], wz_s[...], preferred_element_type=f32).astype(bf16)

    @pl.when(i == z_first + n_blk // 4)
    def _():
        wait(ring_copies(0))
        start(ring_copies(1) + along_x(near) + to_partner(near, 0))

    @pl.when(i == z_first + n_blk // 2 + 1)
    def _():
        wait([state_copy(k) for k in range(n_chip - 1)])
        start([state_copy(k) for k in range(n_chip - 1, 2 * n_chip - 2)])

    @pl.when(i == y_first)
    def _():
        wait([state_copy(k) for k in range(n_chip - 1, 2 * n_chip - 1)])

        def log_of(s):
            t = rcv_s[s - 1, n_state:, :].astype(f32)
            return t[0:1] + t[1:2] + t[2:3]

        f_s[...] = jnp.zeros_like(f_s)
        g_s[...] = jnp.zeros_like(g_s)
        acc = jnp.zeros((1, inner), f32)
        for s in range(1, n_seq):
            wgt = jnp.where(s <= me, jnp.exp(acc), 0.0)
            f_s[...] += wgt * rcv_s[s - 1, :n_state, :].astype(f32)
            acc = acc + log_of(s)
        acc = jnp.zeros((1, inner), f32)
        for s in range(n_seq - 1, 0, -1):
            wgt = jnp.where(s > me, jnp.exp(acc), 0.0)
            g_s[...] += wgt * rcv_s[s - 1, :n_state, :].astype(f32)
            acc = acc + log_of(s)

        n_ch = n_blk * per_blk

        def sweep(t, _):
            for ref, state, c in ((sf_s, f_s, t), (sb_s, g_s, n_ch - 1 - t)):
                mine = ref[c]
                before = state[...]
                ref[c] = before
                state[...] = before * jnp.exp(le_s[c][:1]) + mine
            return 0

        lax.fori_loop(0, n_ch, sweep, 0)

    @pl.when(i >= y_first)
    def _():
        step = i - y_first
        blk = 2 * lax.rem(zy[0] + 1 + step // 2, RING) + lax.rem(step + 1 - zy[1] // 2, 2)
        base = pl.multiple_of(blk * rows, rows)
        trow = lax.broadcasted_iota(jnp.int32, (CHUNK, CHUNK), 0)
        tcol = lax.broadcasted_iota(jnp.int32, (CHUNK, CHUNK), 1)
        later = trow > tcol
        left = tcol < head_dim
        twice = jnp.where(trow == tcol, 2.0, 1.0)
        for c in range(per_blk):
            cc = blk * per_blk + c
            at = pl.multiple_of(base + c * CHUNK, CHUNK)
            dt, ci, ce = dt_s[cc], ci_s[cc], ce_s[cc]
            end = jnp.broadcast_to(ci[:, CHUNK - 1:], ci.shape)
            q = spread_operand([dt, jnp.exp(ci), jnp.exp(end - ce)], CHUNK)
            col = jnp.concatenate([ci, ce, jnp.zeros((CHUNK - 2 * heads, CHUNK), f32)], axis=0).T
            b = bc_s[pl.ds(at, CHUNK), :n_state]
            cm = bc_s[pl.ds(at, CHUNK), n_state:]
            gram = lax.dot_general(cm, b, (((1,), (1,)), ((), ())), preferred_element_type=f32) * twice
            for lo in range(0, inner, SPAN):
                here = slice(lo, lo + SPAN)
                u = u_s[pl.ds(at, CHUNK), here].astype(f32)
                wdt = jnp.dot(q, e_s[:, here], preferred_element_type=f32)
                udt = (u * wdt).astype(bf16)
                outs = []
                for p in range(lo // CHUNK, (lo + SPAN) // CHUNK):
                    mats = []
                    for h in (2 * p, 2 * p + 1):
                        d = jnp.where(later, col[:, h:h + 1] - ci[h:h + 1, :], ce[h:h + 1, :] - col[:, heads + h:heads + h + 1])
                        mats.append((gram * jnp.exp(jnp.minimum(d, 0.0))).astype(bf16))
                    up = udt[:, p * CHUNK - lo:(p + 1) * CHUNK - lo]
                    zero = jnp.zeros_like(up)
                    rhs = jnp.concatenate([jnp.where(left, up, zero), jnp.where(left, zero, up)], axis=0)
                    outs.append(jnp.dot(jnp.concatenate(mats, axis=1), rhs, preferred_element_type=f32))
                y = jnp.concatenate(outs, axis=1) if len(outs) > 1 else outs[0]
                for ref, first in ((sf_s, inner), (sb_s, 2 * inner)):
                    grown = jnp.dot(q, e_s[:, first + lo:first + lo + SPAN], preferred_element_type=f32)
                    y = y + jnp.dot(cm, ref[cc, :, here].astype(bf16), preferred_element_type=f32) * grown
                y = y + skip_ref[:, here] * u
                z = z_s[pl.ds(at, CHUNK), here].astype(f32)
                z_s[pl.ds(at, CHUNK), here] = (y * (z / (1.0 + jnp.exp(-z)))).astype(bf16)
        for c in range(per_blk):
            at = pl.multiple_of(base + c * CHUNK, CHUNK)
            side = c % 2
            owner = blk * (per_blk // 2) + c // 2
            far = (lax.rem(owner // RING - zy[0] + RING, RING), lax.rem(lax.rem(owner, RING) - zy[1] + RING, RING))
            dist, group = (far[1], far[0]) if side == 0 else (far[0], far[1])

            @pl.when(dist == 0)
            def _():
                own_copy(side, group, at).start()

            @pl.when(dist > 0)
            def _():
                gate_copy(side, dist, group, at).start()

    @pl.when(i == y_first + n_blk // 4)
    def _():
        wait(ring_copies(1))
        start(along_x(opposite) + to_partner(opposite, 0))

    @pl.when(i == y_first + 3 * n_blk // 4)
    def _():
        wait(along_x(near + opposite))
        start(to_partner(near + opposite, 1))

    @pl.when(i == 3 * n_blk - 1)
    def _():
        for side in range(2):
            for group in range(RING):
                own_copy(side, group, 0).wait()
                for dist in range(1, RING):
                    gate_copy(side, dist, group, 0).wait()
        wait(to_partner(near + opposite, 0) + to_partner(near + opposite, 1))


def scan_call(x_blk, w_z, w_x, w_bc, w_dt, a_neg, dt_bias, d_skip, w_out, n_seq):
    tokens, d_model = x_blk.shape
    heads = a_neg.shape[0]
    inner = w_x.shape[1]
    head_dim = inner // heads
    n_state = w_bc.shape[1] // 2
    rows = min(512, tokens)
    n_blk = tokens // rows
    n_ch = tokens // CHUNK
    n_copies = 16 + 6 * (n_seq // 2 - 1) + 12
    w_dt = w_dt.T
    f32, bf16 = jnp.float32, jnp.bfloat16

    def whole(a):
        return pl.BlockSpec(a.shape, lambda i: (0, 0), pipeline_mode=pl.Buffered(1))

    return pl.pallas_call(
        functools.partial(scan_kernel, n_blk, n_seq, heads, head_dim),
        grid=(3 * n_blk,),
        out_shape=(jax.ShapeDtypeStruct((2, RING, tokens // (2 * RING), inner), bf16),
                   jax.ShapeDtypeStruct((2 * (RING - 1),) + w_out.shape, bf16)),
        in_specs=[pl.BlockSpec((rows, d_model), lambda i: (jnp.where(i < n_blk, i, jnp.minimum(i - n_blk, n_blk - 1)), 0)),
                  pl.BlockSpec(memory_space=pl.ANY), pl.BlockSpec(memory_space=pl.ANY), pl.BlockSpec(memory_space=pl.ANY), whole(w_dt)]
        + [pl.BlockSpec(memory_space=pltpu.SMEM)] * 3 + [pl.BlockSpec(memory_space=pl.ANY)],
        out_specs=(pl.BlockSpec(memory_space=pl.ANY), pl.BlockSpec(memory_space=pl.ANY)),
        scratch_shapes=[
            pltpu.VMEM((tokens, inner), bf16),
            pltpu.VMEM((tokens, inner), bf16),
            pltpu.VMEM((tokens, 2 * n_state), bf16),
            pltpu.VMEM((n_ch, n_state, inner), f32),
            pltpu.VMEM((n_ch, n_state, inner), f32),
            pltpu.VMEM((n_state, inner), f32),
            pltpu.VMEM((n_state, inner), f32),
            pltpu.VMEM((n_ch, heads, CHUNK), f32),
            pltpu.VMEM((n_ch, heads, CHUNK), f32),
            pltpu.VMEM((n_ch, heads, CHUNK), f32),
            pltpu.VMEM((n_ch, 8, inner), f32),
            pltpu.VMEM((8, inner), f32),
            pltpu.VMEM((CHUNK, 3 * inner), bf16),
            pltpu.VMEM((2, n_state + MSG_PAD, inner), bf16),
            pltpu.VMEM((n_seq - 1, n_state + MSG_PAD, inner), bf16),
            pltpu.VMEM((heads, CHUNK), f32),
            pltpu.VMEM((heads, CHUNK), f32),
            pltpu.VMEM((1, inner), f32),
            pltpu.VMEM(w_x.shape, bf16),
            pltpu.VMEM(w_bc.shape, bf16),
            pltpu.VMEM(w_z.shape, bf16),
            pltpu.SemaphoreType.DMA((3,)),
            pltpu.SemaphoreType.DMA((n_seq - 1,)),
            pltpu.SemaphoreType.DMA((n_seq - 1,)),
            pltpu.SemaphoreType.DMA((n_copies,)),
            pltpu.SemaphoreType.DMA((n_copies,)),
            pltpu.SemaphoreType.DMA((2, RING, RING)),
            pltpu.SemaphoreType.DMA((2, RING, RING)),
            pltpu.SemaphoreType.DMA((2, RING)),
        ],
        compiler_params=pltpu.CompilerParams(collective_id=0, has_side_effects=True, vmem_limit_bytes=60 * 1024 * 1024,
                                             dimension_semantics=('arbitrary',)),
        cost_estimate=pl.CostEstimate(flops=2 * tokens * d_model * (2 * inner + 3 * n_state) * 3, bytes_accessed=60 << 20, transcendentals=0),
    )(x_blk, w_z, w_x, w_bc, w_dt, dt_bias, a_neg, d_skip, w_out)


def out_kernel(n_col, ga_ref, wo_ref, wg_ref, x_ref, out_ref, send_s, recv_s, own_s, near_s, x_s, x_sem, send_sem, recv_sem):
    i = pl.program_id(0)
    zy = tp_coords()
    width = wo_ref.shape[1]
    f32, bf16 = jnp.float32, jnp.bfloat16
    relay, direct, joined = range(3)

    def part_copy(kind, side, b):
        dist = 1 + 2 * lax.rem(b, 2)
        if kind == direct:
            dist = RING - dist
        return pltpu.make_async_remote_copy(
            src_ref=send_s.at[kind, side, b], dst_ref=recv_s.at[kind, side, b],
            send_sem=send_sem.at[kind, side, b], recv_sem=recv_sem.at[kind, side, b],
            device_id={'tp': ring_peer(zy, 1 - side, dist)}, device_id_type=pl.DeviceIdType.MESH)

    def x_copy():
        rows = x_s.shape[0]
        at = pl.multiple_of(lax.axis_index('tp') * rows, rows)
        return pltpu.make_async_copy(x_ref.at[pl.ds(at, rows), :], x_s, x_sem)

    @pl.when(i == 0)
    def _():
        x_copy().start()
        barrier = pltpu.get_barrier_semaphore()
        for axis in range(2):
            for dist in (1, RING - 1):
                pl.semaphore_signal(barrier, inc=1, device_id={'tp': ring_peer(zy, axis, dist)}, device_id_type=pl.DeviceIdType.MESH)

    @pl.when(i < n_col)
    def _():
        right = lax.rem(i, 2) == 0
        for side in range(2):
            acc = jnp.dot(ga_ref[side, 0], wo_ref[...], preferred_element_type=f32)
            for dist in range(1, RING):
                acc = acc + jnp.dot(ga_ref[side, dist], wg_ref[side * 3 + dist - 1], preferred_element_type=f32)
            one, two, three = (acc[dist * CHUNK:(dist + 1) * CHUNK] for dist in range(1, RING))
            own_s[side, i] = acc[:CHUNK]
            send_s[relay, side, i] = two.astype(bf16)
            send_s[direct, side, i] = jnp.where(right, three, one).astype(bf16)
            near_s[side, i] = jnp.where(right, one, three)

    @pl.when(i == 0)
    def _():
        pl.semaphore_wait(pltpu.get_barrier_semaphore(), 4)

    @pl.when(i < n_col)
    def _():
        for kind in (relay, direct):
            for side in range(2):
                part_copy(kind, side, i).start()

    @pl.when((i >= LAG) & (i < n_col + LAG))
    def _():
        b = i - LAG
        for side in range(2):
            part_copy(relay, side, b).wait_recv()
            send_s[joined, side, b] = (near_s[side, b] + recv_s[relay, side, b].astype(f32)).astype(bf16)
        for side in range(2):
            part_copy(joined, side, b).start()

    @pl.when(i == n_col + LAG)
    def _():
        x_copy().wait()

    @pl.when(i >= n_col + LAG)
    def _():
        b = i - n_col - LAG
        cols = pl.ds(pl.multiple_of(b * width, width), width)
        for side in range(2):
            part_copy(relay, side, b).wait_send()
            part_copy(direct, side, b).wait()
            part_copy(joined, side, b).wait()
            acc = own_s[side, b] + recv_s[direct, side, b].astype(f32) + recv_s[joined, side, b].astype(f32)
            at = side * CHUNK
            out_ref[at:at + CHUNK, :] = (x_s[at:at + CHUNK, cols].astype(f32) + acc).astype(bf16)


def out_call(g_all, w_out, w_got, x_blk):
    inner, d_model = w_out.shape
    rows = 2 * CHUNK
    width = min(512, d_model)
    n_col = d_model // width
    f32, bf16 = jnp.float32, jnp.bfloat16

    def column(i):
        return jnp.minimum(i, n_col - 1)

    return pl.pallas_call(
        functools.partial(out_kernel, n_col),
        grid=(2 * n_col + LAG,),
        out_shape=jax.ShapeDtypeStruct((rows, d_model), bf16),
        in_specs=[pl.BlockSpec(g_all.shape, lambda i: (0, 0, 0, 0), pipeline_mode=pl.Buffered(1)),
                  pl.BlockSpec((inner, width), lambda i: (0, column(i))),
                  pl.BlockSpec((2 * (RING - 1), inner, width), lambda i: (0, 0, column(i))),
                  pl.BlockSpec(memory_space=pl.ANY)],
        out_specs=pl.BlockSpec((rows, width), lambda i: (0, jnp.maximum(i - n_col - LAG, 0))),
        scratch_shapes=[
            pltpu.VMEM((3, 2, n_col, CHUNK, width), bf16),
            pltpu.VMEM((3, 2, n_col, CHUNK, width), bf16),
            pltpu.VMEM((2, n_col, CHUNK, width), f32),
            pltpu.VMEM((2, n_col, CHUNK, width), f32),
            pltpu.VMEM((rows, d_model), bf16),
            pltpu.SemaphoreType.DMA,
            pltpu.SemaphoreType.DMA((3, 2, n_col)),
            pltpu.SemaphoreType.DMA((3, 2, n_col)),
        ],
        compiler_params=pltpu.CompilerParams(collective_id=1, has_side_effects=True, vmem_limit_bytes=60 * 1024 * 1024,
                                             dimension_semantics=('arbitrary',)),
        cost_estimate=pl.CostEstimate(flops=2 * 2 * 4 * CHUNK * 4 * inner * d_model, bytes_accessed=40 << 20, transcendentals=0),
    )(g_all, w_out, w_got, x_blk)


def solution(mesh):
    n_seq = mesh.shape['sp']

    def device_fn(x_blk, w_z, w_x, w_bc, w_dt, a_neg, dt_bias, d_skip, w_out):
        g_all, w_got = scan_call(x_blk, w_z, w_x, w_bc, w_dt, a_neg, dt_bias, d_skip, w_out, n_seq)
        return out_call(g_all, w_out, w_got, x_blk)

    in_specs = (P(('dp', 'sp'), None), P(None, 'tp'), P(None, 'tp'), P(None, None), P(None, 'tp'), P('tp'), P('tp'), P('tp'), P('tp', None))
    out_specs = P(('dp', 'sp', 'tp'), None)
    return jax.shard_map(device_fn, mesh=mesh, in_specs=in_specs, out_specs=out_specs, check_vma=False)
```

```python
import functools

import jax
import jax.numpy as jnp
from jax import lax
from jax.experimental import pallas as pl
from jax.experimental.pallas import tpu as pltpu
from jax.sharding import PartitionSpec as P

CHUNK = 128
MSG_PAD = 16
RING = 4
SHARE = 16
LAG = 3
SPAN = 256


def split3(v):
    hi = v.astype(jnp.bfloat16).astype(jnp.float32)
    rest = v - hi
    mid = rest.astype(jnp.bfloat16).astype(jnp.float32)
    return [hi, mid, rest - mid]


def spread_operand(quantities, width):
    rows = [part for q in quantities for part in split3(q)]
    have = sum(r.shape[0] for r in rows)
    rows.append(jnp.zeros((CHUNK - have, width), jnp.float32))
    return jnp.concatenate(rows, axis=0).T.astype(jnp.bfloat16)


def cumsum_lanes(v, lane):
    step = 1
    while step < v.shape[1]:
        v = v + jnp.where(lane >= step, pltpu.roll(v, step, 1), 0.0)
        step *= 2
    return v


def softplus(v):
    return jnp.maximum(v, 0.0) + jnp.log1p(jnp.exp(-jnp.abs(v)))


def tp_coords():
    index = lax.axis_index('tp')
    return index // RING, lax.rem(index, RING)


def ring_peer(zy, axis, dist):
    z, y = zy
    if axis == 0:
        return z * RING + lax.rem(y + dist, RING)
    return lax.rem(z + dist, RING) * RING + y


def scan_kernel(n_blk, n_seq, heads, head_dim, x_ref, wz_ref, wx_ref, wbc_ref, wdt_ref, bias_sm, aneg_sm, skip_sm, wo_ref, ga_ref, wg_ref,
                z_s, u_s, bc_s, sf_s, sb_s, f_s, g_s, dt_s, ci_s, ce_s, le_s, lt_s, e_s, msg_s, rcv_s, bias_ref, aneg_ref, skip_ref, wx_s, wbc_s, wz_s, load_sem, send_sem, recv_sem, ws_sem, wr_sem, gs_sem, gr_sem, own_sem):
    i = pl.program_id(0)
    me = lax.axis_index('sp')
    rows = x_ref.shape[0]
    inner = heads * head_dim
    per_blk = rows // CHUNK
    n_state = bc_s.shape[1] // 2
    f32, bf16 = jnp.float32, jnp.bfloat16
    lane = lax.broadcasted_iota(jnp.int32, (heads, CHUNK), 1)

    zy = tp_coords()
    z_first, y_first = n_blk, 2 * n_blk

    def load(k):
        src, dst = ((wx_ref, wx_s), (wbc_ref, wbc_s), (wz_ref, wz_s))[k]
        return pltpu.make_async_copy(src, dst, load_sem.at[k])

    n_chip = n_seq // 2
    chip, core = me // 2, lax.rem(me, 2)
    half = wo_ref.shape[0] // 2
    whole_rows = half - n_chip * SHARE

    def state_copy(k):
        far = n_chip - 1
        if k < far:
            d = k + 1
            src, slot = msg_s.at[jnp.where(chip + d < n_chip, 0, 1)], 2 * d
            dest = lax.rem(chip + d, n_chip) * 2 + core
        elif k < 2 * far:
            d = k - far + 1
            src, slot, dest = rcv_s.at[2 * d - 1], 2 * d + 1 - 2 * core, chip * 2 + 1 - core
        else:
            src, slot, dest = msg_s.at[core], jnp.where(core == 0, 1, n_seq - 1), chip * 2 + 1 - core
        return pltpu.make_async_remote_copy(
            src_ref=src, dst_ref=rcv_s.at[slot - 1], send_sem=send_sem.at[k], recv_sem=recv_sem.at[k],
            device_id={'sp': dest}, device_id_type=pl.DeviceIdType.MESH)

    def span(shared, everyone=False):
        at = core * half
        if not shared:
            return at, whole_rows
        if everyone:
            return at + whole_rows, n_chip * SHARE
        return at + whole_rows + chip * SHARE, SHARE

    def weight_copy(k, src, slot, at, size, dest):
        rows_at = pl.ds(pl.multiple_of(at, 8), size)
        return pltpu.make_async_remote_copy(
            src_ref=src.at[rows_at, :], dst_ref=wg_ref.at[slot, rows_at, :], send_sem=ws_sem.at[k], recv_sem=wr_sem.at[k],
            device_id=dest, device_id_type=pl.DeviceIdType.MESH)

    def ring_copies(hop):
        out = []
        for axis in range(2):
            for back in range(2):
                dist = RING - 1 if back else 1
                for shared in range(2):
                    at, size = span(shared)
                    k = ((hop * 2 + axis) * 2 + back) * 2 + shared
                    dest = {'tp': ring_peer(zy, axis, dist)}
                    if hop == 0:
                        out.append(weight_copy(k, wo_ref, axis * 3 + dist - 1, at, size, dest))
                    else:
                        out.append(weight_copy(k, wg_ref.at[axis * 3 + dist - 1], axis * 3 + 1, at + back * (size // 2), size // 2, dest))
        return out

    near, opposite = (0, 2, 3, 5), (1, 4)

    def along_x(slots):
        at, size = span(1)
        return [weight_copy(16 + slot * (n_chip - 1) + d - 1, wg_ref.at[slot], slot, at, size, {'sp': lax.rem(chip + d, n_chip) * 2 + core})
                for slot in slots for d in range(1, n_chip)]

    def to_partner(slots, shared):
        at, size = span(shared, everyone=True)
        first = 16 + 6 * (n_chip - 1)
        return [weight_copy(first + slot * 2 + shared, wg_ref.at[slot], slot, at, size, {'sp': chip * 2 + 1 - core}) for slot in slots]

    def start(copies):
        for c in copies:
            c.start()

    def wait(copies):
        for c in copies:
            c.wait()

    def gate_copy(side, dist, group, at):
        return pltpu.make_async_remote_copy(
            src_ref=z_s.at[pl.ds(at, CHUNK), :], dst_ref=ga_ref.at[side, dist, pl.ds(pl.multiple_of(group * CHUNK, CHUNK), CHUNK), :],
            send_sem=gs_sem.at[side, dist, group], recv_sem=gr_sem.at[side, dist, group],
            device_id={'tp': ring_peer(zy, side, dist)}, device_id_type=pl.DeviceIdType.MESH)

    def own_copy(side, group, at):
        return pltpu.make_async_copy(z_s.at[pl.ds(at, CHUNK), :], ga_ref.at[side, 0, pl.ds(pl.multiple_of(group * CHUNK, CHUNK), CHUNK), :],
                                     own_sem.at[side, group])

    @pl.when(i == 0)
    def _():
        barrier = pltpu.get_barrier_semaphore()
        for k in range(3):
            load(k).start()
        for s in range(1, n_seq):
            pl.semaphore_signal(barrier, inc=1, device_id={'sp': lax.rem(me + s, n_seq)}, device_id_type=pl.DeviceIdType.MESH)
        for axis in range(2):
            for dist in range(1, RING):
                pl.semaphore_signal(barrier, inc=1, device_id={'tp': ring_peer(zy, axis, dist)}, device_id_type=pl.DeviceIdType.MESH)
        pl.semaphore_wait(barrier, n_seq - 1 + 2 * (RING - 1))
        start(ring_copies(0))
        head = lax.broadcasted_iota(jnp.int32, bias_ref.shape, 0)
        owner = lax.broadcasted_iota(jnp.int32, skip_ref.shape, 1) // head_dim
        bias, aneg, skip = jnp.zeros_like(bias_ref), jnp.zeros_like(aneg_ref), jnp.zeros_like(skip_ref)
        for h in range(heads):
            bias = jnp.where(head == h, bias_sm[h], bias)
            aneg = jnp.where(head == h, aneg_sm[h], aneg)
            skip = jnp.where(owner == h, 2.0 * skip_sm[h], skip)
        bias_ref[...] = bias
        aneg_ref[...] = aneg
        skip_ref[...] = skip
        k = lax.broadcasted_iota(jnp.int32, e_s.shape, 0)
        j = lax.broadcasted_iota(jnp.int32, e_s.shape, 1)
        hit = (k // (3 * heads) == j // inner) & (k % heads == (j % inner) // head_dim)
        e_s[...] = jnp.where(hit, 1.0, 0.0).astype(bf16)
        f_s[...] = jnp.zeros_like(f_s)
        g_s[...] = jnp.zeros_like(g_s)
        lt_s[...] = jnp.zeros_like(lt_s)
        load(0).wait()
        load(1).wait()

    @pl.when(i < n_blk)
    def _():
        base = pl.multiple_of(i * rows, rows)
        xb = x_ref[...]
        raw = lax.dot_general(wdt_ref[...], xb, (((1,), (1,)), ((), ())), preferred_element_type=f32)
        bc_s[pl.ds(base, rows), :] = jnp.dot(xb, wbc_s[...], preferred_element_type=f32).astype(bf16)
        u_s[pl.ds(base, rows), :] = jnp.dot(xb, wx_s[...], preferred_element_type=f32).astype(bf16)
        for c in range(per_blk):
            cc = i * per_blk + c
            at = pl.multiple_of(base + c * CHUNK, CHUNK)
            dt = softplus(raw[:, c * CHUNK:(c + 1) * CHUNK] + bias_ref[...])
            la = dt * aneg_ref[...]
            ci = cumsum_lanes(la, lane)
            ce = ci - la
            end = jnp.broadcast_to(ci[:, CHUNK - 1:], ci.shape)
            dt_s[cc] = dt
            ci_s[cc] = ci
            ce_s[cc] = ce
            q = spread_operand([jnp.exp(end - ci) * dt, jnp.exp(ce) * dt, end], CHUNK)
            w = jnp.dot(q, e_s[:, :2 * inner], preferred_element_type=f32)
            le = jnp.dot(q[:16], e_s[:, 2 * inner:], preferred_element_type=f32)[:8]
            le_s[cc] = le
            u = u_s[pl.ds(at, CHUNK), :].astype(f32)
            b = bc_s[pl.ds(at, CHUNK), :n_state]
            dims = (((0,), (0,)), ((), ()))
            sf = lax.dot_general(b, (u * w[:, :inner]).astype(bf16), dims, preferred_element_type=f32)
            sb = lax.dot_general(b, (u * w[:, inner:]).astype(bf16), dims, preferred_element_type=f32)
            sf_s[cc] = sf
            sb_s[cc] = sb
            lt = lt_s[...]
            f_s[...] = f_s[...] * jnp.exp(le[:1]) + sf
            g_s[...] = g_s[...] + jnp.exp(lt[:1]) * sb
            lt_s[...] = lt + le

    @pl.when(i == n_blk - 1)
    def _():
        lt = lt_s[:1]
        parts = split3(lt)
        row = lax.broadcasted_iota(jnp.int32, (MSG_PAD, inner), 0)
        tail = jnp.where(row == 0, parts[0], jnp.where(row == 1, parts[1], jnp.where(row == 2, parts[2], 0.0))).astype(bf16)
        for side, ref in ((0, f_s), (1, g_s)):
            msg_s[side, :n_state, :] = ref[...].astype(bf16)
            msg_s[side, n_state:, :] = tail
        start([state_copy(k) for k in (*range(n_chip - 1), 2 * n_chip - 2)])

    @pl.when(i == z_first)
    def _():
        load(2).wait()

    @pl.when((i >= z_first) & (i < y_first))
    def _():
        base = pl.multiple_of((i - z_first) * rows, rows)
        z_s[pl.ds(base, rows), :] = jnp.dot(x_ref[...], wz_s[...], preferred_element_type=f32).astype(bf16)

    @pl.when(i == z_first + n_blk // 4)
    def _():
        wait(ring_copies(0))
        start(ring_copies(1) + along_x(near) + to_partner(near, 0))

    @pl.when(i == z_first + n_blk // 2 + 1)
    def _():
        wait([state_copy(k) for k in range(n_chip - 1)])
        start([state_copy(k) for k in range(n_chip - 1, 2 * n_chip - 2)])

    @pl.when(i == y_first)
    def _():
        wait([state_copy(k) for k in range(n_chip - 1, 2 * n_chip - 1)])

        def log_of(s):
            t = rcv_s[s - 1, n_state:, :].astype(f32)
            return t[0:1] + t[1:2] + t[2:3]

        f_s[...] = jnp.zeros_like(f_s)
        g_s[...] = jnp.zeros_like(g_s)
        acc = jnp.zeros((1, inner), f32)
        for s in range(1, n_seq):
            wgt = jnp.where(s <= me, jnp.exp(acc), 0.0)
            f_s[...] += wgt * rcv_s[s - 1, :n_state, :].astype(f32)
            acc = acc + log_of(s)
        acc = jnp.zeros((1, inner), f32)
        for s in range(n_seq - 1, 0, -1):
            wgt = jnp.where(s > me, jnp.exp(acc), 0.0)
            g_s[...] += wgt * rcv_s[s - 1, :n_state, :].astype(f32)
            acc = acc + log_of(s)

        n_ch = n_blk * per_blk

        def sweep(t, _):
            for ref, state, c in ((sf_s, f_s, t), (sb_s, g_s, n_ch - 1 - t)):
                mine = ref[c]
                before = state[...]
                ref[c] = before
                state[...] = before * jnp.exp(le_s[c][:1]) + mine
            return 0

        lax.fori_loop(0, n_ch, sweep, 0)

    @pl.when(i >= y_first)
    def _():
        step = i - y_first
        blk = 2 * lax.rem(zy[0] + 1 + step // 2, RING) + lax.rem(step + 1 - zy[1] // 2, 2)
        base = pl.multiple_of(blk * rows, rows)
        trow = lax.broadcasted_iota(jnp.int32, (CHUNK, CHUNK), 0)
        tcol = lax.broadcasted_iota(jnp.int32, (CHUNK, CHUNK), 1)
        later = trow > tcol
        left = tcol < head_dim
        twice = jnp.where(trow == tcol, 2.0, 1.0)
        for c in range(per_blk):
            cc = blk * per_blk + c
            at = pl.multiple_of(base + c * CHUNK, CHUNK)
            dt, ci, ce = dt_s[cc], ci_s[cc], ce_s[cc]
            end = jnp.broadcast_to(ci[:, CHUNK - 1:], ci.shape)
            q = spread_operand([dt, jnp.exp(ci), jnp.exp(end - ce)], CHUNK)
            col = jnp.concatenate([ci, ce, jnp.zeros((CHUNK - 2 * heads, CHUNK), f32)], axis=0).T
            b = bc_s[pl.ds(at, CHUNK), :n_state]
            cm = bc_s[pl.ds(at, CHUNK), n_state:]
            gram = lax.dot_general(cm, b, (((1,), (1,)), ((), ())), preferred_element_type=f32) * twice
            for lo in range(0, inner, SPAN):
                here = slice(lo, lo + SPAN)
                u = u_s[pl.ds(at, CHUNK), here].astype(f32)
                wdt = jnp.dot(q, e_s[:, here], preferred_element_type=f32)
                udt = (u * wdt).astype(bf16)
                outs = []
                for p in range(lo // CHUNK, (lo + SPAN) // CHUNK):
                    mats = []
                    for h in (2 * p, 2 * p + 1):
                        d = jnp.where(later, col[:, h:h + 1] - ci[h:h + 1, :], ce[h:h + 1, :] - col[:, heads + h:heads + h + 1])
                        mats.append((gram * jnp.exp(jnp.minimum(d, 0.0))).astype(bf16))
                    up = udt[:, p * CHUNK - lo:(p + 1) * CHUNK - lo]
                    zero = jnp.zeros_like(up)
                    rhs = jnp.concatenate([jnp.where(left, up, zero), jnp.where(left, zero, up)], axis=0)
                    outs.append(jnp.dot(jnp.concatenate(mats, axis=1), rhs, preferred_element_type=f32))
                y = jnp.concatenate(outs, axis=1) if len(outs) > 1 else outs[0]
                for ref, first in ((sf_s, inner), (sb_s, 2 * inner)):
                    grown = jnp.dot(q, e_s[:, first + lo:first + lo + SPAN], preferred_element_type=f32)
                    y = y + jnp.dot(cm, ref[cc, :, here].astype(bf16), preferred_element_type=f32) * grown
                y = y + skip_ref[:, here] * u
                z = z_s[pl.ds(at, CHUNK), here].astype(f32)
                z_s[pl.ds(at, CHUNK), here] = (y * (z / (1.0 + jnp.exp(-z)))).astype(bf16)
        for c in range(per_blk):
            at = pl.multiple_of(base + c * CHUNK, CHUNK)
            side = c % 2
            owner = blk * (per_blk // 2) + c // 2
            far = (lax.rem(owner // RING - zy[0] + RING, RING), lax.rem(lax.rem(owner, RING) - zy[1] + RING, RING))
            dist, group = (far[1], far[0]) if side == 0 else (far[0], far[1])

            @pl.when(dist == 0)
            def _():
                own_copy(side, group, at).start()

            @pl.when(dist > 0)
            def _():
                gate_copy(side, dist, group, at).start()

    @pl.when(i == y_first + n_blk // 4)
    def _():
        wait(ring_copies(1))
        start(along_x(opposite) + to_partner(opposite, 0))

    @pl.when(i == y_first + 3 * n_blk // 4)
    def _():
        wait(along_x(near + opposite))
        start(to_partner(near + opposite, 1))

    @pl.when(i == 3 * n_blk - 1)
    def _():
        for side in range(2):
            for group in range(RING):
                own_copy(side, group, 0).wait()
                for dist in range(1, RING):
                    gate_copy(side, dist, group, 0).wait()
        wait(to_partner(near + opposite, 0) + to_partner(near + opposite, 1))


def scan_call(x_blk, w_z, w_x, w_bc, w_dt, a_neg, dt_bias, d_skip, w_out, n_seq):
    tokens, d_model = x_blk.shape
    heads = a_neg.shape[0]
    inner = w_x.shape[1]
    head_dim = inner // heads
    n_state = w_bc.shape[1] // 2
    rows = min(512, tokens)
    n_blk = tokens // rows
    n_ch = tokens // CHUNK
    n_copies = 16 + 6 * (n_seq // 2 - 1) + 12
    w_dt = w_dt.T
    f32, bf16 = jnp.float32, jnp.bfloat16

    def whole(a):
        return pl.BlockSpec(a.shape, lambda i: (0, 0), pipeline_mode=pl.Buffered(1))

    return pl.pallas_call(
        functools.partial(scan_kernel, n_blk, n_seq, heads, head_dim),
        grid=(3 * n_blk,),
        out_shape=(jax.ShapeDtypeStruct((2, RING, tokens // (2 * RING), inner), bf16),
                   jax.ShapeDtypeStruct((2 * (RING - 1),) + w_out.shape, bf16)),
        in_specs=[pl.BlockSpec((rows, d_model), lambda i: (jnp.where(i < n_blk, i, jnp.minimum(i - n_blk, n_blk - 1)), 0)),
                  pl.BlockSpec(memory_space=pl.ANY), pl.BlockSpec(memory_space=pl.ANY), pl.BlockSpec(memory_space=pl.ANY), whole(w_dt)]
        + [pl.BlockSpec(memory_space=pltpu.SMEM)] * 3 + [pl.BlockSpec(memory_space=pl.ANY)],
        out_specs=(pl.BlockSpec(memory_space=pl.ANY), pl.BlockSpec(memory_space=pl.ANY)),
        scratch_shapes=[
            pltpu.VMEM((tokens, inner), bf16),
            pltpu.VMEM((tokens, inner), bf16),
            pltpu.VMEM((tokens, 2 * n_state), bf16),
            pltpu.VMEM((n_ch, n_state, inner), f32),
            pltpu.VMEM((n_ch, n_state, inner), f32),
            pltpu.VMEM((n_state, inner), f32),
            pltpu.VMEM((n_state, inner), f32),
            pltpu.VMEM((n_ch, heads, CHUNK), f32),
            pltpu.VMEM((n_ch, heads, CHUNK), f32),
            pltpu.VMEM((n_ch, heads, CHUNK), f32),
            pltpu.VMEM((n_ch, 8, inner), f32),
            pltpu.VMEM((8, inner), f32),
            pltpu.VMEM((CHUNK, 3 * inner), bf16),
            pltpu.VMEM((2, n_state + MSG_PAD, inner), bf16),
            pltpu.VMEM((n_seq - 1, n_state + MSG_PAD, inner), bf16),
            pltpu.VMEM((heads, CHUNK), f32),
            pltpu.VMEM((heads, CHUNK), f32),
            pltpu.VMEM((1, inner), f32),
            pltpu.VMEM(w_x.shape, bf16),
            pltpu.VMEM(w_bc.shape, bf16),
            pltpu.VMEM(w_z.shape, bf16),
            pltpu.SemaphoreType.DMA((3,)),
            pltpu.SemaphoreType.DMA((n_seq - 1,)),
            pltpu.SemaphoreType.DMA((n_seq - 1,)),
            pltpu.SemaphoreType.DMA((n_copies,)),
            pltpu.SemaphoreType.DMA((n_copies,)),
            pltpu.SemaphoreType.DMA((2, RING, RING)),
            pltpu.SemaphoreType.DMA((2, RING, RING)),
            pltpu.SemaphoreType.DMA((2, RING)),
        ],
        compiler_params=pltpu.CompilerParams(collective_id=0, has_side_effects=True, vmem_limit_bytes=60 * 1024 * 1024,
                                             dimension_semantics=('arbitrary',)),
        cost_estimate=pl.CostEstimate(flops=2 * tokens * d_model * (2 * inner + 3 * n_state) * 3, bytes_accessed=60 << 20, transcendentals=0),
    )(x_blk, w_z, w_x, w_bc, w_dt, dt_bias, a_neg, d_skip, w_out)


def out_kernel(n_col, ga_ref, wo_ref, wg_ref, x_ref, out_ref, send_s, recv_s, own_s, near_s, x_s, x_sem, send_sem, recv_sem):
    i = pl.program_id(0)
    zy = tp_coords()
    width = wo_ref.shape[1]
    f32, bf16 = jnp.float32, jnp.bfloat16
    relay, direct, joined = range(3)

    def part_copy(kind, side, b):
        dist = 1 + 2 * lax.rem(b, 2)
        if kind == direct:
            dist = RING - dist
        return pltpu.make_async_remote_copy(
            src_ref=send_s.at[kind, side, b], dst_ref=recv_s.at[kind, side, b],
            send_sem=send_sem.at[kind, side, b], recv_sem=recv_sem.at[kind, side, b],
            device_id={'tp': ring_peer(zy, 1 - side, dist)}, device_id_type=pl.DeviceIdType.MESH)

    def x_copy():
        rows = x_s.shape[0]
        at = pl.multiple_of(lax.axis_index('tp') * rows, rows)
        return pltpu.make_async_copy(x_ref.at[pl.ds(at, rows), :], x_s, x_sem)

    @pl.when(i == 0)
    def _():
        x_copy().start()
        barrier = pltpu.get_barrier_semaphore()
        for axis in range(2):
            for dist in (1, RING - 1):
                pl.semaphore_signal(barrier, inc=1, device_id={'tp': ring_peer(zy, axis, dist)}, device_id_type=pl.DeviceIdType.MESH)

    @pl.when(i < n_col)
    def _():
        right = lax.rem(i, 2) == 0
        for side in range(2):
            acc = jnp.dot(ga_ref[side, 0], wo_ref[...], preferred_element_type=f32)
            for dist in range(1, RING):
                acc = acc + jnp.dot(ga_ref[side, dist], wg_ref[side * 3 + dist - 1], preferred_element_type=f32)
            one, two, three = (acc[dist * CHUNK:(dist + 1) * CHUNK] for dist in range(1, RING))
            own_s[side, i] = acc[:CHUNK]
            send_s[relay, side, i] = two.astype(bf16)
            send_s[direct, side, i] = jnp.where(right, three, one).astype(bf16)
            near_s[side, i] = jnp.where(right, one, three)

    @pl.when(i == 0)
    def _():
        pl.semaphore_wait(pltpu.get_barrier_semaphore(), 4)

    @pl.when(i < n_col)
    def _():
        for kind in (relay, direct):
            for side in range(2):
                part_copy(kind, side, i).start()

    @pl.when((i >= LAG) & (i < n_col + LAG))
    def _():
        b = i - LAG
        for side in range(2):
            part_copy(relay, side, b).wait_recv()
            send_s[joined, side, b] = (near_s[side, b] + recv_s[relay, side, b].astype(f32)).astype(bf16)
        for side in range(2):
            part_copy(joined, side, b).start()

    @pl.when(i == n_col + LAG)
    def _():
        x_copy().wait()

    @pl.when(i >= n_col + LAG)
    def _():
        b = i - n_col - LAG
        cols = pl.ds(pl.multiple_of(b * width, width), width)
        for side in range(2):
            part_copy(relay, side, b).wait_send()
            part_copy(direct, side, b).wait()
            part_copy(joined, side, b).wait()
            acc = own_s[side, b] + recv_s[direct, side, b].astype(f32) + recv_s[joined, side, b].astype(f32)
            at = side * CHUNK
            out_ref[at:at + CHUNK, :] = (x_s[at:at + CHUNK, cols].astype(f32) + acc).astype(bf16)


def out_call(g_all, w_out, w_got, x_blk):
    inner, d_model = w_out.shape
    rows = 2 * CHUNK
    width = min(512, d_model)
    n_col = d_model // width
    f32, bf16 = jnp.float32, jnp.bfloat16

    def column(i):
        return jnp.minimum(i, n_col - 1)

    return pl.pallas_call(
        functools.partial(out_kernel, n_col),
        grid=(2 * n_col + LAG,),
        out_shape=jax.ShapeDtypeStruct((rows, d_model), bf16),
        in_specs=[pl.BlockSpec(g_all.shape, lambda i: (0, 0, 0, 0), pipeline_mode=pl.Buffered(1)),
                  pl.BlockSpec((inner, width), lambda i: (0, column(i))),
                  pl.BlockSpec((2 * (RING - 1), inner, width), lambda i: (0, 0, column(i))),
                  pl.BlockSpec(memory_space=pl.ANY)],
        out_specs=pl.BlockSpec((rows, width), lambda i: (0, jnp.maximum(i - n_col - LAG, 0))),
        scratch_shapes=[
            pltpu.VMEM((3, 2, n_col, CHUNK, width), bf16),
            pltpu.VMEM((3, 2, n_col, CHUNK, width), bf16),
            pltpu.VMEM((2, n_col, CHUNK, width), f32),
            pltpu.VMEM((2, n_col, CHUNK, width), f32),
            pltpu.VMEM((rows, d_model), bf16),
            pltpu.SemaphoreType.DMA,
            pltpu.SemaphoreType.DMA((3, 2, n_col)),
            pltpu.SemaphoreType.DMA((3, 2, n_col)),
        ],
        compiler_params=pltpu.CompilerParams(collective_id=1, has_side_effects=True, vmem_limit_bytes=60 * 1024 * 1024,
                                             dimension_semantics=('arbitrary',)),
        cost_estimate=pl.CostEstimate(flops=2 * 2 * 4 * CHUNK * 4 * inner * d_model, bytes_accessed=40 << 20, transcendentals=0),
    )(g_all, w_out, w_got, x_blk)


def solution(mesh):
    n_seq = mesh.shape['sp']

    def device_fn(x_blk, w_z, w_x, w_bc, w_dt, a_neg, dt_bias, d_skip, w_out):
        g_all, w_got = scan_call(x_blk, w_z, w_x, w_bc, w_dt, a_neg, dt_bias, d_skip, w_out, n_seq)
        return out_call(g_all, w_out, w_got, x_blk)

    in_specs = (P(('dp', 'sp'), None), P(None, 'tp'), P(None, 'tp'), P(None, None), P(None, 'tp'), P('tp'), P('tp'), P('tp'), P('tp', None))
    out_specs = P(('dp', 'sp', 'tp'), None)
    return jax.shard_map(device_fn, mesh=mesh, in_specs=in_specs, out_specs=out_specs, check_vma=False)
```

```python
import functools

import jax
import jax.numpy as jnp
from jax import lax
from jax.experimental import pallas as pl
from jax.experimental.pallas import tpu as pltpu
from jax.sharding import PartitionSpec as P

CHUNK = 128
MSG_PAD = 16
RING = 4
SHARE = 16
LAG = 5
SPAN = 256


def split3(v):
    hi = v.astype(jnp.bfloat16).astype(jnp.float32)
    rest = v - hi
    mid = rest.astype(jnp.bfloat16).astype(jnp.float32)
    return [hi, mid, rest - mid]


def spread_operand(quantities, width):
    rows = [part for q in quantities for part in split3(q)]
    have = sum(r.shape[0] for r in rows)
    rows.append(jnp.zeros((CHUNK - have, width), jnp.float32))
    return jnp.concatenate(rows, axis=0).T.astype(jnp.bfloat16)


def cumsum_lanes(v, lane):
    step = 1
    while step < v.shape[1]:
        v = v + jnp.where(lane >= step, pltpu.roll(v, step, 1), 0.0)
        step *= 2
    return v


def softplus(v):
    return jnp.maximum(v, 0.0) + jnp.log1p(jnp.exp(-jnp.abs(v)))


def tp_coords():
    index = lax.axis_index('tp')
    return index // RING, lax.rem(index, RING)


def ring_peer(zy, axis, dist):
    z, y = zy
    if axis == 0:
        return z * RING + lax.rem(y + dist, RING)
    return lax.rem(z + dist, RING) * RING + y


def scan_kernel(n_blk, n_seq, heads, head_dim, x_ref, wz_ref, wx_ref, wbc_ref, wdt_ref, bias_sm, aneg_sm, skip_sm, wo_ref, ga_ref, wg_ref,
                z_s, u_s, bc_s, sf_s, sb_s, f_s, g_s, dt_s, ci_s, ce_s, le_s, lt_s, e_s, msg_s, rcv_s, bias_ref, aneg_ref, skip_ref, wx_s, wbc_s, wz_s, load_sem, send_sem, recv_sem, ws_sem, wr_sem, gs_sem, gr_sem, own_sem):
    i = pl.program_id(0)
    me = lax.axis_index('sp')
    rows = x_ref.shape[0]
    inner = heads * head_dim
    per_blk = rows // CHUNK
    n_state = bc_s.shape[1] // 2
    f32, bf16 = jnp.float32, jnp.bfloat16
    lane = lax.broadcasted_iota(jnp.int32, (heads, CHUNK), 1)

    zy = tp_coords()
    z_first, y_first = n_blk, 2 * n_blk

    def load(k):
        src, dst = ((wx_ref, wx_s), (wbc_ref, wbc_s), (wz_ref, wz_s))[k]
        return pltpu.make_async_copy(src, dst, load_sem.at[k])

    n_chip = n_seq // 2
    chip, core = me // 2, lax.rem(me, 2)
    half = wo_ref.shape[0] // 2
    whole_rows = half - n_chip * SHARE

    def state_copy(k):
        far = n_chip - 1
        if k < far:
            d = k + 1
            src, slot = msg_s.at[jnp.where(chip + d < n_chip, 0, 1)], 2 * d
            dest = lax.rem(chip + d, n_chip) * 2 + core
        elif k < 2 * far:
            d = k - far + 1
            src, slot, dest = rcv_s.at[2 * d - 1], 2 * d + 1 - 2 * core, chip * 2 + 1 - core
        else:
            src, slot, dest = msg_s.at[core], jnp.where(core == 0, 1, n_seq - 1), chip * 2 + 1 - core
        return pltpu.make_async_remote_copy(
            src_ref=src, dst_ref=rcv_s.at[slot - 1], send_sem=send_sem.at[k], recv_sem=recv_sem.at[k],
            device_id={'sp': dest}, device_id_type=pl.DeviceIdType.MESH)

    def span(shared, everyone=False):
        at = core * half
        if not shared:
            return at, whole_rows
        if everyone:
            return at + whole_rows, n_chip * SHARE
        return at + whole_rows + chip * SHARE, SHARE

    def weight_copy(k, src, slot, at, size, dest):
        rows_at = pl.ds(pl.multiple_of(at, 8), size)
        return pltpu.make_async_remote_copy(
            src_ref=src.at[rows_at, :], dst_ref=wg_ref.at[slot, rows_at, :], send_sem=ws_sem.at[k], recv_sem=wr_sem.at[k],
            device_id=dest, device_id_type=pl.DeviceIdType.MESH)

    def ring_copies(hop):
        out = []
        for axis in range(2):
            for back in range(2):
                dist = RING - 1 if back else 1
                for shared in range(2):
                    at, size = span(shared)
                    k = ((hop * 2 + axis) * 2 + back) * 2 + shared
                    dest = {'tp': ring_peer(zy, axis, dist)}
                    if hop == 0:
                        out.append(weight_copy(k, wo_ref, axis * 3 + dist - 1, at, size, dest))
                    else:
                        out.append(weight_copy(k, wg_ref.at[axis * 3 + dist - 1], axis * 3 + 1, at + back * (size // 2), size // 2, dest))
        return out

    near, opposite = (0, 2, 3, 5), (1, 4)

    def along_x(slots):
        at, size = span(1)
        return [weight_copy(16 + slot * (n_chip - 1) + d - 1, wg_ref.at[slot], slot, at, size, {'sp': lax.rem(chip + d, n_chip) * 2 + core})
                for slot in slots for d in range(1, n_chip)]

    def to_partner(slots, shared):
        at, size = span(shared, everyone=True)
        first = 16 + 6 * (n_chip - 1)
        return [weight_copy(first + slot * 2 + shared, wg_ref.at[slot], slot, at, size, {'sp': chip * 2 + 1 - core}) for slot in slots]

    def start(copies):
        for c in copies:
            c.start()

    def wait(copies):
        for c in copies:
            c.wait()

    def gate_copy(side, dist, group, at):
        return pltpu.make_async_remote_copy(
            src_ref=z_s.at[pl.ds(at, CHUNK), :], dst_ref=ga_ref.at[side, dist, pl.ds(pl.multiple_of(group * CHUNK, CHUNK), CHUNK), :],
            send_sem=gs_sem.at[side, dist, group], recv_sem=gr_sem.at[side, dist, group],
            device_id={'tp': ring_peer(zy, side, dist)}, device_id_type=pl.DeviceIdType.MESH)

    def own_copy(side, group, at):
        return pltpu.make_async_copy(z_s.at[pl.ds(at, CHUNK), :], ga_ref.at[side, 0, pl.ds(pl.multiple_of(group * CHUNK, CHUNK), CHUNK), :],
                                     own_sem.at[side, group])

    @pl.when(i == 0)
    def _():
        barrier = pltpu.get_barrier_semaphore()
        for k in range(3):
            load(k).start()
        for s in range(1, n_seq):
            pl.semaphore_signal(barrier, inc=1, device_id={'sp': lax.rem(me + s, n_seq)}, device_id_type=pl.DeviceIdType.MESH)
        for axis in range(2):
            for dist in range(1, RING):
                pl.semaphore_signal(barrier, inc=1, device_id={'tp': ring_peer(zy, axis, dist)}, device_id_type=pl.DeviceIdType.MESH)
        pl.semaphore_wait(barrier, n_seq - 1 + 2 * (RING - 1))
        start(ring_copies(0))
        head = lax.broadcasted_iota(jnp.int32, bias_ref.shape, 0)
        owner = lax.broadcasted_iota(jnp.int32, skip_ref.shape, 1) // head_dim
        bias, aneg, skip = jnp.zeros_like(bias_ref), jnp.zeros_like(aneg_ref), jnp.zeros_like(skip_ref)
        for h in range(heads):
            bias = jnp.where(head == h, bias_sm[h], bias)
            aneg = jnp.where(head == h, aneg_sm[h], aneg)
            skip = jnp.where(owner == h, 2.0 * skip_sm[h], skip)
        bias_ref[...] = bias
        aneg_ref[...] = aneg
        skip_ref[...] = skip
        k = lax.broadcasted_iota(jnp.int32, e_s.shape, 0)
        j = lax.broadcasted_iota(jnp.int32, e_s.shape, 1)
        hit = (k // (3 * heads) == j // inner) & (k % heads == (j % inner) // head_dim)
        e_s[...] = jnp.where(hit, 1.0, 0.0).astype(bf16)
        f_s[...] = jnp.zeros_like(f_s)
        g_s[...] = jnp.zeros_like(g_s)
        lt_s[...] = jnp.zeros_like(lt_s)
        load(0).wait()
        load(1).wait()

    @pl.when(i < n_blk)
    def _():
        base = pl.multiple_of(i * rows, rows)
        xb = x_ref[...]
        raw = lax.dot_general(xb, wdt_ref[...], (((1,), (1,)), ((), ())), preferred_element_type=f32)
        bc_s[pl.ds(base, rows), :] = jnp.dot(xb, wbc_s[...], preferred_element_type=f32).astype(bf16)
        u_s[pl.ds(base, rows), :] = jnp.dot(xb, wx_s[...], preferred_element_type=f32).astype(bf16)
        for c in range(per_blk):
            cc = i * per_blk + c
            at = pl.multiple_of(base + c * CHUNK, CHUNK)
            dt = softplus(raw[c * CHUNK:(c + 1) * CHUNK, :].T + bias_ref[...])
            la = dt * aneg_ref[...]
            ci = cumsum_lanes(la, lane)
            ce = ci - la
            end = jnp.broadcast_to(ci[:, CHUNK - 1:], ci.shape)
            dt_s[cc] = dt
            ci_s[cc] = ci
            ce_s[cc] = ce
            q = spread_operand([jnp.exp(end - ci) * dt, jnp.exp(ce) * dt, end], CHUNK)
            w = jnp.dot(q, e_s[:, :2 * inner], preferred_element_type=f32)
            le = jnp.dot(q[:16], e_s[:, 2 * inner:], preferred_element_type=f32)[:8]
            le_s[cc] = le
            u = u_s[pl.ds(at, CHUNK), :].astype(f32)
            b = bc_s[pl.ds(at, CHUNK), :n_state]
            dims = (((0,), (0,)), ((), ()))
            sf = lax.dot_general(b, (u * w[:, :inner]).astype(bf16), dims, preferred_element_type=f32)
            sb = lax.dot_general(b, (u * w[:, inner:]).astype(bf16), dims, preferred_element_type=f32)
            sf_s[cc] = sf
            sb_s[cc] = sb
            lt = lt_s[...]
            f_s[...] = f_s[...] * jnp.exp(le[:1]) + sf
            g_s[...] = g_s[...] + jnp.exp(lt[:1]) * sb
            lt_s[...] = lt + le

    @pl.when(i == n_blk - 1)
    def _():
        lt = lt_s[:1]
        parts = split3(lt)
        row = lax.broadcasted_iota(jnp.int32, (MSG_PAD, inner), 0)
        tail = jnp.where(row == 0, parts[0], jnp.where(row == 1, parts[1], jnp.where(row == 2, parts[2], 0.0))).astype(bf16)
        for side, ref in ((0, f_s), (1, g_s)):
            msg_s[side, :n_state, :] = ref[...].astype(bf16)
            msg_s[side, n_state:, :] = tail
        start([state_copy(k) for k in (*range(n_chip - 1), 2 * n_chip - 2)])

    @pl.when(i == z_first)
    def _():
        load(2).wait()

    @pl.when((i >= z_first) & (i < y_first))
    def _():
        base = pl.multiple_of((i - z_first) * rows, rows)
        z_s[pl.ds(base, rows), :] = jnp.dot(x_ref[...], wz_s[...], preferred_element_type=f32).astype(bf16)

    @pl.when(i == z_first + n_blk // 4)
    def _():
        wait(ring_copies(0))
        start(ring_copies(1) + along_x(near) + to_partner(near, 0))

    @pl.when(i == z_first + n_blk // 2 + 1)
    def _():
        wait([state_copy(k) for k in range(n_chip - 1)])
        start([state_copy(k) for k in range(n_chip - 1, 2 * n_chip - 2)])

    @pl.when(i == y_first)
    def _():
        wait([state_copy(k) for k in range(n_chip - 1, 2 * n_chip - 1)])

        def log_of(s):
            t = rcv_s[s - 1, n_state:, :].astype(f32)
            return t[0:1] + t[1:2] + t[2:3]

        f_s[...] = jnp.zeros_like(f_s)
        g_s[...] = jnp.zeros_like(g_s)
        acc = jnp.zeros((1, inner), f32)
        for s in range(1, n_seq):
            wgt = jnp.where(s <= me, jnp.exp(acc), 0.0)
            f_s[...] += wgt * rcv_s[s - 1, :n_state, :].astype(f32)
            acc = acc + log_of(s)
        acc = jnp.zeros((1, inner), f32)
        for s in range(n_seq - 1, 0, -1):
            wgt = jnp.where(s > me, jnp.exp(acc), 0.0)
            g_s[...] += wgt * rcv_s[s - 1, :n_state, :].astype(f32)
            acc = acc + log_of(s)

        n_ch = n_blk * per_blk

        def sweep(t, _):
            for ref, state, c in ((sf_s, f_s, t), (sb_s, g_s, n_ch - 1 - t)):
                mine = ref[c]
                before = state[...]
                ref[c] = before
                state[...] = before * jnp.exp(le_s[c][:1]) + mine
            return 0

        lax.fori_loop(0, n_ch, sweep, 0)

    @pl.when(i >= y_first)
    def _():
        step = i - y_first
        blk = 2 * lax.rem(zy[0] + 1 + step // 2, RING) + lax.rem(step + 1 - zy[1] // 2, 2)
        base = pl.multiple_of(blk * rows, rows)
        trow = lax.broadcasted_iota(jnp.int32, (CHUNK, CHUNK), 0)
        tcol = lax.broadcasted_iota(jnp.int32, (CHUNK, CHUNK), 1)
        later = trow > tcol
        left = tcol < head_dim
        twice = jnp.where(trow == tcol, 2.0, 1.0)
        for c in range(per_blk):
            cc = blk * per_blk + c
            at = pl.multiple_of(base + c * CHUNK, CHUNK)
            dt, ci, ce = dt_s[cc], ci_s[cc], ce_s[cc]
            end = jnp.broadcast_to(ci[:, CHUNK - 1:], ci.shape)
            q = spread_operand([dt, jnp.exp(ci), jnp.exp(end - ce)], CHUNK)
            col = jnp.concatenate([ci, ce, jnp.zeros((CHUNK - 2 * heads, CHUNK), f32)], axis=0).T
            b = bc_s[pl.ds(at, CHUNK), :n_state]
            cm = bc_s[pl.ds(at, CHUNK), n_state:]
            gram = lax.dot_general(cm, b, (((1,), (1,)), ((), ())), preferred_element_type=f32) * twice
            for lo in range(0, inner, SPAN):
                here = slice(lo, lo + SPAN)
                u = u_s[pl.ds(at, CHUNK), here].astype(f32)
                wdt = jnp.dot(q, e_s[:, here], preferred_element_type=f32)
                udt = (u * wdt).astype(bf16)
                outs = []
                for p in range(lo // CHUNK, (lo + SPAN) // CHUNK):
                    mats = []
                    for h in (2 * p, 2 * p + 1):
                        d = jnp.where(later, col[:, h:h + 1] - ci[h:h + 1, :], ce[h:h + 1, :] - col[:, heads + h:heads + h + 1])
                        mats.append((gram * jnp.exp(jnp.minimum(d, 0.0))).astype(bf16))
                    up = udt[:, p * CHUNK - lo:(p + 1) * CHUNK - lo]
                    zero = jnp.zeros_like(up)
                    rhs = jnp.concatenate([jnp.where(left, up, zero), jnp.where(left, zero, up)], axis=0)
                    outs.append(jnp.dot(jnp.concatenate(mats, axis=1), rhs, preferred_element_type=f32))
                y = jnp.concatenate(outs, axis=1) if len(outs) > 1 else outs[0]
                for ref, first in ((sf_s, inner), (sb_s, 2 * inner)):
                    grown = jnp.dot(q, e_s[:, first + lo:first + lo + SPAN], preferred_element_type=f32)
                    y = y + jnp.dot(cm, ref[cc, :, here].astype(bf16), preferred_element_type=f32) * grown
                y = y + skip_ref[:, here] * u
                z = z_s[pl.ds(at, CHUNK), here].astype(f32)
                z_s[pl.ds(at, CHUNK), here] = (y * (z / (1.0 + jnp.exp(-z)))).astype(bf16)
        for c in range(per_blk):
            at = pl.multiple_of(base + c * CHUNK, CHUNK)
            side = c % 2
            owner = blk * (per_blk // 2) + c // 2
            far = (lax.rem(owner // RING - zy[0] + RING, RING), lax.rem(lax.rem(owner, RING) - zy[1] + RING, RING))
            dist, group = (far[1], far[0]) if side == 0 else (far[0], far[1])

            @pl.when(dist == 0)
            def _():
                own_copy(side, group, at).start()

            @pl.when(dist > 0)
            def _():
                gate_copy(side, dist, group, at).start()

    @pl.when(i == y_first + n_blk // 4)
    def _():
        wait(ring_copies(1))
        start(along_x(opposite) + to_partner(opposite, 0))

    @pl.when(i == y_first + 3 * n_blk // 4)
    def _():
        wait(along_x(near + opposite))
        start(to_partner(near + opposite, 1))

    @pl.when(i == 3 * n_blk - 1)
    def _():
        for side in range(2):
            for group in range(RING):
                own_copy(side, group, 0).wait()
                for dist in range(1, RING):
                    gate_copy(side, dist, group, 0).wait()
        wait(to_partner(near + opposite, 0) + to_partner(near + opposite, 1))


def scan_call(x_blk, w_z, w_x, w_bc, w_dt, a_neg, dt_bias, d_skip, w_out, n_seq):
    tokens, d_model = x_blk.shape
    heads = a_neg.shape[0]
    inner = w_x.shape[1]
    head_dim = inner // heads
    n_state = w_bc.shape[1] // 2
    rows = min(512, tokens)
    n_blk = tokens // rows
    n_ch = tokens // CHUNK
    n_copies = 16 + 6 * (n_seq // 2 - 1) + 12
    w_dt = w_dt.T
    f32, bf16 = jnp.float32, jnp.bfloat16

    def whole(a):
        return pl.BlockSpec(a.shape, lambda i: (0, 0), pipeline_mode=pl.Buffered(1))

    return pl.pallas_call(
        functools.partial(scan_kernel, n_blk, n_seq, heads, head_dim),
        grid=(3 * n_blk,),
        out_shape=(jax.ShapeDtypeStruct((2, RING, tokens // (2 * RING), inner), bf16),
                   jax.ShapeDtypeStruct((2 * (RING - 1),) + w_out.shape, bf16)),
        in_specs=[pl.BlockSpec((rows, d_model), lambda i: (jnp.where(i < n_blk, i, jnp.minimum(i - n_blk, n_blk - 1)), 0)),
                  pl.BlockSpec(memory_space=pl.ANY), pl.BlockSpec(memory_space=pl.ANY), pl.BlockSpec(memory_space=pl.ANY), whole(w_dt)]
        + [pl.BlockSpec(memory_space=pltpu.SMEM)] * 3 + [pl.BlockSpec(memory_space=pl.ANY)],
        out_specs=(pl.BlockSpec(memory_space=pl.ANY), pl.BlockSpec(memory_space=pl.ANY)),
        scratch_shapes=[
            pltpu.VMEM((tokens, inner), bf16),
            pltpu.VMEM((tokens, inner), bf16),
            pltpu.VMEM((tokens, 2 * n_state), bf16),
            pltpu.VMEM((n_ch, n_state, inner), f32),
            pltpu.VMEM((n_ch, n_state, inner), f32),
            pltpu.VMEM((n_state, inner), f32),
            pltpu.VMEM((n_state, inner), f32),
            pltpu.VMEM((n_ch, heads, CHUNK), f32),
            pltpu.VMEM((n_ch, heads, CHUNK), f32),
            pltpu.VMEM((n_ch, heads, CHUNK), f32),
            pltpu.VMEM((n_ch, 8, inner), f32),
            pltpu.VMEM((8, inner), f32),
            pltpu.VMEM((CHUNK, 3 * inner), bf16),
            pltpu.VMEM((2, n_state + MSG_PAD, inner), bf16),
            pltpu.VMEM((n_seq - 1, n_state + MSG_PAD, inner), bf16),
            pltpu.VMEM((heads, CHUNK), f32),
            pltpu.VMEM((heads, CHUNK), f32),
            pltpu.VMEM((1, inner), f32),
            pltpu.VMEM(w_x.shape, bf16),
            pltpu.VMEM(w_bc.shape, bf16),
            pltpu.VMEM(w_z.shape, bf16),
            pltpu.SemaphoreType.DMA((3,)),
            pltpu.SemaphoreType.DMA((n_seq - 1,)),
            pltpu.SemaphoreType.DMA((n_seq - 1,)),
            pltpu.SemaphoreType.DMA((n_copies,)),
            pltpu.SemaphoreType.DMA((n_copies,)),
            pltpu.SemaphoreType.DMA((2, RING, RING)),
            pltpu.SemaphoreType.DMA((2, RING, RING)),
            pltpu.SemaphoreType.DMA((2, RING)),
        ],
        compiler_params=pltpu.CompilerParams(collective_id=0, has_side_effects=True, vmem_limit_bytes=60 * 1024 * 1024,
                                             dimension_semantics=('arbitrary',)),
        cost_estimate=pl.CostEstimate(flops=2 * tokens * d_model * (2 * inner + 3 * n_state) * 3, bytes_accessed=60 << 20, transcendentals=0),
    )(x_blk, w_z, w_x, w_bc, w_dt, dt_bias, a_neg, d_skip, w_out)


def out_kernel(n_col, ga_ref, wo_ref, wg_ref, x_ref, out_ref, send_s, recv_s, own_s, near_s, x_s, x_sem, send_sem, recv_sem):
    i = pl.program_id(0)
    zy = tp_coords()
    width = wo_ref.shape[1]
    f32, bf16 = jnp.float32, jnp.bfloat16
    relay, direct, joined = range(3)

    def part_copy(kind, side, b):
        dist = 1 + 2 * lax.rem(b, 2)
        if kind == direct:
            dist = RING - dist
        return pltpu.make_async_remote_copy(
            src_ref=send_s.at[kind, side, b], dst_ref=recv_s.at[kind, side, b],
            send_sem=send_sem.at[kind, side, b], recv_sem=recv_sem.at[kind, side, b],
            device_id={'tp': ring_peer(zy, 1 - side, dist)}, device_id_type=pl.DeviceIdType.MESH)

    def x_copy():
        rows = x_s.shape[0]
        at = pl.multiple_of(lax.axis_index('tp') * rows, rows)
        return pltpu.make_async_copy(x_ref.at[pl.ds(at, rows), :], x_s, x_sem)

    @pl.when(i == 0)
    def _():
        x_copy().start()
        barrier = pltpu.get_barrier_semaphore()
        for axis in range(2):
            for dist in (1, RING - 1):
                pl.semaphore_signal(barrier, inc=1, device_id={'tp': ring_peer(zy, axis, dist)}, device_id_type=pl.DeviceIdType.MESH)

    @pl.when(i < n_col)
    def _():
        right = lax.rem(i, 2) == 0
        for side in range(2):
            acc = jnp.dot(ga_ref[side, 0], wo_ref[...], preferred_element_type=f32)
            for dist in range(1, RING):
                acc = acc + jnp.dot(ga_ref[side, dist], wg_ref[side * 3 + dist - 1], preferred_element_type=f32)
            one, two, three = (acc[dist * CHUNK:(dist + 1) * CHUNK] for dist in range(1, RING))
            own_s[side, i] = acc[:CHUNK]
            send_s[relay, side, i] = two.astype(bf16)
            send_s[direct, side, i] = jnp.where(right, three, one).astype(bf16)
            near_s[side, i] = jnp.where(right, one, three)

    @pl.when(i == 0)
    def _():
        pl.semaphore_wait(pltpu.get_barrier_semaphore(), 4)

    @pl.when(i < n_col)
    def _():
        for kind in (relay, direct):
            for side in range(2):
                part_copy(kind, side, i).start()

    @pl.when((i >= LAG) & (i < n_col + LAG))
    def _():
        b = i - LAG
        for side in range(2):
            part_copy(relay, side, b).wait_recv()
            send_s[joined, side, b] = (near_s[side, b] + recv_s[relay, side, b].astype(f32)).astype(bf16)
        for side in range(2):
            part_copy(joined, side, b).start()

    @pl.when(i == n_col + LAG)
    def _():
        x_copy().wait()

    @pl.when(i >= n_col + LAG)
    def _():
        b = i - n_col - LAG
        cols = pl.ds(pl.multiple_of(b * width, width), width)
        for side in range(2):
            part_copy(relay, side, b).wait_send()
            part_copy(direct, side, b).wait()
            part_copy(joined, side, b).wait()
            acc = own_s[side, b] + recv_s[direct, side, b].astype(f32) + recv_s[joined, side, b].astype(f32)
            at = side * CHUNK
            out_ref[at:at + CHUNK, :] = (x_s[at:at + CHUNK, cols].astype(f32) + acc).astype(bf16)


def out_call(g_all, w_out, w_got, x_blk):
    inner, d_model = w_out.shape
    rows = 2 * CHUNK
    width = min(256, d_model)
    n_col = d_model // width
    f32, bf16 = jnp.float32, jnp.bfloat16

    def column(i):
        return jnp.minimum(i, n_col - 1)

    return pl.pallas_call(
        functools.partial(out_kernel, n_col),
        grid=(2 * n_col + LAG,),
        out_shape=jax.ShapeDtypeStruct((rows, d_model), bf16),
        in_specs=[pl.BlockSpec(g_all.shape, lambda i: (0, 0, 0, 0), pipeline_mode=pl.Buffered(1)),
                  pl.BlockSpec((inner, width), lambda i: (0, column(i))),
                  pl.BlockSpec((2 * (RING - 1), inner, width), lambda i: (0, 0, column(i))),
                  pl.BlockSpec(memory_space=pl.ANY)],
        out_specs=pl.BlockSpec((rows, width), lambda i: (0, jnp.maximum(i - n_col - LAG, 0))),
        scratch_shapes=[
            pltpu.VMEM((3, 2, n_col, CHUNK, width), bf16),
            pltpu.VMEM((3, 2, n_col, CHUNK, width), bf16),
            pltpu.VMEM((2, n_col, CHUNK, width), f32),
            pltpu.VMEM((2, n_col, CHUNK, width), f32),
            pltpu.VMEM((rows, d_model), bf16),
            pltpu.SemaphoreType.DMA,
            pltpu.SemaphoreType.DMA((3, 2, n_col)),
            pltpu.SemaphoreType.DMA((3, 2, n_col)),
        ],
        compiler_params=pltpu.CompilerParams(collective_id=1, has_side_effects=True, vmem_limit_bytes=60 * 1024 * 1024,
                                             dimension_semantics=('arbitrary',)),
        cost_estimate=pl.CostEstimate(flops=2 * 2 * 4 * CHUNK * 4 * inner * d_model, bytes_accessed=40 << 20, transcendentals=0),
    )(g_all, w_out, w_got, x_blk)


def solution(mesh):
    n_seq = mesh.shape['sp']

    def device_fn(x_blk, w_z, w_x, w_bc, w_dt, a_neg, dt_bias, d_skip, w_out):
        g_all, w_got = scan_call(x_blk, w_z, w_x, w_bc, w_dt, a_neg, dt_bias, d_skip, w_out, n_seq)
        return out_call(g_all, w_out, w_got, x_blk)

    in_specs = (P(('dp', 'sp'), None), P(None, 'tp'), P(None, 'tp'), P(None, None), P(None, 'tp'), P('tp'), P('tp'), P('tp'), P('tp', None))
    out_specs = P(('dp', 'sp', 'tp'), None)
    return jax.shard_map(device_fn, mesh=mesh, in_specs=in_specs, out_specs=out_specs, check_vma=False)
```
